32 devices in a mesh: facet: 4 (over y, x), col: 8 (over z, core).
Axes of the slice: x: 2, y: 2, z: 4, core: 2. Of those that a mesh axis runs over, the one named last changes fastest.
Arguments:
- facets: bfloat16 [4, 2, 768, 768], P('facet', None, 'col'), may hold values from -6 to 6
- col_offsets: int32 [8], replicated, may hold values from 0 to 767
- sub_rows: int32 [4, 8], P(None, 'col'), may hold values from 0 to 767
- facet_offsets: int32 [4, 2], replicated, may hold values from 0 to 320
- vis_pos: int32 [4, 8, 2, 256], P('facet', 'col'), may hold values from 0 to 1535
- observed: float32 [4, 8, 2, 256], P('facet', 'col'), may hold values from -6 to 6
Outputs:
- predicted: float32 [4, 8, 2, 256], P('facet', 'col')
- facet_update: float32 [4, 2, 768, 768], P('facet', None, 'col')
The draws below stay inside these ranges and needn't reach their ends.
All inputs are finite; a program needn't handle non-finite values.
Results may differ from the reference program's by a relative error of at most 0.0085.
Values may be sent and summed in bfloat16 or wider, within the bound.
A program may use at most 64 MiB of HBM per device.

```python
import math
import jax
import jax.numpy as jnp
from jax import lax

M = 64
SUB = 384
FINE = 1536
YN = 768
VIS = 256
FACETS = 4
COLS = 8
SGCOL = 4


def with_ends(result, stream_key, low, high):
    shape = result.shape
    place = [jax.random.randint(jax.random.fold_in(stream_key, axis), (), 0, shape[axis]) for axis in range(len(shape))]
    result = result.at[tuple(place)].set(low)
    longest = shape.index(max(shape))
    place[longest] = (place[longest] + 1) % shape[longest]
    return result.at[tuple(place)].set(high)


def block_scale(key, dims, shards, smallest, high):
    gain, own = 1.0, jax.random.fold_in(key, 6)
    for dim, shards_of in shards:
        heights = jnp.exp(jax.random.uniform(jax.random.fold_in(own, dim), (shards_of,), jnp.float32, smallest / len(shards), high / len(shards)))
        gain = gain * jnp.repeat(heights, dims[dim] // shards_of).reshape([-1 if axis == dim else 1 for axis in range(len(dims))])
    return gain


def normal_values(own_key, extent, scale, reach, split=(), kind=jnp.bfloat16):
    array = scale * jax.random.normal(own_key, extent, jnp.float32)
    if split:
        array = array * block_scale(own_key, extent, split, -0.22, 0.18)
    return jnp.clip(array, -reach, reach).astype(kind)


def setup_inputs(seed: int = 0) -> dict:
    streams_of = jax.random.split(jax.random.key(seed), 7)
    facets = normal_values(streams_of[0], (FACETS, 2, YN, YN), 1.0, 6.0, ((0, 4), (2, 8)))
    col_offsets = with_ends(jax.random.randint(streams_of[1], (COLS,), 0, YN), jax.random.fold_in(streams_of[1], 1), 0, YN - 1).astype(jnp.int32)
    sub_rows = with_ends(jax.random.randint(streams_of[2], (SGCOL, COLS), 0, YN), jax.random.fold_in(streams_of[2], 1), 0, YN - 1).astype(jnp.int32)
    facet_offsets = with_ends(jax.random.randint(streams_of[3], (FACETS, 2), 0, SUB - M + 1), jax.random.fold_in(streams_of[3], 1), 0, SUB - M).astype(jnp.int32)
    vis_pos = with_ends(jax.random.randint(streams_of[4], (SGCOL, COLS, 2, VIS), 0, FINE), jax.random.fold_in(streams_of[4], 1), 0, FINE - 1).astype(jnp.int32)
    observed = normal_values(streams_of[5], (SGCOL, COLS, 2, VIS), 1.0, 6.0, ((0, 4), (1, 8)), jnp.float32)
    return {"facets": facets, "col_offsets": col_offsets, "sub_rows": sub_rows, "facet_offsets": facet_offsets, "vis_pos": vis_pos, "observed": observed}


def phase_table(first_idx, second_idx, modulus, direction, factor):
    product = first_idx[:, None] * second_idx[None, :] % modulus
    angle = direction * 2.0 * math.pi / modulus * product.astype(jnp.float32)
    return (jnp.cos(angle) * factor, jnp.sin(angle) * factor)

def plain_dot(left, right):
    return jnp.dot(left, right, preferred_element_type=jnp.float32)

def lead_dot(left, right):
    return lax.dot_general(left, right, (((0,), (0,)), ((), ())), preferred_element_type=jnp.float32)

def tail_dot(left, right):
    return lax.dot_general(left, right, (((1,), (1,)), ((), ())), preferred_element_type=jnp.float32)

def batch_prod(form, left, right):
    return jnp.einsum(form, left.astype(jnp.float32), right.astype(jnp.float32), precision=lax.Precision.HIGHEST)

def place_blocks(blocks, facet_offsets, sub_count):
    zero_idx = jnp.zeros((), jnp.int32)
    canvas = jnp.zeros((2, sub_count, SUB, SUB), jnp.float32)

    def add_block(facet_idx, canvas):
        corner_at = (zero_idx, zero_idx, facet_offsets[facet_idx, 0].astype(jnp.int32), facet_offsets[facet_idx, 1].astype(jnp.int32))
        current = lax.dynamic_slice(canvas, corner_at, (2, sub_count, M, M))
        return lax.dynamic_update_slice(canvas, current + blocks[facet_idx], corner_at)
    return lax.fori_loop(0, blocks.shape[0], add_block, canvas).astype(jnp.bfloat16)

def degrid(sub_image, positions, measured):
    across = jnp.arange(SUB, dtype=jnp.int32)
    spread = 1.0 / math.sqrt(SUB)

    def one_table(points):
        return phase_table(points, across, FINE, 1.0, spread)
    u_re, u_im = jax.vmap(one_table)(positions[:, 0])
    v_re, v_im = jax.vmap(one_table)(positions[:, 1])
    u_re = u_re.astype(jnp.bfloat16)
    u_im = u_im.astype(jnp.bfloat16)
    rows_re = batch_prod('sna,sab->snb', u_re, sub_image[0]) - batch_prod('sna,sab->snb', u_im, sub_image[1])
    rows_im = batch_prod('sna,sab->snb', u_re, sub_image[1]) + batch_prod('sna,sab->snb', u_im, sub_image[0])
    pred_re = lax.optimization_barrier(jnp.sum(rows_re * v_re - rows_im * v_im, axis=2))
    pred_im = lax.optimization_barrier(jnp.sum(rows_re * v_im + rows_im * v_re, axis=2))
    predicted = jnp.stack([pred_re, pred_im], axis=1)
    diff_re = (pred_re - measured[:, 0])[:, :, None]
    diff_im = (pred_im - measured[:, 1])[:, :, None]
    weight = SUB / math.sqrt(positions.shape[2])
    wgt_re = ((diff_re * v_re + diff_im * v_im) * weight).astype(jnp.bfloat16)
    wgt_im = ((diff_im * v_re - diff_re * v_im) * weight).astype(jnp.bfloat16)
    grad_re = batch_prod('sna,snb->sab', u_re, wgt_re) + batch_prod('sna,snb->sab', u_im, wgt_im)
    grad_im = batch_prod('sna,snb->sab', u_re, wgt_im) - batch_prod('sna,snb->sab', u_im, wgt_re)
    return (predicted, jnp.stack([grad_re, grad_im]).astype(jnp.bfloat16))

def reference(facets, col_offsets, sub_rows, facet_offsets, vis_pos, observed):
    facet_count = facets.shape[0]
    sub_count = sub_rows.shape[0]
    col_count = col_offsets.shape[0]
    zero_idx = jnp.zeros((), jnp.int32)
    along_facet = jnp.arange(YN, dtype=jnp.int32)
    narrow_idx = jnp.arange(M, dtype=jnp.int32)
    inv_root = 1.0 / math.sqrt(YN)
    facet_re = facets[:, 0].reshape(facet_count * YN, YN)
    facet_im = facets[:, 1].reshape(facet_count * YN, YN)
    back_scale = math.sqrt(YN / (M * sub_count))

    def arrange(block):
        return block.reshape(sub_count, M, facet_count, M).transpose(2, 0, 1, 3)

    def regroup(block):
        return block.transpose(1, 2, 0, 3).reshape(sub_count * M, facet_count * M)

    def unfold(block):
        return block.reshape(YN, facet_count, M).transpose(1, 0, 2).reshape(facet_count * YN, M)

    def cut_blocks(gradient):

        def cut_one(offsets):
            corner_at = (zero_idx, zero_idx, offsets[0].astype(jnp.int32), offsets[1].astype(jnp.int32))
            return lax.dynamic_slice(gradient, corner_at, (2, sub_count, M, M))
        return jax.vmap(cut_one)(facet_offsets)

    def column_step(accum, column):
        w_re, w_im = phase_table(along_facet, narrow_idx + col_offsets[column], YN, -1.0, inv_root)
        w_re = w_re.astype(jnp.bfloat16)
        w_im = w_im.astype(jnp.bfloat16)
        strip_re = (plain_dot(facet_re, w_re) - plain_dot(facet_im, w_im)).astype(jnp.bfloat16)
        strip_im = (plain_dot(facet_re, w_im) + plain_dot(facet_im, w_re)).astype(jnp.bfloat16)
        strip_re = strip_re.reshape(facet_count, YN, M).transpose(1, 0, 2).reshape(YN, facet_count * M)
        strip_im = strip_im.reshape(facet_count, YN, M).transpose(1, 0, 2).reshape(YN, facet_count * M)
        targets = (narrow_idx[None, :] + sub_rows[:, column][:, None]).reshape(sub_count * M)
        e_re, e_im = phase_table(targets, along_facet, YN, -1.0, inv_root)
        e_re = e_re.astype(jnp.bfloat16)
        e_im = e_im.astype(jnp.bfloat16)
        contrib_re = (plain_dot(e_re, strip_re) - plain_dot(e_im, strip_im)).astype(jnp.bfloat16)
        contrib_im = (plain_dot(e_re, strip_im) + plain_dot(e_im, strip_re)).astype(jnp.bfloat16)
        blocks = jnp.stack([arrange(contrib_re), arrange(contrib_im)], axis=1).astype(jnp.float32)
        sub_image = place_blocks(blocks, facet_offsets, sub_count)
        predicted, gradient = degrid(sub_image, vis_pos[:, column], observed[:, column])
        backs = cut_blocks(gradient)
        back_re = regroup(backs[:, 0])
        back_im = regroup(backs[:, 1])
        delta_re = ((lead_dot(e_re, back_re) + lead_dot(e_im, back_im)) * back_scale).astype(jnp.bfloat16)
        delta_im = ((lead_dot(e_re, back_im) - lead_dot(e_im, back_re)) * back_scale).astype(jnp.bfloat16)
        delta_re = unfold(delta_re)
        delta_im = unfold(delta_im)
        add_re = tail_dot(delta_re, w_re) + tail_dot(delta_im, w_im)
        add_im = tail_dot(delta_im, w_re) - tail_dot(delta_re, w_im)
        return ((accum[0] + add_re, accum[1] + add_im), predicted)
    start_acc = (jnp.zeros((facet_count * YN, YN), jnp.float32), jnp.zeros((facet_count * YN, YN), jnp.float32))
    (acc_re, acc_im), predicted = lax.scan(column_step, start_acc, jnp.arange(col_count, dtype=jnp.int32))
    up_scale = math.sqrt(YN / (M * col_count))
    update = jnp.stack([acc_re, acc_im]).reshape(2, facet_count, YN, YN).transpose(1, 0, 2, 3) * up_scale
    return (predicted.transpose(1, 0, 2, 3), update)
```

```python
import functools
import math

import jax
import jax.numpy as jnp
from jax import lax
from jax.experimental import pallas as pl
from jax.experimental.pallas import tpu as pltpu
from jax.sharding import PartitionSpec as P

M = 64
SUB = 384
FINE = 1536
YN = 768
MARGIN = 8192
PATHS_BEFORE = 2
MESH = pl.DeviceIdType.MESH
F32 = jnp.float32
BF16 = jnp.bfloat16


def cis(product, modulus, direction):
    turns = jnp.floor(product * (1.0 / modulus) + 0.5)
    half = (product - turns * modulus) * (direction * math.pi / modulus)
    z = half * half
    s = half * (1.0 + z * (-1 / 6 + z * (1 / 120 + z * (-1 / 5040 + z * (1 / 362880 + z * (-1 / 39916800))))))
    c = 1.0 + z * (-1 / 2 + z * (1 / 24 + z * (-1 / 720 + z * (1 / 40320 + z * (-1 / 3628800 + z * (1 / 479001600))))))
    return 1.0 - 2.0 * s * s, 2.0 * s * c


def iota(shape, axis):
    return lax.broadcasted_iota(jnp.int32, shape, axis).astype(F32)


def dot(left, right, dims):
    return lax.dot_general(left, right, (dims, ((), ())), preferred_element_type=F32)


NN = ((1,), (0,))
NT = ((1,), (1,))
TN = ((0,), (0,))
N_POWER = 7


def cmul(a, b):
    return a[0] * b[0] - a[1] * b[1], a[0] * b[1] + a[1] * b[0]


def loop(n, step, carry=()):
    return lax.fori_loop(0, n, step, carry, unroll=n <= 4)


def kernel(
    n_facet,
    n_col,
    facets_hbm,
    col_offsets_hbm,
    sub_rows_hbm,
    facet_offsets_hbm,
    vis_pos_hbm,
    observed_hbm,
    predicted,
    sides,
    wall,
    facet_buf,
    col_offsets,
    sub_rows,
    facet_offsets,
    vis_pos,
    observed,
    base,
    turn,
    subt,
    u_tab,
    v_tab,
    strip_out,
    strip_in,
    contrib_out,
    contrib_in,
    marks,
    points,
    shifts,
    powers,
    firsts,
    own_base,
    own_turn,
    paths,
    diffs,
    load_sem,
    col_send,
    col_recv,
    facet_send,
    facet_recv,
    diff_send,
    diff_recv,
):
    my_f = lax.axis_index("facet")
    my_c = lax.axis_index("col")
    n_rows = facet_buf.shape[1]
    n_vis = vis_pos.shape[3]
    room = paths.shape[1] // 2

    loads = [
        pltpu.make_async_copy(source, held, load_sem.at[i])
        for i, (source, held) in enumerate(
            (
                (col_offsets_hbm, col_offsets),
                (sub_rows_hbm, sub_rows),
                (facets_hbm.at[0], facet_buf),
                (facet_offsets_hbm, facet_offsets),
                (vis_pos_hbm, vis_pos),
                (observed_hbm, observed),
            )
        )
    ]
    for load in loads:
        load.start()
    barrier = pltpu.get_barrier_semaphore()
    n_pair = n_col // 2
    my_pair, my_core = my_c // 2, lax.rem(my_c, 2)
    side = my_pair // (n_pair // 2)
    mirrored = my_pair + side * (n_pair - 1 - 2 * my_pair)
    pair_order = []
    for place in range(n_pair - 1, 0, -1):
        target = place - (mirrored + n_pair - place) // n_pair
        pair_order.append(target + side * (n_pair - 1 - 2 * target))
    pair_order.append(my_pair)
    col_order = []
    for pair in pair_order:
        col_order += [2 * pair + 1 - my_core, 2 * pair + my_core]
    facet_order = [lax.rem(my_f + 1 + i, n_facet) for i in range(n_facet)]
    for c in col_order[:-1]:
        pl.semaphore_signal(barrier, inc=1, device_id=(my_f, c), device_id_type=MESH)
    for f in facet_order[:-1]:
        pl.semaphore_signal(barrier, inc=1, device_id=(f, my_c), device_id_type=MESH)

    def col_copy(phase, out, into, slot_out, slot_in, target):
        return pltpu.make_async_remote_copy(
            src_ref=out.at[slot_out],
            dst_ref=into.at[slot_in],
            send_sem=col_send.at[phase, slot_out],
            recv_sem=col_recv.at[phase, slot_in],
            device_id=(my_f, target),
            device_id_type=MESH,
        )

    def facet_copy(phase, out, into, slot_out, slot_in, target):
        return pltpu.make_async_remote_copy(
            src_ref=out.at[slot_out],
            dst_ref=into.at[slot_in],
            send_sem=facet_send.at[phase, slot_out],
            recv_sem=facet_recv.at[phase, slot_in],
            device_id=(target, my_c),
            device_id_type=MESH,
        )

    def mark_copy(target, slot):
        mine = marks.at[my_f, slot]
        return pltpu.make_async_remote_copy(
            src_ref=mine,
            dst_ref=mine,
            send_sem=col_send.at[1, target],
            recv_sem=col_recv.at[1, slot],
            device_id=(my_f, target),
            device_id_type=MESH,
        )

    def marks_copy(target, slot):
        return pltpu.make_async_remote_copy(
            src_ref=marks.at[slot],
            dst_ref=marks.at[slot],
            send_sem=facet_send.at[1, target],
            recv_sem=facet_recv.at[1, slot],
            device_id=(target, my_c),
            device_id_type=MESH,
        )

    def diff_copy(f, c, from_f, from_c):
        mine = diffs.at[from_f, from_c]
        return pltpu.make_async_remote_copy(
            src_ref=mine,
            dst_ref=mine,
            send_sem=diff_send.at[f, c],
            recv_sem=diff_recv.at[from_f, from_c],
            device_id=(f, c),
            device_id_type=MESH,
        )

    base_re, base_im = cis(iota((M, YN), 0) * iota((M, YN), 1), YN, -1.0)
    inv_root = 1.0 / math.sqrt(YN)
    base[0] = base_re * inv_root
    base[1] = base_im * inv_root
    along = iota((1, YN), 1)
    loads[0].wait()
    loads[1].wait()
    for c in range(n_col):
        turn[0, pl.ds(c, 1)] = along * col_offsets[c].astype(F32)
    for s in range(n_facet):
        turn[0, pl.ds(n_col + s, 1)] = along * sub_rows[0, s].astype(F32)
    turn_re, turn_im = cis(turn[0], YN, -1.0)
    turn[0] = turn_re
    turn[1] = turn_im

    def table(into, row, slot):
        re, im = turn[0, pl.ds(row, 1)], turn[1, pl.ds(row, 1)]
        into[slot, :M] = (base[0] * re - base[1] * im).astype(BF16)
        into[slot, M:] = (base[0] * im + base[1] * re).astype(BF16)

    lane = lax.broadcasted_iota(jnp.int32, (1, 2 * M), 1)
    minus_plus = jnp.where(lane < M, -1.0, 1.0)

    def swapped(value):
        return pltpu.roll(value, M, 1)

    for load in loads[3:]:
        load.wait()
    wide = marks.shape[3] - n_vis
    marks[my_f, my_c, :, :n_vis] = vis_pos[0, 0, :1] + vis_pos[0, 0, 1:] * 65536
    marks[my_f, my_c, :, n_vis:] = jnp.full((1, wide), sub_rows[0, my_f], jnp.int32)

    loads[2].wait()
    both = facet_buf[...]
    if n_rows % 16:
        both = both.astype(F32).reshape(2 * n_rows, YN).astype(BF16)
    else:
        both = both.reshape(2 * n_rows, YN)
    early = n_col - 1
    for i, c in enumerate(col_order):
        table(wall, c, c)
        prod = dot(both, wall[c], NT)
        part = (prod[:n_rows] + minus_plus * swapped(prod[n_rows:])).astype(BF16)
        if i < n_col - 1:
            strip_out[c] = part
        else:
            strip_in[c] = part
        if i == early - 1:
            pl.semaphore_wait(barrier, n_col - 1 + n_facet - 1)
            for ready in col_order[:-1]:
                mark_copy(ready, my_c).start()
            for ready in col_order[:early]:
                col_copy(0, strip_out, strip_in, ready, my_c, ready).start()
        elif early <= i < n_col - 1:
            col_copy(0, strip_out, strip_in, c, my_c, c).start()

    for s in range(n_facet):
        table(subt, n_col + s, s)
    for tab, which in ((u_tab, 0), (v_tab, 1)):
        point = vis_pos[0, 0, pl.ds(which, 1)].astype(F32)
        low_re, low_im = cis(iota((M, n_vis), 0) * point, FINE, 1.0)
        low_re = low_re * (1.0 / math.sqrt(SUB))
        low_im = low_im * (1.0 / math.sqrt(SUB))
        for f in range(n_facet):
            high_re, high_im = cis(point * facet_offsets[which, f].astype(F32), FINE, 1.0)
            tab[f, :M] = (low_re * high_re - low_im * high_im).astype(tab.dtype)
            tab[f, M:] = (low_re * high_im + low_im * high_re).astype(tab.dtype)
    near_re, near_im = cis(
        iota((M, n_rows), 0) * (iota((M, n_rows), 1) + (my_c * n_rows).astype(F32)), YN, -1.0
    )
    own_base[0] = near_re * inv_root
    own_base[1] = near_im * inv_root
    for c in col_order[:-1]:
        mark_copy(c, c).wait_recv()
    for f in facet_order[:-1]:
        marks_copy(f, my_f).start()

    for c in col_order[:-1]:
        col_copy(0, strip_out, strip_in, c, c, c).wait_recv()
    strip = strip_in[...]
    if n_rows % 16:
        strip = strip.astype(F32).reshape(YN, 2 * M).astype(BF16)
    else:
        strip = strip.reshape(YN, 2 * M)
    for i, s in enumerate(facet_order):
        prod = dot(subt[s], strip, NN)
        part = (prod[:M] + minus_plus * swapped(prod[M:])).astype(BF16)
        if i < n_facet - 1:
            contrib_out[s] = part
            facet_copy(0, contrib_out, contrib_in, s, my_f, s).start()
        else:
            contrib_in[s] = part

    for f in facet_order[:-1]:
        marks_copy(f, f).wait_recv()
    sub = lax.broadcasted_iota(jnp.int32, (8, n_vis), 0)
    bits = [lax.rem(sub // (1 << p), 2) == 1 for p in range(3)]
    rows_at = (my_c * n_rows).astype(F32)

    def spread(s, carry):
        for c in range(n_col):
            unit = s * n_col + c
            points[pl.ds(unit, 1)] = marks[s, c, :, :n_vis]
            shifts[pl.ds(unit, 1)] = marks[s, c, :, n_vis:]
        rows = pl.ds(pl.multiple_of(s * n_col, n_col), n_col)
        shift = shifts[rows].astype(F32) * (iota((n_col, wide), 1) + rows_at)
        own_turn[0, rows], own_turn[1, rows] = cis(shift, YN, -1.0)
        packed = points[rows]
        high = packed // 65536
        for which, point in ((0, packed - high * 65536), (1, high)):
            point = point.astype(F32)
            powers[which, 0, 0, rows], powers[which, 0, 1, rows] = cis(
                point * facet_offsets[which, my_f].astype(F32), FINE, -1.0
            )
            value = cis(point, FINE, -1.0)
            for p in range(1, N_POWER):
                powers[which, p, 0, rows], powers[which, p, 1, rows] = value
                if p < N_POWER - 1:
                    value = cmul(value, value)
        return carry

    loop(n_facet, spread)

    def power(which, p, unit):
        return powers[which, p, 0, pl.ds(unit, 1)], powers[which, p, 1, pl.ds(unit, 1)]

    def first(which, unit):
        value = None
        for p in range(3):
            re, im = power(which, 1 + p, unit)
            step = jnp.where(bits[p], re, 1.0), jnp.where(bits[p], im, 0.0)
            value = step if value is None else cmul(value, step)
        return cmul(value, power(which, 0, unit))

    def filled(which, start, unit):
        parts = [start]
        for p in range(4, N_POWER):
            by = power(which, p, unit)
            parts += [cmul(part, by) for part in parts]
        return [jnp.concatenate([part[i] for part in parts], axis=0) for i in range(2)]

    def make_path(c):
        def one(s, carry):
            unit = s * n_col + c
            u_re, u_im = filled(0, first(0, unit), unit)
            u_re, u_im = u_re.astype(BF16), u_im.astype(BF16)
            v_first = first(1, unit)
            firsts[unit, 0], firsts[unit, 1] = v_first
            re = own_turn[0, pl.ds(unit, 1), :n_rows]
            im = own_turn[1, pl.ds(unit, 1), :n_rows]
            e_re, e_im = cmul((own_base[0], own_base[1]), (re, im))
            e_tab = jnp.concatenate([e_re, e_im], axis=0).astype(BF16)
            paths[unit, :n_rows] = dot(e_tab, jnp.concatenate([u_re, u_im], axis=0), TN).astype(BF16)
            paths[unit, room : room + n_rows] = dot(
                e_tab, jnp.concatenate([u_im, -u_re], axis=0), TN
            ).astype(BF16)
            return carry

        loop(n_facet, one)

    near_order = col_order[::-1]
    for c in near_order[:PATHS_BEFORE]:
        make_path(c)

    pred_re = jnp.zeros((M, n_vis), F32)
    pred_im = jnp.zeros((M, n_vis), F32)
    for i in range(n_facet):
        f = facet_order[n_facet - 1 - i]
        if i > 0:
            facet_copy(0, contrib_out, contrib_in, f, f, f).wait_recv()
        with_re = dot(contrib_in[f], u_tab[f, :M], TN)
        with_im = dot(contrib_in[f], u_tab[f, M:], TN)
        rows_re = with_re[:M] - with_im[M:]
        rows_im = with_im[:M] + with_re[M:]
        v_re, v_im = v_tab[f, :M], v_tab[f, M:]
        pred_re += rows_re * v_re - rows_im * v_im
        pred_im += rows_re * v_im + rows_im * v_re
    pred_re = jnp.sum(pred_re, axis=0, keepdims=True)
    pred_im = jnp.sum(pred_im, axis=0, keepdims=True)
    predicted[0, 0, pl.ds(0, 1)] = pred_re
    predicted[0, 0, pl.ds(1, 1)] = pred_im
    weight = SUB / math.sqrt(n_vis) / SUB
    weight *= math.sqrt(YN / (M * n_facet)) * math.sqrt(YN / (M * n_col))
    diffs[my_f, my_c] = ((predicted[0, 0] - observed[0, 0]) * weight).astype(diffs.dtype)
    for c in col_order[:-1]:

        def send(i, carry, c=c):
            diff_copy(lax.rem(my_f + i, n_facet), c, my_f, my_c).start()
            return carry

        loop(n_facet, send)
    for f in facet_order[:-1]:
        diff_copy(f, my_c, my_f, my_c).start()

    for c in near_order[PATHS_BEFORE:]:
        make_path(c)

    def gather(c, own):
        def one(i, total):
            s = lax.rem(my_f + i, n_facet)
            unit = s * n_col + c
            diff = diffs[s, c].astype(F32)
            diff = diff[:1], diff[1:]
            start = cmul((firsts[unit, 0], firsts[unit, 1]), diff)
            wgt = jnp.concatenate(filled(1, start, unit), axis=0).astype(BF16)
            return total + dot(paths[unit], wgt, NT)

        def wait(i, carry):
            s = lax.rem(my_f + i, n_facet)
            diff_copy(s, c, s, c).wait_recv()
            return carry

        if own:
            for s in facet_order[:-1]:
                diff_copy(s, c, s, c).wait_recv()
        else:
            loop(n_facet, wait)
        prod = loop(n_facet, one, jnp.zeros((2 * room, 2 * M), F32))
        re, im = prod[:n_rows], prod[room : room + n_rows]
        at = pl.ds(pl.multiple_of(c * 2 * M, 2 * M), 2 * M)
        sides[:n_rows, at] = (re + minus_plus * swapped(im)).astype(BF16)
        sides[room : room + n_rows, at] = (im - minus_plus * swapped(re)).astype(BF16)

    for i, c in enumerate(near_order):
        gather(c, i == 0)

    for c in col_order[:-1]:
        col_copy(0, strip_out, strip_in, c, c, c).wait_send()
        mark_copy(c, my_c).wait_send()

        def sent(f, carry, c=c):
            diff_copy(f, c, my_f, my_c).wait_send()
            return carry

        loop(n_facet, sent)
    for f in facet_order[:-1]:
        facet_copy(0, contrib_out, contrib_in, f, f, f).wait_send()
        marks_copy(f, my_f).wait_send()
        diff_copy(f, my_c, my_f, my_c).wait_send()


def finish_kernel(predicted, sides, wall, predicted_hbm, update_hbm, update, sems):
    copies = [pltpu.make_async_copy(predicted, predicted_hbm, sems.at[0])]
    copies[0].start()
    n_rows = update.shape[1]
    room = sides.shape[0] // 2
    walls = wall[...].reshape(sides.shape[1], update.shape[2])
    step = 256
    for i in range(update.shape[2] // step):
        at = slice(i * step, (i + 1) * step)
        prod = dot(sides[...], walls[:, at], NN)
        update[0, :, at] = prod[:n_rows]
        update[1, :, at] = prod[room : room + n_rows]
        copies.append(pltpu.make_async_copy(update.at[:, :, at], update_hbm.at[0, :, :, at], sems.at[1 + i]))
        copies[-1].start()
    for copy in copies:
        copy.wait()


def finish(predicted, sides, wall, facets_shape):
    vmem = pl.BlockSpec(memory_space=pltpu.VMEM)
    hbm = pl.BlockSpec(memory_space=pltpu.HBM)
    return pl.pallas_call(
        finish_kernel,
        out_shape=(
            jax.ShapeDtypeStruct(predicted.shape, F32),
            jax.ShapeDtypeStruct(facets_shape, F32),
        ),
        in_specs=[vmem] * 3,
        out_specs=(hbm, hbm),
        scratch_shapes=[
            pltpu.VMEM(facets_shape[1:], F32),
            pltpu.SemaphoreType.DMA((1 + facets_shape[3] // 256,)),
        ],
        compiler_params=pltpu.CompilerParams(vmem_limit_bytes=2**22),
        name="finish",
    )(predicted, sides, wall)


def body(n_facet, n_col, facets, col_offsets, sub_rows, facet_offsets, vis_pos, observed):
    assert sub_rows.shape[0] == n_facet
    n_rows = facets.shape[2]
    n_vis = vis_pos.shape[3]
    vmem = pl.BlockSpec(memory_space=pltpu.VMEM)
    facet_blocks = pltpu.VMEM((n_facet, M, 2 * M), BF16)
    col_blocks = pltpu.VMEM((n_col, n_rows, 2 * M), BF16)
    table_rows = n_col + n_facet
    room = -(-n_rows // 16) * 16
    wide = -(-n_rows // 128) * 128
    n_units = n_col * n_facet
    sides = (2 * room, n_col * 2 * M)
    wall = (n_col, 2 * M, YN)
    held = 4 * observed.size + 2 * (math.prod(sides) + math.prod(wall))
    vmem_left = (67043328 - held) // 1024 * 1024 - MARGIN
    results = pl.pallas_call(
            functools.partial(kernel, n_facet, n_col),
            out_shape=(pltpu.VMEM(observed.shape, F32), pltpu.VMEM(sides, BF16), pltpu.VMEM(wall, BF16)),
            in_specs=[pl.BlockSpec(memory_space=pltpu.HBM)] * 6,
            out_specs=(vmem, vmem, vmem),
            scratch_shapes=[
                pltpu.VMEM((2, n_rows, YN), BF16),
                pltpu.SMEM(col_offsets.shape, jnp.int32),
                pltpu.SMEM(sub_rows.shape[::-1], jnp.int32),
                pltpu.SMEM(facet_offsets.shape[::-1], jnp.int32),
                pltpu.VMEM(vis_pos.shape, jnp.int32),
                pltpu.VMEM(observed.shape, F32),
                pltpu.VMEM((2, M, YN), F32),
                pltpu.VMEM((2, table_rows, YN), F32),
                pltpu.VMEM((n_facet, 2 * M, YN), BF16),
                pltpu.VMEM((n_facet, 2 * M, n_vis), BF16),
                pltpu.VMEM((n_facet, 2 * M, n_vis), F32),
                col_blocks,
                col_blocks,
                facet_blocks,
                facet_blocks,
                pltpu.VMEM((n_facet, n_col, 1, n_vis + wide), jnp.int32),
                pltpu.VMEM((n_units, n_vis), jnp.int32),
                pltpu.VMEM((n_units, wide), jnp.int32),
                pltpu.VMEM((2, N_POWER, 2, n_units, n_vis), F32),
                pltpu.VMEM((n_units, 2, 8, n_vis), F32),
                pltpu.VMEM((2, M, n_rows), F32),
                pltpu.VMEM((2, n_units, wide), F32),
                pltpu.VMEM((n_units, 2 * room, n_vis), BF16),
                pltpu.VMEM((n_facet, n_col, 2, n_vis), BF16),
                pltpu.SemaphoreType.DMA((6,)),
                pltpu.SemaphoreType.DMA((2, n_col)),
                pltpu.SemaphoreType.DMA((2, n_col)),
                pltpu.SemaphoreType.DMA((2, n_facet)),
                pltpu.SemaphoreType.DMA((2, n_facet)),
                pltpu.SemaphoreType.DMA((n_facet, n_col)),
                pltpu.SemaphoreType.DMA((n_facet, n_col)),
            ],
            compiler_params=pltpu.CompilerParams(
                collective_id=0, has_side_effects=True, vmem_limit_bytes=vmem_left
            ),
            name="predict_update",
        )(facets, col_offsets, sub_rows.T, facet_offsets.T, vis_pos, observed)
    return finish(*results, facets.shape)


def solution(mesh):
    in_specs = (
        P("facet", None, "col", None),
        P(),
        P(None, "col"),
        P(),
        P("facet", "col", None, None),
        P("facet", "col", None, None),
    )
    out_specs = (P("facet", "col", None, None), P("facet", None, "col", None))
    step = functools.partial(body, mesh.shape["facet"], mesh.shape["col"])
    return jax.shard_map(step, mesh=mesh, in_specs=in_specs, out_specs=out_specs, check_vma=False)
```

```python
import functools
import math

import jax
import jax.numpy as jnp
from jax import lax
from jax.experimental import pallas as pl
from jax.experimental.pallas import tpu as pltpu
from jax.sharding import PartitionSpec as P

M = 64
SUB = 384
FINE = 1536
YN = 768
MARGIN = 8192
PATHS_BEFORE = 4
MESH = pl.DeviceIdType.MESH
F32 = jnp.float32
BF16 = jnp.bfloat16


def cis(product, modulus, direction):
    turns = jnp.floor(product * (1.0 / modulus) + 0.5)
    half = (product - turns * modulus) * (direction * math.pi / modulus)
    z = half * half
    s = half * (1.0 + z * (-1 / 6 + z * (1 / 120 + z * (-1 / 5040 + z * (1 / 362880 + z * (-1 / 39916800))))))
    c = 1.0 + z * (-1 / 2 + z * (1 / 24 + z * (-1 / 720 + z * (1 / 40320 + z * (-1 / 3628800 + z * (1 / 479001600))))))
    return 1.0 - 2.0 * s * s, 2.0 * s * c


def iota(shape, axis):
    return lax.broadcasted_iota(jnp.int32, shape, axis).astype(F32)


def dot(left, right, dims):
    return lax.dot_general(left, right, (dims, ((), ())), preferred_element_type=F32)


NN = ((1,), (0,))
NT = ((1,), (1,))
TN = ((0,), (0,))
N_POWER = 7


def cmul(a, b):
    return a[0] * b[0] - a[1] * b[1], a[0] * b[1] + a[1] * b[0]


def loop(n, step, carry=()):
    return lax.fori_loop(0, n, step, carry, unroll=n <= 4)


def kernel(
    n_facet,
    n_col,
    facets_hbm,
    col_offsets_hbm,
    sub_rows_hbm,
    facet_offsets_hbm,
    vis_pos_hbm,
    observed_hbm,
    predicted,
    sides,
    wall,
    partial,
    facet_buf,
    col_offsets,
    sub_rows,
    facet_offsets,
    vis_pos,
    observed,
    base,
    turn,
    subt,
    u_tab,
    v_tab,
    strip_out,
    strip_in,
    contrib_out,
    contrib_in,
    marks,
    points,
    shifts,
    powers,
    firsts,
    own_base,
    own_turn,
    paths,
    diffs,
    load_sem,
    col_send,
    col_recv,
    facet_send,
    facet_recv,
    diff_send,
    diff_recv,
):
    my_f = lax.axis_index("facet")
    my_c = lax.axis_index("col")
    n_rows = facet_buf.shape[1]
    n_vis = vis_pos.shape[3]
    room = paths.shape[1] // 2

    loads = [
        pltpu.make_async_copy(source, held, load_sem.at[i])
        for i, (source, held) in enumerate(
            (
                (col_offsets_hbm, col_offsets),
                (sub_rows_hbm, sub_rows),
                (facets_hbm.at[0], facet_buf),
                (facet_offsets_hbm, facet_offsets),
                (vis_pos_hbm, vis_pos),
                (observed_hbm, observed),
            )
        )
    ]
    for load in loads:
        load.start()
    barrier = pltpu.get_barrier_semaphore()
    n_pair = n_col // 2
    my_pair, my_core = my_c // 2, lax.rem(my_c, 2)
    side = my_pair // (n_pair // 2)
    mirrored = my_pair + side * (n_pair - 1 - 2 * my_pair)
    pair_order = []
    for place in range(n_pair - 1, 0, -1):
        target = place - (mirrored + n_pair - place) // n_pair
        pair_order.append(target + side * (n_pair - 1 - 2 * target))
    pair_order.append(my_pair)
    col_order = []
    for pair in pair_order:
        col_order += [2 * pair + 1 - my_core, 2 * pair + my_core]
    facet_order = [lax.rem(my_f + 1 + i, n_facet) for i in range(n_facet)]
    for c in col_order[:-1]:
        pl.semaphore_signal(barrier, inc=1, device_id=(my_f, c), device_id_type=MESH)
    for f in facet_order[:-1]:
        pl.semaphore_signal(barrier, inc=1, device_id=(f, my_c), device_id_type=MESH)

    def col_copy(phase, out, into, slot_out, slot_in, target):
        return pltpu.make_async_remote_copy(
            src_ref=out.at[slot_out],
            dst_ref=into.at[slot_in],
            send_sem=col_send.at[phase, slot_out],
            recv_sem=col_recv.at[phase, slot_in],
            device_id=(my_f, target),
            device_id_type=MESH,
        )

    def facet_copy(phase, out, into, slot_out, slot_in, target):
        return pltpu.make_async_remote_copy(
            src_ref=out.at[slot_out],
            dst_ref=into.at[slot_in],
            send_sem=facet_send.at[phase, slot_out],
            recv_sem=facet_recv.at[phase, slot_in],
            device_id=(target, my_c),
            device_id_type=MESH,
        )

    def mark_copy(target, slot):
        mine = marks.at[my_f, slot]
        return pltpu.make_async_remote_copy(
            src_ref=mine,
            dst_ref=mine,
            send_sem=col_send.at[1, target],
            recv_sem=col_recv.at[1, slot],
            device_id=(my_f, target),
            device_id_type=MESH,
        )

    def marks_copy(target, slot):
        return pltpu.make_async_remote_copy(
            src_ref=marks.at[slot],
            dst_ref=marks.at[slot],
            send_sem=facet_send.at[1, target],
            recv_sem=facet_recv.at[1, slot],
            device_id=(target, my_c),
            device_id_type=MESH,
        )

    def diff_copy(f, c, from_f, from_c):
        mine = diffs.at[from_f, from_c]
        return pltpu.make_async_remote_copy(
            src_ref=mine,
            dst_ref=mine,
            send_sem=diff_send.at[f, c],
            recv_sem=diff_recv.at[from_f, from_c],
            device_id=(f, c),
            device_id_type=MESH,
        )

    base_re, base_im = cis(iota((M, YN), 0) * iota((M, YN), 1), YN, -1.0)
    inv_root = 1.0 / math.sqrt(YN)
    base[0] = base_re * inv_root
    base[1] = base_im * inv_root
    along = iota((1, YN), 1)
    loads[0].wait()
    loads[1].wait()
    for c in range(n_col):
        turn[0, pl.ds(c, 1)] = along * col_offsets[c].astype(F32)
    for s in range(n_facet):
        turn[0, pl.ds(n_col + s, 1)] = along * sub_rows[0, s].astype(F32)
    turn_re, turn_im = cis(turn[0], YN, -1.0)
    turn[0] = turn_re
    turn[1] = turn_im

    def table(into, row, slot):
        re, im = turn[0, pl.ds(row, 1)], turn[1, pl.ds(row, 1)]
        into[slot, :M] = (base[0] * re - base[1] * im).astype(BF16)
        into[slot, M:] = (base[0] * im + base[1] * re).astype(BF16)

    lane = lax.broadcasted_iota(jnp.int32, (1, 2 * M), 1)
    minus_plus = jnp.where(lane < M, -1.0, 1.0)

    def swapped(value):
        return pltpu.roll(value, M, 1)

    for load in loads[3:]:
        load.wait()
    wide = marks.shape[3] - n_vis
    marks[my_f, my_c, :, :n_vis] = vis_pos[0, 0, :1] + vis_pos[0, 0, 1:] * 65536
    marks[my_f, my_c, :, n_vis:] = jnp.full((1, wide), sub_rows[0, my_f], jnp.int32)

    loads[2].wait()
    both = facet_buf[...]
    if n_rows % 16:
        both = both.astype(F32).reshape(2 * n_rows, YN).astype(BF16)
    else:
        both = both.reshape(2 * n_rows, YN)
    early = n_col - 1
    for i, c in enumerate(col_order):
        place = n_col - 1 - i
        table(wall, c, place)
        prod = dot(both, wall[place], NT)
        part = (prod[:n_rows] + minus_plus * swapped(prod[n_rows:])).astype(BF16)
        if i < n_col - 1:
            strip_out[c] = part
        else:
            strip_in[c] = part
        if i == early - 1:
            pl.semaphore_wait(barrier, n_col - 1 + n_facet - 1)
            for ready in col_order[:-1]:
                mark_copy(ready, my_c).start()
            for ready in col_order[:early]:
                col_copy(0, strip_out, strip_in, ready, my_c, ready).start()
        elif early <= i < n_col - 1:
            col_copy(0, strip_out, strip_in, c, my_c, c).start()

    for s in range(n_facet):
        table(subt, n_col + s, s)
    for tab, which in ((u_tab, 0), (v_tab, 1)):
        point = vis_pos[0, 0, pl.ds(which, 1)].astype(F32)
        low_re, low_im = cis(iota((M, n_vis), 0) * point, FINE, 1.0)
        low_re = low_re * (1.0 / math.sqrt(SUB))
        low_im = low_im * (1.0 / math.sqrt(SUB))
        for f in range(n_facet):
            high_re, high_im = cis(point * facet_offsets[which, f].astype(F32), FINE, 1.0)
            tab[f, :M] = (low_re * high_re - low_im * high_im).astype(tab.dtype)
            tab[f, M:] = (low_re * high_im + low_im * high_re).astype(tab.dtype)
    near_re, near_im = cis(
        iota((M, n_rows), 0) * (iota((M, n_rows), 1) + (my_c * n_rows).astype(F32)), YN, -1.0
    )
    own_base[0] = near_re * inv_root
    own_base[1] = near_im * inv_root
    for c in col_order[:-1]:
        mark_copy(c, c).wait_recv()
    for f in facet_order[:-1]:
        marks_copy(f, my_f).start()

    for c in col_order[:-1]:
        col_copy(0, strip_out, strip_in, c, c, c).wait_recv()
    strip = strip_in[...]
    if n_rows % 16:
        strip = strip.astype(F32).reshape(YN, 2 * M).astype(BF16)
    else:
        strip = strip.reshape(YN, 2 * M)
    prods = dot(subt[...].reshape(n_facet * 2 * M, YN), strip, NN)
    for s in range(n_facet):
        prod = prods[s * 2 * M : (s + 1) * 2 * M]
        contrib_out[s] = (prod[:M] + minus_plus * swapped(prod[M:])).astype(BF16)
    for s in facet_order[:-1]:
        facet_copy(0, contrib_out, contrib_in, s, my_f, s).start()
    contrib_in[my_f] = contrib_out[my_f]

    for f in facet_order[:-1]:
        marks_copy(f, f).wait_recv()
    sub = lax.broadcasted_iota(jnp.int32, (8, n_vis), 0)
    bits = [lax.rem(sub // (1 << p), 2) == 1 for p in range(3)]
    rows_at = (my_c * n_rows).astype(F32)

    def spread(s, carry):
        for c in range(n_col):
            unit = s * n_col + c
            points[pl.ds(unit, 1)] = marks[s, c, :, :n_vis]
            shifts[pl.ds(unit, 1)] = marks[s, c, :, n_vis:]
        rows = pl.ds(pl.multiple_of(s * n_col, n_col), n_col)
        shift = shifts[rows].astype(F32) * (iota((n_col, wide), 1) + rows_at)
        own_turn[0, rows], own_turn[1, rows] = cis(shift, YN, -1.0)
        packed = points[rows]
        high = packed // 65536
        for which, point in ((0, packed - high * 65536), (1, high)):
            point = point.astype(F32)
            powers[which, 0, 0, rows], powers[which, 0, 1, rows] = cis(
                point * facet_offsets[which, my_f].astype(F32), FINE, -1.0
            )
            value = cis(point, FINE, -1.0)
            for p in range(1, N_POWER):
                powers[which, p, 0, rows], powers[which, p, 1, rows] = value
                if p < N_POWER - 1:
                    value = cmul(value, value)
        return carry

    loop(n_facet, spread)

    def power(which, p, unit):
        return powers[which, p, 0, pl.ds(unit, 1)], powers[which, p, 1, pl.ds(unit, 1)]

    def first(which, unit):
        value = None
        for p in range(3):
            re, im = power(which, 1 + p, unit)
            step = jnp.where(bits[p], re, 1.0), jnp.where(bits[p], im, 0.0)
            value = step if value is None else cmul(value, step)
        return cmul(value, power(which, 0, unit))

    def filled(which, start, unit):
        parts = [start]
        for p in range(4, N_POWER):
            by = power(which, p, unit)
            parts += [cmul(part, by) for part in parts]
        return [jnp.concatenate([part[i] for part in parts], axis=0) for i in range(2)]

    def make_path(c):
        def one(s, carry):
            unit = s * n_col + c
            u_re, u_im = filled(0, first(0, unit), unit)
            u_re, u_im = u_re.astype(BF16), u_im.astype(BF16)
            v_first = first(1, unit)
            firsts[unit, 0], firsts[unit, 1] = v_first
            re = own_turn[0, pl.ds(unit, 1), :n_rows]
            im = own_turn[1, pl.ds(unit, 1), :n_rows]
            e_re, e_im = cmul((own_base[0], own_base[1]), (re, im))
            e_tab = jnp.concatenate([e_re, e_im], axis=0).astype(BF16)
            paths[unit, :n_rows] = dot(e_tab, jnp.concatenate([u_re, u_im], axis=0), TN).astype(BF16)
            paths[unit, room : room + n_rows] = dot(
                e_tab, jnp.concatenate([u_im, -u_re], axis=0), TN
            ).astype(BF16)
            return carry

        loop(n_facet, one)

    near_order = col_order[::-1]
    for c in near_order[:PATHS_BEFORE]:
        make_path(c)

    pred_re = jnp.zeros((M, n_vis), F32)
    pred_im = jnp.zeros((M, n_vis), F32)
    for f in facet_order[:-1]:
        facet_copy(0, contrib_out, contrib_in, f, f, f).wait_recv()
    for f in range(n_facet):
        with_re = dot(contrib_in[f], u_tab[f, :M], TN)
        with_im = dot(contrib_in[f], u_tab[f, M:], TN)
        rows_re = with_re[:M] - with_im[M:]
        rows_im = with_im[:M] + with_re[M:]
        v_re, v_im = v_tab[f, :M], v_tab[f, M:]
        pred_re += rows_re * v_re - rows_im * v_im
        pred_im += rows_re * v_im + rows_im * v_re
    pred_re = jnp.sum(pred_re, axis=0, keepdims=True)
    pred_im = jnp.sum(pred_im, axis=0, keepdims=True)
    predicted[0, 0, pl.ds(0, 1)] = pred_re
    predicted[0, 0, pl.ds(1, 1)] = pred_im
    weight = SUB / math.sqrt(n_vis) / SUB
    weight *= math.sqrt(YN / (M * n_facet)) * math.sqrt(YN / (M * n_col))
    diffs[my_f, my_c] = ((predicted[0, 0] - observed[0, 0]) * weight).astype(diffs.dtype)
    for c in col_order[:-1]:

        def send(i, carry, c=c):
            diff_copy(lax.rem(my_f + i, n_facet), c, my_f, my_c).start()
            return carry

        loop(n_facet, send)
    for f in facet_order[:-1]:
        diff_copy(f, my_c, my_f, my_c).start()

    for c in near_order[PATHS_BEFORE:]:
        make_path(c)

    def gather(place):
        c = near_order[place]

        def one(i, total):
            s = lax.rem(my_f + i, n_facet)
            unit = s * n_col + c
            diff = diffs[s, c].astype(F32)
            diff = diff[:1], diff[1:]
            start = cmul((firsts[unit, 0], firsts[unit, 1]), diff)
            wgt = jnp.concatenate(filled(1, start, unit), axis=0).astype(BF16)
            return total + dot(paths[unit], wgt, NT)

        prod = loop(n_facet, one, jnp.zeros((2 * room, 2 * M), F32))
        re, im = prod[:n_rows], prod[room : room + n_rows]
        at = slice(place * 2 * M, (place + 1) * 2 * M)
        sides[:n_rows, at] = (re + minus_plus * swapped(im)).astype(BF16)
        sides[room : room + n_rows, at] = (im - minus_plus * swapped(re)).astype(BF16)

    def wait_for(place):
        c = near_order[place]
        if place == 0:
            for s in facet_order[:-1]:
                diff_copy(s, c, s, c).wait_recv()
            return

        def wait(s, carry):
            diff_copy(s, c, s, c).wait_recv()
            return carry

        loop(n_facet, wait)

    half = n_col // 2
    for places in (range(half), range(half, n_col)):
        for place in places:
            wait_for(place)
        for place in places:
            gather(place)
        if places[0] == 0:
            partial[...] = dot(sides[:, : half * 2 * M], wall[:half].reshape(half * 2 * M, YN), NN)

    for c in col_order[:-1]:
        col_copy(0, strip_out, strip_in, c, c, c).wait_send()
        mark_copy(c, my_c).wait_send()

        def sent(f, carry, c=c):
            diff_copy(f, c, my_f, my_c).wait_send()
            return carry

        loop(n_facet, sent)
    for f in facet_order[:-1]:
        facet_copy(0, contrib_out, contrib_in, f, f, f).wait_send()
        marks_copy(f, my_f).wait_send()
        diff_copy(f, my_c, my_f, my_c).wait_send()


def finish_kernel(predicted, sides, wall, partial, predicted_hbm, update_hbm, update, sems):
    copies = [pltpu.make_async_copy(predicted, predicted_hbm, sems.at[0])]
    copies[0].start()
    n_rows = update.shape[1]
    room = sides.shape[0] // 2
    depth = sides.shape[1] // 2
    half = wall.shape[0] // 2
    walls = wall[half:].reshape(depth, update.shape[2])
    step = 256
    for i in range(update.shape[2] // step):
        at = slice(i * step, (i + 1) * step)
        prod = dot(sides[:, depth:], walls[:, at], NN) + partial[:, at]
        update[0, :, at] = prod[:n_rows]
        update[1, :, at] = prod[room : room + n_rows]
        copies.append(pltpu.make_async_copy(update.at[:, :, at], update_hbm.at[0, :, :, at], sems.at[1 + i]))
        copies[-1].start()
    for copy in copies:
        copy.wait()


def finish(predicted, sides, wall, partial, facets_shape):
    vmem = pl.BlockSpec(memory_space=pltpu.VMEM)
    hbm = pl.BlockSpec(memory_space=pltpu.HBM)
    return pl.pallas_call(
        finish_kernel,
        out_shape=(
            jax.ShapeDtypeStruct(predicted.shape, F32),
            jax.ShapeDtypeStruct(facets_shape, F32),
        ),
        in_specs=[vmem] * 4,
        out_specs=(hbm, hbm),
        scratch_shapes=[
            pltpu.VMEM(facets_shape[1:], F32),
            pltpu.SemaphoreType.DMA((1 + facets_shape[3] // 256,)),
        ],
        compiler_params=pltpu.CompilerParams(vmem_limit_bytes=2**22),
        name="finish",
    )(predicted, sides, wall, partial)


def body(n_facet, n_col, facets, col_offsets, sub_rows, facet_offsets, vis_pos, observed):
    assert sub_rows.shape[0] == n_facet
    n_rows = facets.shape[2]
    n_vis = vis_pos.shape[3]
    vmem = pl.BlockSpec(memory_space=pltpu.VMEM)
    facet_blocks = pltpu.VMEM((n_facet, M, 2 * M), BF16)
    col_blocks = pltpu.VMEM((n_col, n_rows, 2 * M), BF16)
    table_rows = n_col + n_facet
    room = -(-n_rows // 16) * 16
    wide = -(-n_rows // 128) * 128
    n_units = n_col * n_facet
    sides = (2 * room, n_col * 2 * M)
    wall = (n_col, 2 * M, YN)
    partial = (2 * room, YN)
    held = 4 * (observed.size + math.prod(partial)) + 2 * (math.prod(sides) + math.prod(wall))
    vmem_left = (67043328 - held) // 1024 * 1024 - MARGIN
    results = pl.pallas_call(
            functools.partial(kernel, n_facet, n_col),
            out_shape=(
                pltpu.VMEM(observed.shape, F32),
                pltpu.VMEM(sides, BF16),
                pltpu.VMEM(wall, BF16),
                pltpu.VMEM(partial, F32),
            ),
            in_specs=[pl.BlockSpec(memory_space=pltpu.HBM)] * 6,
            out_specs=(vmem, vmem, vmem, vmem),
            scratch_shapes=[
                pltpu.VMEM((2, n_rows, YN), BF16),
                pltpu.SMEM(col_offsets.shape, jnp.int32),
                pltpu.SMEM(sub_rows.shape[::-1], jnp.int32),
                pltpu.SMEM(facet_offsets.shape[::-1], jnp.int32),
                pltpu.VMEM(vis_pos.shape, jnp.int32),
                pltpu.VMEM(observed.shape, F32),
                pltpu.VMEM((2, M, YN), F32),
                pltpu.VMEM((2, table_rows, YN), F32),
                pltpu.VMEM((n_facet, 2 * M, YN), BF16),
                pltpu.VMEM((n_facet, 2 * M, n_vis), BF16),
                pltpu.VMEM((n_facet, 2 * M, n_vis), F32),
                col_blocks,
                col_blocks,
                facet_blocks,
                facet_blocks,
                pltpu.VMEM((n_facet, n_col, 1, n_vis + wide), jnp.int32),
                pltpu.VMEM((n_units, n_vis), jnp.int32),
                pltpu.VMEM((n_units, wide), jnp.int32),
                pltpu.VMEM((2, N_POWER, 2, n_units, n_vis), F32),
                pltpu.VMEM((n_units, 2, 8, n_vis), F32),
                pltpu.VMEM((2, M, n_rows), F32),
                pltpu.VMEM((2, n_units, wide), F32),
                pltpu.VMEM((n_units, 2 * room, n_vis), BF16),
                pltpu.VMEM((n_facet, n_col, 2, n_vis), BF16),
                pltpu.SemaphoreType.DMA((6,)),
                pltpu.SemaphoreType.DMA((2, n_col)),
                pltpu.SemaphoreType.DMA((2, n_col)),
                pltpu.SemaphoreType.DMA((2, n_facet)),
                pltpu.SemaphoreType.DMA((2, n_facet)),
                pltpu.SemaphoreType.DMA((n_facet, n_col)),
                pltpu.SemaphoreType.DMA((n_facet, n_col)),
            ],
            compiler_params=pltpu.CompilerParams(
                collective_id=0, has_side_effects=True, vmem_limit_bytes=vmem_left
            ),
            name="predict_update",
        )(facets, col_offsets, sub_rows.T, facet_offsets.T, vis_pos, observed)
    return finish(*results, facets.shape)


def solution(mesh):
    in_specs = (
        P("facet", None, "col", None),
        P(),
        P(None, "col"),
        P(),
        P("facet", "col", None, None),
        P("facet", "col", None, None),
    )
    out_specs = (P("facet", "col", None, None), P("facet", None, "col", None))
    step = functools.partial(body, mesh.shape["facet"], mesh.shape["col"])
    return jax.shard_map(step, mesh=mesh, in_specs=in_specs, out_specs=out_specs, check_vma=False)
```

```python
import functools
import math

import jax
import jax.numpy as jnp
from jax import lax
from jax.experimental import pallas as pl
from jax.experimental.pallas import tpu as pltpu
from jax.sharding import PartitionSpec as P

M = 64
SUB = 384
FINE = 1536
YN = 768
MARGIN = 8192
PATHS_BEFORE = 4
MESH = pl.DeviceIdType.MESH
F32 = jnp.float32
BF16 = jnp.bfloat16


def cis(product, modulus, direction):
    turns = jnp.floor(product * (1.0 / modulus) + 0.5)
    half = (product - turns * modulus) * (direction * math.pi / modulus)
    z = half * half
    s = half * (1.0 + z * (-1 / 6 + z * (1 / 120 + z * (-1 / 5040 + z * (1 / 362880 + z * (-1 / 39916800))))))
    c = 1.0 + z * (-1 / 2 + z * (1 / 24 + z * (-1 / 720 + z * (1 / 40320 + z * (-1 / 3628800 + z * (1 / 479001600))))))
    return 1.0 - 2.0 * s * s, 2.0 * s * c


def iota(shape, axis):
    return lax.broadcasted_iota(jnp.int32, shape, axis).astype(F32)


def dot(left, right, dims):
    return lax.dot_general(left, right, (dims, ((), ())), preferred_element_type=F32)


NN = ((1,), (0,))
NT = ((1,), (1,))
TN = ((0,), (0,))
STRIP, MARK, MARKS, CONTRIB, OWN, NEAR, FAR = range(7)
N_POWER = 7


def cmul(a, b):
    return a[0] * b[0] - a[1] * b[1], a[0] * b[1] + a[1] * b[0]


def loop(n, step, carry=()):
    return lax.fori_loop(0, n, step, carry, unroll=n <= 4)


def kernel(
    n_facet,
    n_col,
    facets_hbm,
    col_offsets_hbm,
    sub_rows_hbm,
    facet_offsets_hbm,
    vis_pos_hbm,
    observed_hbm,
    predicted,
    sides,
    wall,
    partial,
    facet_buf,
    col_offsets,
    sub_rows,
    facet_offsets,
    vis_pos,
    observed,
    base,
    turn,
    subt,
    u_tab,
    v_tab,
    strip_out,
    strip_in,
    contrib_out,
    contrib_in,
    marks,
    points,
    shifts,
    powers,
    firsts,
    own_base,
    own_turn,
    paths,
    diffs,
    load_sem,
    send_sem,
    recv_sem,
):
    my_f = lax.axis_index("facet")
    my_c = lax.axis_index("col")
    n_rows = facet_buf.shape[1]
    n_vis = vis_pos.shape[3]
    room = paths.shape[1] // 2

    loads = [
        pltpu.make_async_copy(source, held, load_sem.at[i])
        for i, (source, held) in enumerate(
            (
                (col_offsets_hbm, col_offsets),
                (sub_rows_hbm, sub_rows),
                (facets_hbm.at[0], facet_buf),
                (facet_offsets_hbm, facet_offsets),
                (vis_pos_hbm, vis_pos),
                (observed_hbm, observed),
            )
        )
    ]
    for load in loads:
        load.start()
    barrier = pltpu.get_barrier_semaphore()
    n_pair = n_col // 2
    my_pair, my_core = my_c // 2, lax.rem(my_c, 2)
    side = my_pair // (n_pair // 2)
    mirrored = my_pair + side * (n_pair - 1 - 2 * my_pair)
    pair_order = []
    for place in range(n_pair - 1, 0, -1):
        target = place - (mirrored + n_pair - place) // n_pair
        pair_order.append(target + side * (n_pair - 1 - 2 * target))
    pair_order.append(my_pair)
    col_order = []
    for pair in pair_order:
        col_order += [2 * pair + 1 - my_core, 2 * pair + my_core]
    facet_order = [lax.rem(my_f + 1 + i, n_facet) for i in range(n_facet)]
    for c in col_order[:-1]:
        pl.semaphore_signal(barrier, inc=1, device_id=(my_f, c), device_id_type=MESH)
    for f in facet_order[:-1]:
        pl.semaphore_signal(barrier, inc=1, device_id=(f, my_c), device_id_type=MESH)

    def remote(kind, source, into, f, c):
        return pltpu.make_async_remote_copy(
            src_ref=source,
            dst_ref=into,
            send_sem=send_sem.at[kind],
            recv_sem=recv_sem.at[kind],
            device_id=(f, c),
            device_id_type=MESH,
        )

    def all_of(kind, block):
        return remote(kind, block, block, my_f, my_c)

    strips_all = all_of(STRIP, strip_in.at[: n_col - 1])
    mark_all = all_of(MARK, marks.at[0, : n_col - 1])
    marks_all = all_of(MARKS, marks.at[: n_facet - 1])
    contribs_all = all_of(CONTRIB, contrib_in.at[: n_facet - 1])
    half = n_col // 2
    diffs_own = all_of(OWN, diffs.at[: n_facet - 1, 0])
    diffs_near = all_of(NEAR, diffs.at[:, : half - 1])
    diffs_far = all_of(FAR, diffs.at[:, :half])

    base_re, base_im = cis(iota((M, YN), 0) * iota((M, YN), 1), YN, -1.0)
    inv_root = 1.0 / math.sqrt(YN)
    base[0] = base_re * inv_root
    base[1] = base_im * inv_root
    along = iota((1, YN), 1)
    loads[0].wait()
    loads[1].wait()
    for c in range(n_col):
        turn[0, pl.ds(c, 1)] = along * col_offsets[c].astype(F32)
    for s in range(n_facet):
        turn[0, pl.ds(n_col + s, 1)] = along * sub_rows[0, s].astype(F32)
    turn_re, turn_im = cis(turn[0], YN, -1.0)
    turn[0] = turn_re
    turn[1] = turn_im

    def table(into, row, slot):
        re, im = turn[0, pl.ds(row, 1)], turn[1, pl.ds(row, 1)]
        into[slot, :M] = (base[0] * re - base[1] * im).astype(BF16)
        into[slot, M:] = (base[0] * im + base[1] * re).astype(BF16)

    lane = lax.broadcasted_iota(jnp.int32, (1, 2 * M), 1)
    minus_plus = jnp.where(lane < M, -1.0, 1.0)

    def swapped(value):
        return pltpu.roll(value, M, 1)

    for load in loads[3:]:
        load.wait()
    wide = marks.shape[3] - n_vis
    marks[my_f, my_c, :, :n_vis] = vis_pos[0, 0, :1] + vis_pos[0, 0, 1:] * 65536
    marks[my_f, my_c, :, n_vis:] = jnp.full((1, wide), sub_rows[0, my_f], jnp.int32)

    loads[2].wait()
    both = facet_buf[...]
    if n_rows % 16:
        both = both.astype(F32).reshape(2 * n_rows, YN).astype(BF16)
    else:
        both = both.reshape(2 * n_rows, YN)
    early = n_col - 1
    for i, c in enumerate(col_order):
        place = n_col - 1 - i
        table(wall, c, place)
        prod = dot(both, wall[place], NT)
        part = (prod[:n_rows] + minus_plus * swapped(prod[n_rows:])).astype(BF16)
        if i < n_col - 1:
            strip_out[c] = part
        else:
            strip_in[c] = part
        if i == early - 1:
            pl.semaphore_wait(barrier, n_col - 1 + n_facet - 1)
            for ready in col_order[:-1]:
                remote(MARK, marks.at[my_f, my_c], marks.at[my_f, my_c], my_f, ready).start()
            for ready in col_order[:early]:
                remote(STRIP, strip_out.at[ready], strip_in.at[my_c], my_f, ready).start()
        elif early <= i < n_col - 1:
            remote(STRIP, strip_out.at[c], strip_in.at[my_c], my_f, c).start()

    for s in range(n_facet):
        table(subt, n_col + s, s)
    for tab, which in ((u_tab, 0), (v_tab, 1)):
        point = vis_pos[0, 0, pl.ds(which, 1)].astype(F32)
        low_re, low_im = cis(iota((M, n_vis), 0) * point, FINE, 1.0)
        low_re = low_re * (1.0 / math.sqrt(SUB))
        low_im = low_im * (1.0 / math.sqrt(SUB))
        for f in range(n_facet):
            high_re, high_im = cis(point * facet_offsets[which, f].astype(F32), FINE, 1.0)
            tab[f, :M] = (low_re * high_re - low_im * high_im).astype(tab.dtype)
            tab[f, M:] = (low_re * high_im + low_im * high_re).astype(tab.dtype)
    near_re, near_im = cis(
        iota((M, n_rows), 0) * (iota((M, n_rows), 1) + (my_c * n_rows).astype(F32)), YN, -1.0
    )
    own_base[0] = near_re * inv_root
    own_base[1] = near_im * inv_root
    mark_all.wait_recv()
    for f in facet_order[:-1]:
        remote(MARKS, marks.at[my_f], marks.at[my_f], f, my_c).start()

    strips_all.wait_recv()
    strip = strip_in[...]
    if n_rows % 16:
        strip = strip.astype(F32).reshape(YN, 2 * M).astype(BF16)
    else:
        strip = strip.reshape(YN, 2 * M)
    prods = dot(subt[...].reshape(n_facet * 2 * M, YN), strip, NN)
    for s in range(n_facet):
        prod = prods[s * 2 * M : (s + 1) * 2 * M]
        contrib_out[s] = (prod[:M] + minus_plus * swapped(prod[M:])).astype(BF16)
    for s in facet_order[:-1]:
        remote(CONTRIB, contrib_out.at[s], contrib_in.at[my_f], s, my_c).start()
    contrib_in[my_f] = contrib_out[my_f]

    marks_all.wait_recv()
    sub = lax.broadcasted_iota(jnp.int32, (8, n_vis), 0)
    bits = [lax.rem(sub // (1 << p), 2) == 1 for p in range(3)]
    rows_at = (my_c * n_rows).astype(F32)

    def spread(s, carry):
        for c in range(n_col):
            unit = s * n_col + c
            points[pl.ds(unit, 1)] = marks[s, c, :, :n_vis]
            shifts[pl.ds(unit, 1)] = marks[s, c, :, n_vis:]
        rows = pl.ds(pl.multiple_of(s * n_col, n_col), n_col)
        shift = shifts[rows].astype(F32) * (iota((n_col, wide), 1) + rows_at)
        own_turn[0, rows], own_turn[1, rows] = cis(shift, YN, -1.0)
        packed = points[rows]
        high = packed // 65536
        for which, point in ((0, packed - high * 65536), (1, high)):
            point = point.astype(F32)
            powers[which, 0, 0, rows], powers[which, 0, 1, rows] = cis(
                point * facet_offsets[which, my_f].astype(F32), FINE, -1.0
            )
            value = cis(point, FINE, -1.0)
            for p in range(1, N_POWER):
                powers[which, p, 0, rows], powers[which, p, 1, rows] = value
                if p < N_POWER - 1:
                    value = cmul(value, value)
        return carry

    loop(n_facet, spread)

    def power(which, p, unit):
        return powers[which, p, 0, pl.ds(unit, 1)], powers[which, p, 1, pl.ds(unit, 1)]

    def first(which, unit):
        value = None
        for p in range(3):
            re, im = power(which, 1 + p, unit)
            step = jnp.where(bits[p], re, 1.0), jnp.where(bits[p], im, 0.0)
            value = step if value is None else cmul(value, step)
        return cmul(value, power(which, 0, unit))

    def filled(which, start, unit):
        parts = [start]
        for p in range(4, N_POWER):
            by = power(which, p, unit)
            parts += [cmul(part, by) for part in parts]
        return [jnp.concatenate([part[i] for part in parts], axis=0) for i in range(2)]

    def make_path(c):
        def one(s, carry):
            unit = s * n_col + c
            u_re, u_im = filled(0, first(0, unit), unit)
            u_re, u_im = u_re.astype(BF16), u_im.astype(BF16)
            v_first = first(1, unit)
            firsts[unit, 0], firsts[unit, 1] = v_first
            re = own_turn[0, pl.ds(unit, 1), :n_rows]
            im = own_turn[1, pl.ds(unit, 1), :n_rows]
            e_re, e_im = cmul((own_base[0], own_base[1]), (re, im))
            e_tab = jnp.concatenate([e_re, e_im], axis=0).astype(BF16)
            paths[unit, :n_rows] = dot(e_tab, jnp.concatenate([u_re, u_im], axis=0), TN).astype(BF16)
            paths[unit, room : room + n_rows] = dot(
                e_tab, jnp.concatenate([u_im, -u_re], axis=0), TN
            ).astype(BF16)
            return carry

        loop(n_facet, one)

    near_order = col_order[::-1]
    for c in near_order[:PATHS_BEFORE]:
        make_path(c)

    pred_re = jnp.zeros((M, n_vis), F32)
    pred_im = jnp.zeros((M, n_vis), F32)
    contribs_all.wait_recv()
    for f in range(n_facet):
        with_re = dot(contrib_in[f], u_tab[f, :M], TN)
        with_im = dot(contrib_in[f], u_tab[f, M:], TN)
        rows_re = with_re[:M] - with_im[M:]
        rows_im = with_im[:M] + with_re[M:]
        v_re, v_im = v_tab[f, :M], v_tab[f, M:]
        pred_re += rows_re * v_re - rows_im * v_im
        pred_im += rows_re * v_im + rows_im * v_re
    pred_re = jnp.sum(pred_re, axis=0, keepdims=True)
    pred_im = jnp.sum(pred_im, axis=0, keepdims=True)
    predicted[0, 0, pl.ds(0, 1)] = pred_re
    predicted[0, 0, pl.ds(1, 1)] = pred_im
    weight = SUB / math.sqrt(n_vis) / SUB
    weight *= math.sqrt(YN / (M * n_facet)) * math.sqrt(YN / (M * n_col))
    diffs[my_f, my_c] = ((predicted[0, 0] - observed[0, 0]) * weight).astype(diffs.dtype)
    diff = diffs.at[my_f, my_c]
    for i, c in enumerate(col_order[:-1]):
        kind = FAR if i < half else NEAR

        def send(i, carry, c=c, kind=kind):
            remote(kind, diff, diff, lax.rem(my_f + i, n_facet), c).start()
            return carry

        loop(n_facet, send)
    for f in facet_order[:-1]:
        remote(OWN, diff, diff, f, my_c).start()

    for c in near_order[PATHS_BEFORE:]:
        make_path(c)

    def gather(place):
        c = near_order[place]

        def one(i, total):
            s = lax.rem(my_f + i, n_facet)
            unit = s * n_col + c
            diff = diffs[s, c].astype(F32)
            diff = diff[:1], diff[1:]
            start = cmul((firsts[unit, 0], firsts[unit, 1]), diff)
            wgt = jnp.concatenate(filled(1, start, unit), axis=0).astype(BF16)
            return total + dot(paths[unit], wgt, NT)

        prod = loop(n_facet, one, jnp.zeros((2 * room, 2 * M), F32))
        re, im = prod[:n_rows], prod[room : room + n_rows]
        at = slice(place * 2 * M, (place + 1) * 2 * M)
        sides[:n_rows, at] = (re + minus_plus * swapped(im)).astype(BF16)
        sides[room : room + n_rows, at] = (im - minus_plus * swapped(re)).astype(BF16)

    diffs_own.wait_recv()
    diffs_near.wait_recv()
    for place in range(half):
        gather(place)
    partial[...] = dot(sides[:, : half * 2 * M], wall[:half].reshape(half * 2 * M, YN), NN)
    diffs_far.wait_recv()
    for place in range(half, n_col):
        gather(place)

    for sent in (strips_all, mark_all, marks_all, contribs_all, diffs_own, diffs_near, diffs_far):
        sent.wait_send()


def finish_kernel(predicted, sides, wall, partial, predicted_hbm, update_hbm, update, sems):
    copies = [pltpu.make_async_copy(predicted, predicted_hbm, sems.at[0])]
    copies[0].start()
    n_rows = update.shape[1]
    room = sides.shape[0] // 2
    depth = sides.shape[1] // 2
    half = wall.shape[0] // 2
    walls = wall[half:].reshape(depth, update.shape[2])
    step = 256
    for i in range(update.shape[2] // step):
        at = slice(i * step, (i + 1) * step)
        prod = dot(sides[:, depth:], walls[:, at], NN) + partial[:, at]
        update[0, :, at] = prod[:n_rows]
        update[1, :, at] = prod[room : room + n_rows]
        copies.append(pltpu.make_async_copy(update.at[:, :, at], update_hbm.at[0, :, :, at], sems.at[1 + i]))
        copies[-1].start()
    for copy in copies:
        copy.wait()


def finish(predicted, sides, wall, partial, facets_shape):
    vmem = pl.BlockSpec(memory_space=pltpu.VMEM)
    hbm = pl.BlockSpec(memory_space=pltpu.HBM)
    return pl.pallas_call(
        finish_kernel,
        out_shape=(
            jax.ShapeDtypeStruct(predicted.shape, F32),
            jax.ShapeDtypeStruct(facets_shape, F32),
        ),
        in_specs=[vmem] * 4,
        out_specs=(hbm, hbm),
        scratch_shapes=[
            pltpu.VMEM(facets_shape[1:], F32),
            pltpu.SemaphoreType.DMA((1 + facets_shape[3] // 256,)),
        ],
        compiler_params=pltpu.CompilerParams(vmem_limit_bytes=2**22),
        name="finish",
    )(predicted, sides, wall, partial)


def body(n_facet, n_col, facets, col_offsets, sub_rows, facet_offsets, vis_pos, observed):
    assert sub_rows.shape[0] == n_facet
    n_rows = facets.shape[2]
    n_vis = vis_pos.shape[3]
    vmem = pl.BlockSpec(memory_space=pltpu.VMEM)
    facet_blocks = pltpu.VMEM((n_facet, M, 2 * M), BF16)
    col_blocks = pltpu.VMEM((n_col, n_rows, 2 * M), BF16)
    table_rows = n_col + n_facet
    room = -(-n_rows // 16) * 16
    wide = -(-n_rows // 128) * 128
    n_units = n_col * n_facet
    sides = (2 * room, n_col * 2 * M)
    wall = (n_col, 2 * M, YN)
    partial = (2 * room, YN)
    held = 4 * (observed.size + math.prod(partial)) + 2 * (math.prod(sides) + math.prod(wall))
    vmem_left = (67043328 - held) // 1024 * 1024 - MARGIN
    results = pl.pallas_call(
            functools.partial(kernel, n_facet, n_col),
            out_shape=(
                pltpu.VMEM(observed.shape, F32),
                pltpu.VMEM(sides, BF16),
                pltpu.VMEM(wall, BF16),
                pltpu.VMEM(partial, F32),
            ),
            in_specs=[pl.BlockSpec(memory_space=pltpu.HBM)] * 6,
            out_specs=(vmem, vmem, vmem, vmem),
            scratch_shapes=[
                pltpu.VMEM((2, n_rows, YN), BF16),
                pltpu.SMEM(col_offsets.shape, jnp.int32),
                pltpu.SMEM(sub_rows.shape[::-1], jnp.int32),
                pltpu.SMEM(facet_offsets.shape[::-1], jnp.int32),
                pltpu.VMEM(vis_pos.shape, jnp.int32),
                pltpu.VMEM(observed.shape, F32),
                pltpu.VMEM((2, M, YN), F32),
                pltpu.VMEM((2, table_rows, YN), F32),
                pltpu.VMEM((n_facet, 2 * M, YN), BF16),
                pltpu.VMEM((n_facet, 2 * M, n_vis), BF16),
                pltpu.VMEM((n_facet, 2 * M, n_vis), F32),
                col_blocks,
                col_blocks,
                facet_blocks,
                facet_blocks,
                pltpu.VMEM((n_facet, n_col, 1, n_vis + wide), jnp.int32),
                pltpu.VMEM((n_units, n_vis), jnp.int32),
                pltpu.VMEM((n_units, wide), jnp.int32),
                pltpu.VMEM((2, N_POWER, 2, n_units, n_vis), F32),
                pltpu.VMEM((n_units, 2, 8, n_vis), F32),
                pltpu.VMEM((2, M, n_rows), F32),
                pltpu.VMEM((2, n_units, wide), F32),
                pltpu.VMEM((n_units, 2 * room, n_vis), BF16),
                pltpu.VMEM((n_facet, n_col, 2, n_vis), BF16),
                pltpu.SemaphoreType.DMA((6,)),
                pltpu.SemaphoreType.DMA((7,)),
                pltpu.SemaphoreType.DMA((7,)),
            ],
            compiler_params=pltpu.CompilerParams(
                collective_id=0, has_side_effects=True, vmem_limit_bytes=vmem_left
            ),
            name="predict_update",
        )(facets, col_offsets, sub_rows.T, facet_offsets.T, vis_pos, observed)
    return finish(*results, facets.shape)


def solution(mesh):
    in_specs = (
        P("facet", None, "col", None),
        P(),
        P(None, "col"),
        P(),
        P("facet", "col", None, None),
        P("facet", "col", None, None),
    )
    out_specs = (P("facet", "col", None, None), P("facet", None, "col", None))
    step = functools.partial(body, mesh.shape["facet"], mesh.shape["col"])
    return jax.shard_map(step, mesh=mesh, in_specs=in_specs, out_specs=out_specs, check_vma=False)
```

```python
import functools
import math

import jax
import jax.numpy as jnp
from jax import lax
from jax.experimental import pallas as pl
from jax.experimental.pallas import tpu as pltpu
from jax.sharding import PartitionSpec as P

M = 64
SUB = 384
FINE = 1536
YN = 768
MARGIN = 8192
MESH = pl.DeviceIdType.MESH
F32 = jnp.float32
BF16 = jnp.bfloat16


def cis(product, modulus, direction):
    turns = jnp.floor(product * (1.0 / modulus) + 0.5)
    half = (product - turns * modulus) * (direction * math.pi / modulus)
    z = half * half
    s = half * (1.0 + z * (-1 / 6 + z * (1 / 120 + z * (-1 / 5040 + z * (1 / 362880 + z * (-1 / 39916800))))))
    c = 1.0 + z * (-1 / 2 + z * (1 / 24 + z * (-1 / 720 + z * (1 / 40320 + z * (-1 / 3628800 + z * (1 / 479001600))))))
    return 1.0 - 2.0 * s * s, 2.0 * s * c


def iota(shape, axis):
    return lax.broadcasted_iota(jnp.int32, shape, axis).astype(F32)


def dot(left, right, dims):
    return lax.dot_general(left, right, (dims, ((), ())), preferred_element_type=F32)


NN = ((1,), (0,))
NT = ((1,), (1,))
TN = ((0,), (0,))
STRIP, MARK, MARKS, PEER, MEASURED, SEEN, NEAR, FAR = range(8)
N_POWER = 7


def cmul(a, b):
    return a[0] * b[0] - a[1] * b[1], a[0] * b[1] + a[1] * b[0]


def loop(n, step, carry=()):
    return lax.fori_loop(0, n, step, carry, unroll=n <= 4)


def kernel(
    n_facet,
    n_col,
    facets_hbm,
    col_offsets_hbm,
    sub_rows_hbm,
    facet_offsets_hbm,
    vis_pos_hbm,
    observed_hbm,
    predicted,
    sides,
    wall,
    partial,
    facet_buf,
    col_offsets,
    sub_rows,
    facet_offsets,
    vis_pos,
    observed,
    base,
    turn,
    subt,
    u_tab,
    v_tab,
    strip_out,
    strip_in,
    seen_out,
    seen_in,
    peers,
    measured,
    marks,
    points,
    shifts,
    powers,
    firsts,
    own_base,
    own_turn,
    paths,
    diffs,
    load_sem,
    send_sem,
    recv_sem,
):
    my_f = lax.axis_index("facet")
    my_c = lax.axis_index("col")
    n_rows = facet_buf.shape[1]
    n_vis = vis_pos.shape[3]
    room = paths.shape[1] // 2

    loads = [
        pltpu.make_async_copy(source, held, load_sem.at[i])
        for i, (source, held) in enumerate(
            (
                (col_offsets_hbm, col_offsets),
                (sub_rows_hbm, sub_rows),
                (facets_hbm.at[0], facet_buf),
                (facet_offsets_hbm, facet_offsets),
                (vis_pos_hbm, vis_pos),
                (observed_hbm, observed),
            )
        )
    ]
    for load in loads:
        load.start()
    barrier = pltpu.get_barrier_semaphore()
    n_pair = n_col // 2
    my_pair, my_core = my_c // 2, lax.rem(my_c, 2)
    side = my_pair // (n_pair // 2)
    mirrored = my_pair + side * (n_pair - 1 - 2 * my_pair)
    pair_order = []
    for place in range(n_pair - 1, 0, -1):
        target = place - (mirrored + n_pair - place) // n_pair
        pair_order.append(target + side * (n_pair - 1 - 2 * target))
    pair_order.append(my_pair)
    col_order = []
    for pair in pair_order:
        col_order += [2 * pair + 1 - my_core, 2 * pair + my_core]
    bits = n_facet.bit_length() - 1
    assert n_facet == 1 << bits
    facet_order = []
    for i in range(n_facet - 1, -1, -1):
        turns = [(i >> b & 1) * (1 << b) * (1 - 2 * lax.rem(my_f // (1 << b), 2)) for b in range(bits)]
        facet_order.append(my_f + sum(turns))
    for c in col_order[:-1]:
        pl.semaphore_signal(barrier, inc=1, device_id=(my_f, c), device_id_type=MESH)
    for f in facet_order[:-1]:
        pl.semaphore_signal(barrier, inc=1, device_id=(f, my_c), device_id_type=MESH)

    def remote(kind, source, into, f, c):
        return pltpu.make_async_remote_copy(
            src_ref=source,
            dst_ref=into,
            send_sem=send_sem.at[kind],
            recv_sem=recv_sem.at[kind],
            device_id=(f, c),
            device_id_type=MESH,
        )

    def all_of(kind, block):
        return remote(kind, block, block, my_f, my_c)

    strips_all = all_of(STRIP, strip_in.at[: n_col - 1])
    mark_all = all_of(MARK, marks.at[0, : n_col - 1])
    marks_all = all_of(MARKS, marks.at[: n_facet - 1])
    peers_all = all_of(PEER, peers.at[: n_facet - 1])
    seen_all = all_of(SEEN, seen_in.at[: n_facet - 1])
    half = n_col // 2
    measured_all = all_of(MEASURED, measured.at[: n_facet - 1])
    diffs_near = all_of(NEAR, diffs.at[: half - 1])
    diffs_far = all_of(FAR, diffs.at[:half])

    base_re, base_im = cis(iota((M, YN), 0) * iota((M, YN), 1), YN, -1.0)
    inv_root = 1.0 / math.sqrt(YN)
    base[0] = base_re * inv_root
    base[1] = base_im * inv_root
    along = iota((1, YN), 1)
    loads[0].wait()
    loads[1].wait()
    for c in range(n_col):
        turn[0, pl.ds(c, 1)] = along * col_offsets[c].astype(F32)
    for s in range(n_facet):
        turn[0, pl.ds(n_col + s, 1)] = along * sub_rows[0, s].astype(F32)
    turn_re, turn_im = cis(turn[0], YN, -1.0)
    turn[0] = turn_re
    turn[1] = turn_im

    def table(into, row, slot):
        re, im = turn[0, pl.ds(row, 1)], turn[1, pl.ds(row, 1)]
        into[slot, :M] = (base[0] * re - base[1] * im).astype(BF16)
        into[slot, M:] = (base[0] * im + base[1] * re).astype(BF16)

    lane = lax.broadcasted_iota(jnp.int32, (1, 2 * M), 1)
    minus_plus = jnp.where(lane < M, -1.0, 1.0)

    def swapped(value):
        return pltpu.roll(value, M, 1)

    for load in loads[3:]:
        load.wait()
    wide = marks.shape[3] - n_vis
    own_points = vis_pos[0, 0, :1] + vis_pos[0, 0, 1:] * 65536
    peers[my_f] = own_points
    measured[my_f] = observed[0, 0]
    marks[my_f, my_c, :, :n_vis] = own_points
    marks[my_f, my_c, :, n_vis:] = jnp.full((1, wide), sub_rows[0, my_f], jnp.int32)

    loads[2].wait()
    both = facet_buf[...]
    if n_rows % 16:
        both = both.astype(F32).reshape(2 * n_rows, YN).astype(BF16)
    else:
        both = both.reshape(2 * n_rows, YN)
    early = 2
    for i, c in enumerate(col_order):
        place = n_col - 1 - i
        table(wall, c, place)
        prod = dot(both, wall[place], NT)
        part = (prod[:n_rows] + minus_plus * swapped(prod[n_rows:])).astype(BF16)
        if i < n_col - 1:
            strip_out[c] = part
        else:
            strip_in[c] = part
        if i == early - 1:
            pl.semaphore_wait(barrier, n_col - 1 + n_facet - 1)
            for ready in col_order[:-1]:
                remote(MARK, marks.at[my_f, my_c], marks.at[my_f, my_c], my_f, ready).start()
            for f in facet_order[:-1]:
                remote(PEER, peers.at[my_f], peers.at[my_f], f, my_c).start()
                remote(MEASURED, measured.at[my_f], measured.at[my_f], f, my_c).start()
            for ready in col_order[:early]:
                remote(STRIP, strip_out.at[ready], strip_in.at[my_c], my_f, ready).start()
        elif early <= i < n_col - 1:
            remote(STRIP, strip_out.at[c], strip_in.at[my_c], my_f, c).start()

    for s in range(n_facet):
        table(subt, n_col + s, s)
    near_re, near_im = cis(
        iota((M, n_rows), 0) * (iota((M, n_rows), 1) + (my_c * n_rows).astype(F32)), YN, -1.0
    )
    own_base[0] = near_re * inv_root
    own_base[1] = near_im * inv_root
    def unpack(packed):
        high = packed // 65536
        return packed - high * 65536, high

    peers_all.wait_recv()

    def make_tables(s, carry):
        for tab, which, point in zip((u_tab, v_tab), range(2), unpack(peers[s])):
            at = iota((M, n_vis), 0) + facet_offsets[which, my_f].astype(F32)
            re, im = cis(at * point.astype(F32), FINE, 1.0)
            tab[s, :M] = (re * (1.0 / math.sqrt(SUB))).astype(tab.dtype)
            tab[s, M:] = (im * (1.0 / math.sqrt(SUB))).astype(tab.dtype)
        return carry

    loop(n_facet, make_tables)
    mark_all.wait_recv()
    for f in facet_order[:-1]:
        remote(MARKS, marks.at[my_f], marks.at[my_f], f, my_c).start()

    strips_all.wait_recv()
    strip = strip_in[...]
    if n_rows % 16:
        strip = strip.astype(F32).reshape(YN, 2 * M).astype(BF16)
    else:
        strip = strip.reshape(YN, 2 * M)
    prods = dot(subt[...].reshape(n_facet * 2 * M, YN), strip, NN)
    for s in range(n_facet):
        prod = prods[s * 2 * M : (s + 1) * 2 * M]
        part = (prod[:M] + minus_plus * swapped(prod[M:])).astype(BF16)
        with_re = dot(part, u_tab[s, :M], TN)
        with_im = dot(part, u_tab[s, M:], TN)
        rows_re = with_re[:M] - with_im[M:]
        rows_im = with_im[:M] + with_re[M:]
        v_re, v_im = v_tab[s, :M], v_tab[s, M:]
        seen_out[s, :1] = jnp.sum(rows_re * v_re - rows_im * v_im, axis=0, keepdims=True)
        seen_out[s, 1:] = jnp.sum(rows_re * v_im + rows_im * v_re, axis=0, keepdims=True)
    for f in facet_order[:-1]:
        remote(SEEN, seen_out, seen_in.at[my_f], f, my_c).start()
    seen_in[my_f] = seen_out[...]

    marks_all.wait_recv()
    sub = lax.broadcasted_iota(jnp.int32, (8, n_vis), 0)
    odd = [lax.rem(sub // (1 << p), 2) == 1 for p in range(3)]
    rows_at = (my_c * n_rows).astype(F32)

    def spread(s, carry):
        for c in range(n_col):
            unit = s * n_col + c
            points[pl.ds(unit, 1)] = marks[s, c, :, :n_vis]
            shifts[pl.ds(unit, 1)] = marks[s, c, :, n_vis:]
        rows = pl.ds(pl.multiple_of(s * n_col, n_col), n_col)
        shift = shifts[rows].astype(F32) * (iota((n_col, wide), 1) + rows_at)
        own_turn[0, rows], own_turn[1, rows] = cis(shift, YN, -1.0)
        packed = points[rows]
        for which, point in enumerate(unpack(packed)):
            point = point.astype(F32)
            powers[which, 0, 0, rows], powers[which, 0, 1, rows] = cis(
                point * facet_offsets[which, my_f].astype(F32), FINE, -1.0
            )
            value = cis(point, FINE, -1.0)
            for p in range(1, N_POWER):
                powers[which, p, 0, rows], powers[which, p, 1, rows] = value
                if p < N_POWER - 1:
                    value = cmul(value, value)
        return carry

    loop(n_facet, spread)

    def power(which, p, unit):
        return powers[which, p, 0, pl.ds(unit, 1)], powers[which, p, 1, pl.ds(unit, 1)]

    def first(which, unit):
        value = None
        for p in range(3):
            re, im = power(which, 1 + p, unit)
            step = jnp.where(odd[p], re, 1.0), jnp.where(odd[p], im, 0.0)
            value = step if value is None else cmul(value, step)
        return cmul(value, power(which, 0, unit))

    def filled(which, start, unit):
        parts = [start]
        for p in range(4, N_POWER):
            by = power(which, p, unit)
            parts += [cmul(part, by) for part in parts]
        return [jnp.concatenate([part[i] for part in parts], axis=0) for i in range(2)]

    def make_path(c):
        def one(s, carry):
            unit = s * n_col + c
            u_re, u_im = filled(0, first(0, unit), unit)
            u_re, u_im = u_re.astype(BF16), u_im.astype(BF16)
            v_first = first(1, unit)
            firsts[unit, 0], firsts[unit, 1] = v_first
            re = own_turn[0, pl.ds(unit, 1), :n_rows]
            im = own_turn[1, pl.ds(unit, 1), :n_rows]
            e_re, e_im = cmul((own_base[0], own_base[1]), (re, im))
            e_tab = jnp.concatenate([e_re, e_im], axis=0).astype(BF16)
            paths[unit, :n_rows] = dot(e_tab, jnp.concatenate([u_re, u_im], axis=0), TN).astype(BF16)
            paths[unit, room : room + n_rows] = dot(
                e_tab, jnp.concatenate([u_im, -u_re], axis=0), TN
            ).astype(BF16)
            return carry

        loop(n_facet, one)

    near_order = col_order[::-1]
    for c in near_order[:6]:
        make_path(c)

    seen_all.wait_recv()
    measured_all.wait_recv()
    weight = SUB / math.sqrt(n_vis) / SUB
    weight *= math.sqrt(YN / (M * n_facet)) * math.sqrt(YN / (M * n_col))
    pred = seen_in[0]
    for f in range(1, n_facet):
        pred += seen_in[f]
    diffs[my_c] = ((pred - measured[...]) * weight).astype(diffs.dtype)
    for i, c in enumerate(col_order[:-1]):
        remote(FAR if i < half else NEAR, diffs.at[my_c], diffs.at[my_c], my_f, c).start()
    mine = seen_in[0, my_f]
    for f in range(1, n_facet):
        mine += seen_in[f, my_f]
    predicted[0, 0] = mine

    for c in near_order[6:]:
        make_path(c)

    def gather(place):
        c = near_order[place]

        def one(i, total):
            s = lax.rem(my_f + i, n_facet)
            unit = s * n_col + c
            diff = diffs[c, s].astype(F32)
            diff = diff[:1], diff[1:]
            start = cmul((firsts[unit, 0], firsts[unit, 1]), diff)
            wgt = jnp.concatenate(filled(1, start, unit), axis=0).astype(BF16)
            return total + dot(paths[unit], wgt, NT)

        prod = loop(n_facet, one, jnp.zeros((2 * room, 2 * M), F32))
        re, im = prod[:n_rows], prod[room : room + n_rows]
        at = slice(place * 2 * M, (place + 1) * 2 * M)
        sides[:n_rows, at] = (re + minus_plus * swapped(im)).astype(BF16)
        sides[room : room + n_rows, at] = (im - minus_plus * swapped(re)).astype(BF16)

    diffs_near.wait_recv()
    for place in range(half):
        gather(place)
    partial[...] = dot(sides[:, : half * 2 * M], wall[:half].reshape(half * 2 * M, YN), NN)
    diffs_far.wait_recv()
    for place in range(half, n_col):
        gather(place)

    for sent in (strips_all, mark_all, marks_all, peers_all, measured_all, seen_all, diffs_near, diffs_far):
        sent.wait_send()


def finish_kernel(predicted, sides, wall, partial, predicted_hbm, update_hbm, update, sems):
    copies = [pltpu.make_async_copy(predicted, predicted_hbm, sems.at[0])]
    copies[0].start()
    n_rows = update.shape[1]
    room = sides.shape[0] // 2
    depth = sides.shape[1] // 2
    half = wall.shape[0] // 2
    walls = wall[half:].reshape(depth, update.shape[2])
    step = 256
    for i in range(update.shape[2] // step):
        at = slice(i * step, (i + 1) * step)
        prod = dot(sides[:, depth:], walls[:, at], NN) + partial[:, at]
        update[0, :, at] = prod[:n_rows]
        update[1, :, at] = prod[room : room + n_rows]
        copies.append(pltpu.make_async_copy(update.at[:, :, at], update_hbm.at[0, :, :, at], sems.at[1 + i]))
        copies[-1].start()
    for copy in copies:
        copy.wait()


def finish(predicted, sides, wall, partial, facets_shape):
    vmem = pl.BlockSpec(memory_space=pltpu.VMEM)
    hbm = pl.BlockSpec(memory_space=pltpu.HBM)
    return pl.pallas_call(
        finish_kernel,
        out_shape=(
            jax.ShapeDtypeStruct(predicted.shape, F32),
            jax.ShapeDtypeStruct(facets_shape, F32),
        ),
        in_specs=[vmem] * 4,
        out_specs=(hbm, hbm),
        scratch_shapes=[
            pltpu.VMEM(facets_shape[1:], F32),
            pltpu.SemaphoreType.DMA((1 + facets_shape[3] // 256,)),
        ],
        compiler_params=pltpu.CompilerParams(vmem_limit_bytes=2**22),
        name="finish",
    )(predicted, sides, wall, partial)


def body(n_facet, n_col, facets, col_offsets, sub_rows, facet_offsets, vis_pos, observed):
    assert sub_rows.shape[0] == n_facet
    n_rows = facets.shape[2]
    n_vis = vis_pos.shape[3]
    vmem = pl.BlockSpec(memory_space=pltpu.VMEM)
    col_blocks = pltpu.VMEM((n_col, n_rows, 2 * M), BF16)
    table_rows = n_col + n_facet
    room = -(-n_rows // 16) * 16
    wide = -(-n_rows // 128) * 128
    n_units = n_col * n_facet
    sides = (2 * room, n_col * 2 * M)
    wall = (n_col, 2 * M, YN)
    partial = (2 * room, YN)
    held = 4 * (observed.size + math.prod(partial)) + 2 * (math.prod(sides) + math.prod(wall))
    vmem_left = (67043328 - held) // 1024 * 1024 - MARGIN
    results = pl.pallas_call(
            functools.partial(kernel, n_facet, n_col),
            out_shape=(
                pltpu.VMEM(observed.shape, F32),
                pltpu.VMEM(sides, BF16),
                pltpu.VMEM(wall, BF16),
                pltpu.VMEM(partial, F32),
            ),
            in_specs=[pl.BlockSpec(memory_space=pltpu.HBM)] * 6,
            out_specs=(vmem, vmem, vmem, vmem),
            scratch_shapes=[
                pltpu.VMEM((2, n_rows, YN), BF16),
                pltpu.SMEM(col_offsets.shape, jnp.int32),
                pltpu.SMEM(sub_rows.shape[::-1], jnp.int32),
                pltpu.SMEM(facet_offsets.shape[::-1], jnp.int32),
                pltpu.VMEM(vis_pos.shape, jnp.int32),
                pltpu.VMEM(observed.shape, F32),
                pltpu.VMEM((2, M, YN), F32),
                pltpu.VMEM((2, table_rows, YN), F32),
                pltpu.VMEM((n_facet, 2 * M, YN), BF16),
                pltpu.VMEM((n_facet, 2 * M, n_vis), BF16),
                pltpu.VMEM((n_facet, 2 * M, n_vis), F32),
                col_blocks,
                col_blocks,
                pltpu.VMEM((n_facet, 2, n_vis), F32),
                pltpu.VMEM((n_facet, n_facet, 2, n_vis), F32),
                pltpu.VMEM((n_facet, 1, n_vis), jnp.int32),
                pltpu.VMEM((n_facet, 2, n_vis), F32),
                pltpu.VMEM((n_facet, n_col, 1, n_vis + wide), jnp.int32),
                pltpu.VMEM((n_units, n_vis), jnp.int32),
                pltpu.VMEM((n_units, wide), jnp.int32),
                pltpu.VMEM((2, N_POWER, 2, n_units, n_vis), F32),
                pltpu.VMEM((n_units, 2, 8, n_vis), F32),
                pltpu.VMEM((2, M, n_rows), F32),
                pltpu.VMEM((2, n_units, wide), F32),
                pltpu.VMEM((n_units, 2 * room, n_vis), BF16),
                pltpu.VMEM((n_col, n_facet, 2, n_vis), BF16),
                pltpu.SemaphoreType.DMA((6,)),
                pltpu.SemaphoreType.DMA((8,)),
                pltpu.SemaphoreType.DMA((8,)),
            ],
            compiler_params=pltpu.CompilerParams(
                collective_id=0, has_side_effects=True, vmem_limit_bytes=vmem_left
            ),
            name="predict_update",
        )(facets, col_offsets, sub_rows.T, facet_offsets.T, vis_pos, observed)
    return finish(*results, facets.shape)


def solution(mesh):
    in_specs = (
        P("facet", None, "col", None),
        P(),
        P(None, "col"),
        P(),
        P("facet", "col", None, None),
        P("facet", "col", None, None),
    )
    out_specs = (P("facet", "col", None, None), P("facet", None, "col", None))
    step = functools.partial(body, mesh.shape["facet"], mesh.shape["col"])
    return jax.shard_map(step, mesh=mesh, in_specs=in_specs, out_specs=out_specs, check_vma=False)
```

```python
import functools
import math

import jax
import jax.numpy as jnp
from jax import lax
from jax.experimental import pallas as pl
from jax.experimental.pallas import tpu as pltpu
from jax.sharding import PartitionSpec as P

M = 64
SUB = 384
FINE = 1536
YN = 768
MARGIN = 8192
MESH = pl.DeviceIdType.MESH
F32 = jnp.float32
BF16 = jnp.bfloat16


def cis(product, modulus, direction):
    turns = jnp.floor(product * (1.0 / modulus) + 0.5)
    half = (product - turns * modulus) * (direction * math.pi / modulus)
    z = half * half
    s = half * (1.0 + z * (-1 / 6 + z * (1 / 120 + z * (-1 / 5040 + z * (1 / 362880 + z * (-1 / 39916800))))))
    c = 1.0 + z * (-1 / 2 + z * (1 / 24 + z * (-1 / 720 + z * (1 / 40320 + z * (-1 / 3628800 + z * (1 / 479001600))))))
    return 1.0 - 2.0 * s * s, 2.0 * s * c


def iota(shape, axis):
    return lax.broadcasted_iota(jnp.int32, shape, axis).astype(F32)


def dot(left, right, dims):
    return lax.dot_general(left, right, (dims, ((), ())), preferred_element_type=F32)


NN = ((1,), (0,))
NT = ((1,), (1,))
TN = ((0,), (0,))
STRIP, MARK, MARKS, PEER, MEASURED, SEEN, NEAR, FAR, ANSWER = range(9)
N_POWER = 7


def cmul(a, b):
    return a[0] * b[0] - a[1] * b[1], a[0] * b[1] + a[1] * b[0]


def loop(n, step, carry=()):
    return lax.fori_loop(0, n, step, carry, unroll=n <= 4)


def kernel(
    n_facet,
    n_col,
    facets_hbm,
    col_offsets_hbm,
    sub_rows_hbm,
    facet_offsets_hbm,
    vis_pos_hbm,
    observed_hbm,
    predicted,
    sides,
    wall,
    partial,
    facet_buf,
    col_offsets,
    sub_rows,
    facet_offsets,
    vis_pos,
    observed,
    base,
    turn,
    subt,
    u_tab,
    v_tab,
    strip_out,
    strip_in,
    seen_out,
    seen_in,
    peers,
    measured,
    answer,
    marks,
    points,
    shifts,
    powers,
    firsts,
    own_base,
    own_turn,
    paths,
    diffs,
    load_sem,
    send_sem,
    recv_sem,
):
    my_f = lax.axis_index("facet")
    my_c = lax.axis_index("col")
    n_rows = facet_buf.shape[1]
    n_vis = vis_pos.shape[3]
    room = paths.shape[1] // 2

    loads = [
        pltpu.make_async_copy(source, held, load_sem.at[i])
        for i, (source, held) in enumerate(
            (
                (col_offsets_hbm, col_offsets),
                (sub_rows_hbm, sub_rows),
                (facets_hbm.at[0], facet_buf),
                (facet_offsets_hbm, facet_offsets),
                (vis_pos_hbm, vis_pos),
                (observed_hbm, observed),
            )
        )
    ]
    for load in loads:
        load.start()
    barrier = pltpu.get_barrier_semaphore()
    n_pair = n_col // 2
    my_pair, my_core = my_c // 2, lax.rem(my_c, 2)
    side = my_pair // (n_pair // 2)
    mirrored = my_pair + side * (n_pair - 1 - 2 * my_pair)
    pair_order = []
    for place in range(n_pair - 1, 0, -1):
        target = place - (mirrored + n_pair - place) // n_pair
        pair_order.append(target + side * (n_pair - 1 - 2 * target))
    pair_order.append(my_pair)
    col_order = []
    for pair in pair_order:
        col_order += [2 * pair + 1 - my_core, 2 * pair + my_core]
    bits = n_facet.bit_length() - 1
    assert n_facet == 1 << bits
    facet_order = []
    for i in range(n_facet - 1, -1, -1):
        turns = [(i >> b & 1) * (1 << b) * (1 - 2 * lax.rem(my_f // (1 << b), 2)) for b in range(bits)]
        facet_order.append(my_f + sum(turns))
    for c in col_order[:-1]:
        pl.semaphore_signal(barrier, inc=1, device_id=(my_f, c), device_id_type=MESH)
    for f in facet_order[:-1]:
        pl.semaphore_signal(barrier, inc=1, device_id=(f, my_c), device_id_type=MESH)

    def remote(kind, source, into, f, c):
        return pltpu.make_async_remote_copy(
            src_ref=source,
            dst_ref=into,
            send_sem=send_sem.at[kind],
            recv_sem=recv_sem.at[kind],
            device_id=(f, c),
            device_id_type=MESH,
        )

    def all_of(kind, block):
        return remote(kind, block, block, my_f, my_c)

    strips_all = all_of(STRIP, strip_in.at[: n_col - 1])
    mark_all = all_of(MARK, marks.at[0, : n_col - 1])
    marks_all = all_of(MARKS, marks.at[: n_facet - 1])
    peers_all = all_of(PEER, peers.at[: n_facet - 1])
    gate = 2 * my_pair + 1
    at_gate = my_core == 1
    seat = my_core * n_facet + my_f
    half = n_col // 2
    diffs_far = all_of(FAR, diffs.at[:half])

    base_re, base_im = cis(iota((M, YN), 0) * iota((M, YN), 1), YN, -1.0)
    inv_root = 1.0 / math.sqrt(YN)
    base[0] = base_re * inv_root
    base[1] = base_im * inv_root
    along = iota((1, YN), 1)
    loads[0].wait()
    loads[1].wait()
    for c in range(n_col):
        turn[0, pl.ds(c, 1)] = along * col_offsets[c].astype(F32)
    for s in range(n_facet):
        turn[0, pl.ds(n_col + s, 1)] = along * sub_rows[0, s].astype(F32)
    turn_re, turn_im = cis(turn[0], YN, -1.0)
    turn[0] = turn_re
    turn[1] = turn_im

    def table(into, row, slot):
        re, im = turn[0, pl.ds(row, 1)], turn[1, pl.ds(row, 1)]
        into[slot, :M] = (base[0] * re - base[1] * im).astype(BF16)
        into[slot, M:] = (base[0] * im + base[1] * re).astype(BF16)

    lane = lax.broadcasted_iota(jnp.int32, (1, 2 * M), 1)
    minus_plus = jnp.where(lane < M, -1.0, 1.0)

    def swapped(value):
        return pltpu.roll(value, M, 1)

    for load in loads[3:]:
        load.wait()
    wide = marks.shape[3] - n_vis
    own_points = vis_pos[0, 0, :1] + vis_pos[0, 0, 1:] * 65536
    peers[my_f] = own_points
    measured[seat] = observed[0, 0]
    marks[my_f, my_c, :, :n_vis] = own_points
    marks[my_f, my_c, :, n_vis:] = jnp.full((1, wide), sub_rows[0, my_f], jnp.int32)

    loads[2].wait()
    both = facet_buf[...]
    if n_rows % 16:
        both = both.astype(F32).reshape(2 * n_rows, YN).astype(BF16)
    else:
        both = both.reshape(2 * n_rows, YN)
    early = 2
    for i, c in enumerate(col_order):
        place = n_col - 1 - i
        table(wall, c, place)
        prod = dot(both, wall[place], NT)
        part = (prod[:n_rows] + minus_plus * swapped(prod[n_rows:])).astype(BF16)
        if i < n_col - 1:
            strip_out[c] = part
        else:
            strip_in[c] = part
        if i == early - 1:
            pl.semaphore_wait(barrier, n_col - 1 + n_facet - 1)
            for ready in col_order[:-1]:
                remote(MARK, marks.at[my_f, my_c], marks.at[my_f, my_c], my_f, ready).start()
            for f in facet_order[:-1]:
                remote(PEER, peers.at[my_f], peers.at[my_f], f, my_c).start()
            for ready in col_order[:early]:
                remote(STRIP, strip_out.at[ready], strip_in.at[my_c], my_f, ready).start()
        elif early <= i < n_col - 1:
            remote(STRIP, strip_out.at[c], strip_in.at[my_c], my_f, c).start()

    for s in range(n_facet):
        table(subt, n_col + s, s)
    near_re, near_im = cis(
        iota((M, n_rows), 0) * (iota((M, n_rows), 1) + (my_c * n_rows).astype(F32)), YN, -1.0
    )
    own_base[0] = near_re * inv_root
    own_base[1] = near_im * inv_root
    def unpack(packed):
        high = packed // 65536
        return packed - high * 65536, high

    peers_all.wait_recv()

    def to_gates(kind, source, into):
        for f in facet_order[:-1]:
            remote(kind, source, into, f, gate).start()

        @pl.when(my_core == 0)
        def _():
            remote(kind, source, into, my_f, gate).start()

    to_gates(MEASURED, measured.at[seat], measured.at[seat])

    def make_tables(s, carry):
        for tab, which, point in zip((u_tab, v_tab), range(2), unpack(peers[s])):
            at = iota((M, n_vis), 0) + facet_offsets[which, my_f].astype(F32)
            re, im = cis(at * point.astype(F32), FINE, 1.0)
            tab[s, :M] = (re * (1.0 / math.sqrt(SUB))).astype(tab.dtype)
            tab[s, M:] = (im * (1.0 / math.sqrt(SUB))).astype(tab.dtype)
        return carry

    loop(n_facet, make_tables)
    mark_all.wait_recv()
    for f in facet_order[:-1]:
        remote(MARKS, marks.at[my_f], marks.at[my_f], f, my_c).start()

    strips_all.wait_recv()
    strip = strip_in[...]
    if n_rows % 16:
        strip = strip.astype(F32).reshape(YN, 2 * M).astype(BF16)
    else:
        strip = strip.reshape(YN, 2 * M)
    prods = dot(subt[...].reshape(n_facet * 2 * M, YN), strip, NN)
    for s in range(n_facet):
        prod = prods[s * 2 * M : (s + 1) * 2 * M]
        part = (prod[:M] + minus_plus * swapped(prod[M:])).astype(BF16)
        with_re = dot(part, u_tab[s, :M], TN)
        with_im = dot(part, u_tab[s, M:], TN)
        rows_re = with_re[:M] - with_im[M:]
        rows_im = with_im[:M] + with_re[M:]
        v_re, v_im = v_tab[s, :M], v_tab[s, M:]
        seen_out[s, :1] = jnp.sum(rows_re * v_re - rows_im * v_im, axis=0, keepdims=True)
        seen_out[s, 1:] = jnp.sum(rows_re * v_im + rows_im * v_re, axis=0, keepdims=True)
    to_gates(SEEN, seen_out, seen_in.at[seat])

    @pl.when(at_gate)
    def _():
        seen_in[seat] = seen_out[...]

    marks_all.wait_recv()
    sub = lax.broadcasted_iota(jnp.int32, (8, n_vis), 0)
    odd = [lax.rem(sub // (1 << p), 2) == 1 for p in range(3)]
    rows_at = (my_c * n_rows).astype(F32)

    def spread(s, carry):
        for c in range(n_col):
            unit = s * n_col + c
            points[pl.ds(unit, 1)] = marks[s, c, :, :n_vis]
            shifts[pl.ds(unit, 1)] = marks[s, c, :, n_vis:]
        rows = pl.ds(pl.multiple_of(s * n_col, n_col), n_col)
        shift = shifts[rows].astype(F32) * (iota((n_col, wide), 1) + rows_at)
        own_turn[0, rows], own_turn[1, rows] = cis(shift, YN, -1.0)
        packed = points[rows]
        for which, point in enumerate(unpack(packed)):
            point = point.astype(F32)
            powers[which, 0, 0, rows], powers[which, 0, 1, rows] = cis(
                point * facet_offsets[which, my_f].astype(F32), FINE, -1.0
            )
            value = cis(point, FINE, -1.0)
            for p in range(1, N_POWER):
                powers[which, p, 0, rows], powers[which, p, 1, rows] = value
                if p < N_POWER - 1:
                    value = cmul(value, value)
        return carry

    loop(n_facet, spread)

    def power(which, p, unit):
        return powers[which, p, 0, pl.ds(unit, 1)], powers[which, p, 1, pl.ds(unit, 1)]

    def first(which, unit):
        value = None
        for p in range(3):
            re, im = power(which, 1 + p, unit)
            step = jnp.where(odd[p], re, 1.0), jnp.where(odd[p], im, 0.0)
            value = step if value is None else cmul(value, step)
        return cmul(value, power(which, 0, unit))

    def filled(which, start, unit):
        parts = [start]
        for p in range(4, N_POWER):
            by = power(which, p, unit)
            parts += [cmul(part, by) for part in parts]
        return [jnp.concatenate([part[i] for part in parts], axis=0) for i in range(2)]

    def make_path(c):
        def one(s, carry):
            unit = s * n_col + c
            u_re, u_im = filled(0, first(0, unit), unit)
            u_re, u_im = u_re.astype(BF16), u_im.astype(BF16)
            v_first = first(1, unit)
            firsts[unit, 0], firsts[unit, 1] = v_first
            re = own_turn[0, pl.ds(unit, 1), :n_rows]
            im = own_turn[1, pl.ds(unit, 1), :n_rows]
            e_re, e_im = cmul((own_base[0], own_base[1]), (re, im))
            e_tab = jnp.concatenate([e_re, e_im], axis=0).astype(BF16)
            paths[unit, :n_rows] = dot(e_tab, jnp.concatenate([u_re, u_im], axis=0), TN).astype(BF16)
            paths[unit, room : room + n_rows] = dot(
                e_tab, jnp.concatenate([u_im, -u_re], axis=0), TN
            ).astype(BF16)
            return carry

        loop(n_facet, one)

    near_order = col_order[::-1]
    for c in near_order[:6]:
        make_path(c)

    weight = SUB / math.sqrt(n_vis) / SUB
    weight *= math.sqrt(YN / (M * n_facet)) * math.sqrt(YN / (M * n_col))

    @pl.when(at_gate)
    def _():
        all_of(MEASURED, measured.at[: 2 * n_facet - 1]).wait_recv()
        all_of(SEEN, seen_in.at[: 2 * n_facet - 1]).wait_recv()
        for core in range(2):
            first = core * n_facet
            pred = seen_in[first]
            for f in range(1, n_facet):
                pred += seen_in[first + f]
            diff = (pred - measured[first : first + n_facet]) * weight
            diffs[2 * my_pair + core] = diff.astype(diffs.dtype)
        block = diffs.at[pl.ds(2 * my_pair, 2)]
        for i, c in enumerate(col_order[:-1]):
            remote(FAR if i < half else NEAR, block, block, my_f, c).start()
        for core in range(2):
            mine = seen_in[core * n_facet, my_f]
            for f in range(1, n_facet):
                mine += seen_in[core * n_facet + f, my_f]
            answer[core] = mine
        remote(ANSWER, answer.at[0], answer.at[0], my_f, 2 * my_pair).start()
        predicted[0, 0] = answer[1]

    for c in near_order[6:]:
        make_path(c)

    def gather(place):
        c = near_order[place]

        def one(i, total):
            s = lax.rem(my_f + i, n_facet)
            unit = s * n_col + c
            diff = diffs[c, s].astype(F32)
            diff = diff[:1], diff[1:]
            start = cmul((firsts[unit, 0], firsts[unit, 1]), diff)
            wgt = jnp.concatenate(filled(1, start, unit), axis=0).astype(BF16)
            return total + dot(paths[unit], wgt, NT)

        prod = loop(n_facet, one, jnp.zeros((2 * room, 2 * M), F32))
        re, im = prod[:n_rows], prod[room : room + n_rows]
        at = slice(place * 2 * M, (place + 1) * 2 * M)
        sides[:n_rows, at] = (re + minus_plus * swapped(im)).astype(BF16)
        sides[room : room + n_rows, at] = (im - minus_plus * swapped(re)).astype(BF16)

    @pl.when(at_gate)
    def _():
        all_of(NEAR, diffs.at[: half - 2]).wait_recv()

    @pl.when(my_core == 0)
    def _():
        all_of(NEAR, diffs.at[:half]).wait_recv()

    for place in range(half):
        gather(place)
    partial[...] = dot(sides[:, : half * 2 * M], wall[:half].reshape(half * 2 * M, YN), NN)
    diffs_far.wait_recv()
    for place in range(half, n_col):
        gather(place)

    for sent in (strips_all, mark_all, marks_all, peers_all):
        sent.wait_send()

    @pl.when(at_gate)
    def _():
        all_of(MEASURED, measured.at[: n_facet - 1]).wait_send()
        all_of(SEEN, seen_in.at[: n_facet - 1]).wait_send()
        all_of(FAR, diffs).wait_send()
        all_of(NEAR, diffs.at[: n_col - 2]).wait_send()
        all_of(ANSWER, answer.at[0]).wait_send()

    @pl.when(my_core == 0)
    def _():
        all_of(MEASURED, measured.at[:n_facet]).wait_send()
        all_of(SEEN, seen_in.at[:n_facet]).wait_send()
        all_of(ANSWER, answer.at[0]).wait_recv()
        predicted[0, 0] = answer[0]


def finish_kernel(predicted, sides, wall, partial, predicted_hbm, update_hbm, update, sems):
    copies = [pltpu.make_async_copy(predicted, predicted_hbm, sems.at[0])]
    copies[0].start()
    n_rows = update.shape[1]
    room = sides.shape[0] // 2
    depth = sides.shape[1] // 2
    half = wall.shape[0] // 2
    walls = wall[half:].reshape(depth, update.shape[2])
    step = 256
    for i in range(update.shape[2] // step):
        at = slice(i * step, (i + 1) * step)
        prod = dot(sides[:, depth:], walls[:, at], NN) + partial[:, at]
        update[0, :, at] = prod[:n_rows]
        update[1, :, at] = prod[room : room + n_rows]
        copies.append(pltpu.make_async_copy(update.at[:, :, at], update_hbm.at[0, :, :, at], sems.at[1 + i]))
        copies[-1].start()
    for copy in copies:
        copy.wait()


def finish(predicted, sides, wall, partial, facets_shape):
    vmem = pl.BlockSpec(memory_space=pltpu.VMEM)
    hbm = pl.BlockSpec(memory_space=pltpu.HBM)
    return pl.pallas_call(
        finish_kernel,
        out_shape=(
            jax.ShapeDtypeStruct(predicted.shape, F32),
            jax.ShapeDtypeStruct(facets_shape, F32),
        ),
        in_specs=[vmem] * 4,
        out_specs=(hbm, hbm),
        scratch_shapes=[
            pltpu.VMEM(facets_shape[1:], F32),
            pltpu.SemaphoreType.DMA((1 + facets_shape[3] // 256,)),
        ],
        compiler_params=pltpu.CompilerParams(vmem_limit_bytes=2**22),
        name="finish",
    )(predicted, sides, wall, partial)


def body(n_facet, n_col, facets, col_offsets, sub_rows, facet_offsets, vis_pos, observed):
    assert sub_rows.shape[0] == n_facet
    n_rows = facets.shape[2]
    n_vis = vis_pos.shape[3]
    vmem = pl.BlockSpec(memory_space=pltpu.VMEM)
    col_blocks = pltpu.VMEM((n_col, n_rows, 2 * M), BF16)
    table_rows = n_col + n_facet
    room = -(-n_rows // 16) * 16
    wide = -(-n_rows // 128) * 128
    n_units = n_col * n_facet
    sides = (2 * room, n_col * 2 * M)
    wall = (n_col, 2 * M, YN)
    partial = (2 * room, YN)
    held = 4 * (observed.size + math.prod(partial)) + 2 * (math.prod(sides) + math.prod(wall))
    vmem_left = (67043328 - held) // 1024 * 1024 - MARGIN
    results = pl.pallas_call(
            functools.partial(kernel, n_facet, n_col),
            out_shape=(
                pltpu.VMEM(observed.shape, F32),
                pltpu.VMEM(sides, BF16),
                pltpu.VMEM(wall, BF16),
                pltpu.VMEM(partial, F32),
            ),
            in_specs=[pl.BlockSpec(memory_space=pltpu.HBM)] * 6,
            out_specs=(vmem, vmem, vmem, vmem),
            scratch_shapes=[
                pltpu.VMEM((2, n_rows, YN), BF16),
                pltpu.SMEM(col_offsets.shape, jnp.int32),
                pltpu.SMEM(sub_rows.shape[::-1], jnp.int32),
                pltpu.SMEM(facet_offsets.shape[::-1], jnp.int32),
                pltpu.VMEM(vis_pos.shape, jnp.int32),
                pltpu.VMEM(observed.shape, F32),
                pltpu.VMEM((2, M, YN), F32),
                pltpu.VMEM((2, table_rows, YN), F32),
                pltpu.VMEM((n_facet, 2 * M, YN), BF16),
                pltpu.VMEM((n_facet, 2 * M, n_vis), BF16),
                pltpu.VMEM((n_facet, 2 * M, n_vis), F32),
                col_blocks,
                col_blocks,
                pltpu.VMEM((n_facet, 2, n_vis), F32),
                pltpu.VMEM((2 * n_facet, n_facet, 2, n_vis), F32),
                pltpu.VMEM((n_facet, 1, n_vis), jnp.int32),
                pltpu.VMEM((2 * n_facet, 2, n_vis), F32),
                pltpu.VMEM((2, 2, n_vis), F32),
                pltpu.VMEM((n_facet, n_col, 1, n_vis + wide), jnp.int32),
                pltpu.VMEM((n_units, n_vis), jnp.int32),
                pltpu.VMEM((n_units, wide), jnp.int32),
                pltpu.VMEM((2, N_POWER, 2, n_units, n_vis), F32),
                pltpu.VMEM((n_units, 2, 8, n_vis), F32),
                pltpu.VMEM((2, M, n_rows), F32),
                pltpu.VMEM((2, n_units, wide), F32),
                pltpu.VMEM((n_units, 2 * room, n_vis), BF16),
                pltpu.VMEM((n_col, n_facet, 2, n_vis), BF16),
                pltpu.SemaphoreType.DMA((6,)),
                pltpu.SemaphoreType.DMA((9,)),
                pltpu.SemaphoreType.DMA((9,)),
            ],
            compiler_params=pltpu.CompilerParams(
                collective_id=0, has_side_effects=True, vmem_limit_bytes=vmem_left
            ),
            name="predict_update",
        )(facets, col_offsets, sub_rows.T, facet_offsets.T, vis_pos, observed)
    return finish(*results, facets.shape)


def solution(mesh):
    in_specs = (
        P("facet", None, "col", None),
        P(),
        P(None, "col"),
        P(),
        P("facet", "col", None, None),
        P("facet", "col", None, None),
    )
    out_specs = (P("facet", "col", None, None), P("facet", None, "col", None))
    step = functools.partial(body, mesh.shape["facet"], mesh.shape["col"])
    return jax.shard_map(step, mesh=mesh, in_specs=in_specs, out_specs=out_specs, check_vma=False)
```

```python
import functools
import math

import jax
import jax.numpy as jnp
from jax import lax
from jax.experimental import pallas as pl
from jax.experimental.pallas import tpu as pltpu
from jax.sharding import PartitionSpec as P

M = 64
SUB = 384
FINE = 1536
YN = 768
MARGIN = 8192
MESH = pl.DeviceIdType.MESH
F32 = jnp.float32
BF16 = jnp.bfloat16


def cis(product, modulus, direction):
    turns = jnp.floor(product * (1.0 / modulus) + 0.5)
    half = (product - turns * modulus) * (direction * math.pi / modulus)
    z = half * half
    s = half * (1.0 + z * (-1 / 6 + z * (1 / 120 + z * (-1 / 5040 + z * (1 / 362880 + z * (-1 / 39916800))))))
    c = 1.0 + z * (-1 / 2 + z * (1 / 24 + z * (-1 / 720 + z * (1 / 40320 + z * (-1 / 3628800 + z * (1 / 479001600))))))
    return 1.0 - 2.0 * s * s, 2.0 * s * c


def iota(shape, axis):
    return lax.broadcasted_iota(jnp.int32, shape, axis).astype(F32)


def dot(left, right, dims):
    return lax.dot_general(left, right, (dims, ((), ())), preferred_element_type=F32)


NN = ((1,), (0,))
NT = ((1,), (1,))
TN = ((0,), (0,))
STRIP, CLOSE, MARK, MARKS, PEER, MEASURED, SEEN, NEAR, FAR, ANSWER = range(10)
N_POWER = 7


def cmul(a, b):
    return a[0] * b[0] - a[1] * b[1], a[0] * b[1] + a[1] * b[0]


def loop(n, step, carry=()):
    return lax.fori_loop(0, n, step, carry, unroll=n <= 4)


def kernel(
    n_facet,
    n_col,
    facets_hbm,
    col_offsets_hbm,
    sub_rows_hbm,
    facet_offsets_hbm,
    vis_pos_hbm,
    observed_hbm,
    predicted,
    sides,
    wall,
    partial,
    facet_buf,
    col_offsets,
    sub_rows,
    facet_offsets,
    vis_pos,
    observed,
    base,
    turn,
    subt,
    u_tab,
    v_tab,
    strip_out,
    strip_in,
    near_prods,
    seen_out,
    seen_in,
    peers,
    measured,
    answer,
    marks,
    points,
    shifts,
    powers,
    firsts,
    own_base,
    own_turn,
    paths,
    diffs,
    load_sem,
    send_sem,
    recv_sem,
):
    my_f = lax.axis_index("facet")
    my_c = lax.axis_index("col")
    n_rows = facet_buf.shape[1]
    n_vis = vis_pos.shape[3]
    room = paths.shape[1] // 2

    loads = [
        pltpu.make_async_copy(source, held, load_sem.at[i])
        for i, (source, held) in enumerate(
            (
                (col_offsets_hbm, col_offsets),
                (sub_rows_hbm, sub_rows),
                (facets_hbm.at[0], facet_buf),
                (facet_offsets_hbm, facet_offsets),
                (vis_pos_hbm, vis_pos),
                (observed_hbm, observed),
            )
        )
    ]
    for load in loads:
        load.start()
    barrier = pltpu.get_barrier_semaphore()
    n_pair = n_col // 2
    my_pair, my_core = my_c // 2, lax.rem(my_c, 2)
    side = my_pair // (n_pair // 2)
    mirrored = my_pair + side * (n_pair - 1 - 2 * my_pair)
    pair_order = []
    for place in range(n_pair - 1, 0, -1):
        target = place - (mirrored + n_pair - place) // n_pair
        pair_order.append(target + side * (n_pair - 1 - 2 * target))
    pair_order.append(my_pair)
    col_order = []
    for pair in pair_order[:-1]:
        col_order += [2 * pair, 2 * pair + 1]
    col_order += [2 * my_pair + 1 - my_core, my_c]
    bits = n_facet.bit_length() - 1
    assert n_facet == 1 << bits
    facet_order = []
    for i in range(n_facet - 1, -1, -1):
        turns = [(i >> b & 1) * (1 << b) * (1 - 2 * lax.rem(my_f // (1 << b), 2)) for b in range(bits)]
        facet_order.append(my_f + sum(turns))
    for c in col_order[:-1]:
        pl.semaphore_signal(barrier, inc=1, device_id=(my_f, c), device_id_type=MESH)
    for f in facet_order[:-1]:
        pl.semaphore_signal(barrier, inc=1, device_id=(f, my_c), device_id_type=MESH)

    def remote(kind, source, into, f, c):
        return pltpu.make_async_remote_copy(
            src_ref=source,
            dst_ref=into,
            send_sem=send_sem.at[kind],
            recv_sem=recv_sem.at[kind],
            device_id=(f, c),
            device_id_type=MESH,
        )

    def all_of(kind, block):
        return remote(kind, block, block, my_f, my_c)

    mark_all = all_of(MARK, marks.at[0, : n_col - 1])
    marks_all = all_of(MARKS, marks.at[: n_facet - 1])
    peers_all = all_of(PEER, peers.at[: n_facet - 1])
    gate = 2 * my_pair + 1
    at_gate = my_core == 1
    seat = my_core * n_facet + my_f
    half = n_col // 2
    strips_far = all_of(STRIP, strip_in.at[:half])
    strips_near = all_of(CLOSE, strip_in.at[: half - 1])
    near_start = side * half
    far_start = half - near_start
    diffs_far = all_of(FAR, diffs.at[:half])

    base_re, base_im = cis(iota((M, YN), 0) * iota((M, YN), 1), YN, -1.0)
    inv_root = 1.0 / math.sqrt(YN)
    base[0] = base_re * inv_root
    base[1] = base_im * inv_root
    along = iota((1, YN), 1)
    loads[0].wait()
    loads[1].wait()
    for c in range(n_col):
        turn[0, pl.ds(c, 1)] = along * col_offsets[c].astype(F32)
    for s in range(n_facet):
        turn[0, pl.ds(n_col + s, 1)] = along * sub_rows[0, s].astype(F32)
    turn_re, turn_im = cis(turn[0], YN, -1.0)
    turn[0] = turn_re
    turn[1] = turn_im

    def table(into, row, slot):
        re, im = turn[0, pl.ds(row, 1)], turn[1, pl.ds(row, 1)]
        into[slot, :M] = (base[0] * re - base[1] * im).astype(BF16)
        into[slot, M:] = (base[0] * im + base[1] * re).astype(BF16)

    lane = lax.broadcasted_iota(jnp.int32, (1, 2 * M), 1)
    minus_plus = jnp.where(lane < M, -1.0, 1.0)

    def swapped(value):
        return pltpu.roll(value, M, 1)

    for load in loads[3:]:
        load.wait()
    wide = marks.shape[3] - n_vis
    own_points = vis_pos[0, 0, :1] + vis_pos[0, 0, 1:] * 65536
    peers[my_f] = own_points
    measured[seat] = observed[0, 0]
    marks[my_f, my_c, :, :n_vis] = own_points
    marks[my_f, my_c, :, n_vis:] = jnp.full((1, wide), sub_rows[0, my_f], jnp.int32)

    loads[2].wait()
    both = facet_buf[...]
    if n_rows % 16:
        both = both.astype(F32).reshape(2 * n_rows, YN).astype(BF16)
    else:
        both = both.reshape(2 * n_rows, YN)
    early = half
    for i, c in enumerate(col_order):
        place = n_col - 1 - i
        table(wall, c, place)
        prod = dot(both, wall[place], NT)
        part = (prod[:n_rows] + minus_plus * swapped(prod[n_rows:])).astype(BF16)
        if i < n_col - 1:
            strip_out[c] = part
        else:
            strip_in[c] = part
        if i == early - 1:
            pl.semaphore_wait(barrier, n_col - 1 + n_facet - 1)
            for ready in col_order[:-1]:
                remote(MARK, marks.at[my_f, my_c], marks.at[my_f, my_c], my_f, ready).start()
            for f in facet_order[:-1]:
                remote(PEER, peers.at[my_f], peers.at[my_f], f, my_c).start()
            for ready in col_order[:early]:
                remote(STRIP, strip_out.at[ready], strip_in.at[my_c], my_f, ready).start()
        elif early <= i < n_col - 1:
            kind = STRIP if i < half else CLOSE
            remote(kind, strip_out.at[c], strip_in.at[my_c], my_f, c).start()

    for s in range(n_facet):
        table(subt, n_col + s, s)
    near_re, near_im = cis(
        iota((M, n_rows), 0) * (iota((M, n_rows), 1) + (my_c * n_rows).astype(F32)), YN, -1.0
    )
    own_base[0] = near_re * inv_root
    own_base[1] = near_im * inv_root
    def unpack(packed):
        high = packed // 65536
        return packed - high * 65536, high

    peers_all.wait_recv()

    def to_gates(kind, source, into):
        for f in facet_order[:-1]:
            remote(kind, source, into, f, gate).start()

        @pl.when(my_core == 0)
        def _():
            remote(kind, source, into, my_f, gate).start()

    to_gates(MEASURED, measured.at[seat], measured.at[seat])

    def make_tables(s, carry):
        for tab, which, point in zip((u_tab, v_tab), range(2), unpack(peers[s])):
            at = iota((M, n_vis), 0) + facet_offsets[which, my_f].astype(F32)
            re, im = cis(at * point.astype(F32), FINE, 1.0)
            tab[s, :M] = (re * (1.0 / math.sqrt(SUB))).astype(tab.dtype)
            tab[s, M:] = (im * (1.0 / math.sqrt(SUB))).astype(tab.dtype)
        return carry

    loop(n_facet, make_tables)
    mark_all.wait_recv()
    for f in facet_order[:-1]:
        remote(MARKS, marks.at[my_f], marks.at[my_f], f, my_c).start()

    depth = half * n_rows

    def contribute(start):
        strip = strip_in[pl.ds(start, half)]
        if n_rows % 16:
            strip = strip.astype(F32).reshape(depth, 2 * M).astype(BF16)
        else:
            strip = strip.reshape(depth, 2 * M)
        part = subt[:, :, pl.ds(pl.multiple_of(start * n_rows, depth), depth)]
        return dot(part.reshape(n_facet * 2 * M, depth), strip, NN)

    strips_near.wait_recv()
    near_prods[...] = contribute(near_start)
    strips_far.wait_recv()
    prods = contribute(far_start) + near_prods[...]
    for s in range(n_facet):
        prod = prods[s * 2 * M : (s + 1) * 2 * M]
        part = (prod[:M] + minus_plus * swapped(prod[M:])).astype(BF16)
        with_re = dot(part, u_tab[s, :M], TN)
        with_im = dot(part, u_tab[s, M:], TN)
        rows_re = with_re[:M] - with_im[M:]
        rows_im = with_im[:M] + with_re[M:]
        v_re, v_im = v_tab[s, :M], v_tab[s, M:]
        seen_out[s, :1] = jnp.sum(rows_re * v_re - rows_im * v_im, axis=0, keepdims=True)
        seen_out[s, 1:] = jnp.sum(rows_re * v_im + rows_im * v_re, axis=0, keepdims=True)
    to_gates(SEEN, seen_out, seen_in.at[seat])

    @pl.when(at_gate)
    def _():
        seen_in[seat] = seen_out[...]

    marks_all.wait_recv()
    sub = lax.broadcasted_iota(jnp.int32, (8, n_vis), 0)
    odd = [lax.rem(sub // (1 << p), 2) == 1 for p in range(3)]
    rows_at = (my_c * n_rows).astype(F32)

    def spread(s, carry):
        for c in range(n_col):
            unit = s * n_col + c
            points[pl.ds(unit, 1)] = marks[s, c, :, :n_vis]
            shifts[pl.ds(unit, 1)] = marks[s, c, :, n_vis:]
        rows = pl.ds(pl.multiple_of(s * n_col, n_col), n_col)
        shift = shifts[rows].astype(F32) * (iota((n_col, wide), 1) + rows_at)
        own_turn[0, rows], own_turn[1, rows] = cis(shift, YN, -1.0)
        packed = points[rows]
        for which, point in enumerate(unpack(packed)):
            point = point.astype(F32)
            powers[which, 0, 0, rows], powers[which, 0, 1, rows] = cis(
                point * facet_offsets[which, my_f].astype(F32), FINE, -1.0
            )
            value = cis(point, FINE, -1.0)
            for p in range(1, N_POWER):
                powers[which, p, 0, rows], powers[which, p, 1, rows] = value
                if p < N_POWER - 1:
                    value = cmul(value, value)
        return carry

    loop(n_facet, spread)

    def power(which, p, unit):
        return powers[which, p, 0, pl.ds(unit, 1)], powers[which, p, 1, pl.ds(unit, 1)]

    def first(which, unit):
        value = None
        for p in range(3):
            re, im = power(which, 1 + p, unit)
            step = jnp.where(odd[p], re, 1.0), jnp.where(odd[p], im, 0.0)
            value = step if value is None else cmul(value, step)
        return cmul(value, power(which, 0, unit))

    def filled(which, start, unit):
        parts = [start]
        for p in range(4, N_POWER):
            by = power(which, p, unit)
            parts += [cmul(part, by) for part in parts]
        return [jnp.concatenate([part[i] for part in parts], axis=0) for i in range(2)]

    def make_path(c):
        def one(s, carry):
            unit = s * n_col + c
            u_re, u_im = filled(0, first(0, unit), unit)
            u_re, u_im = u_re.astype(BF16), u_im.astype(BF16)
            v_first = first(1, unit)
            firsts[unit, 0], firsts[unit, 1] = v_first
            re = own_turn[0, pl.ds(unit, 1), :n_rows]
            im = own_turn[1, pl.ds(unit, 1), :n_rows]
            e_re, e_im = cmul((own_base[0], own_base[1]), (re, im))
            e_tab = jnp.concatenate([e_re, e_im], axis=0).astype(BF16)
            paths[unit, :n_rows] = dot(e_tab, jnp.concatenate([u_re, u_im], axis=0), TN).astype(BF16)
            paths[unit, room : room + n_rows] = dot(
                e_tab, jnp.concatenate([u_im, -u_re], axis=0), TN
            ).astype(BF16)
            return carry

        loop(n_facet, one)

    near_order = col_order[::-1]
    for c in near_order[:6]:
        make_path(c)

    weight = SUB / math.sqrt(n_vis) / SUB
    weight *= math.sqrt(YN / (M * n_facet)) * math.sqrt(YN / (M * n_col))

    @pl.when(at_gate)
    def _():
        all_of(MEASURED, measured.at[: 2 * n_facet - 1]).wait_recv()
        all_of(SEEN, seen_in.at[: 2 * n_facet - 1]).wait_recv()
        for core in range(2):
            first = core * n_facet
            pred = seen_in[first]
            for f in range(1, n_facet):
                pred += seen_in[first + f]
            diff = (pred - measured[first : first + n_facet]) * weight
            diffs[2 * my_pair + core] = diff.astype(diffs.dtype)
        block = diffs.at[pl.ds(2 * my_pair, 2)]
        for i, c in enumerate(col_order[:-1]):
            remote(FAR if i < half else NEAR, block, block, my_f, c).start()
        for core in range(2):
            mine = seen_in[core * n_facet, my_f]
            for f in range(1, n_facet):
                mine += seen_in[core * n_facet + f, my_f]
            answer[core] = mine
        remote(ANSWER, answer.at[0], answer.at[0], my_f, 2 * my_pair).start()
        predicted[0, 0] = answer[1]

    for c in near_order[6:]:
        make_path(c)

    def gather(place):
        c = near_order[place]

        def one(i, total):
            s = lax.rem(my_f + i, n_facet)
            unit = s * n_col + c
            diff = diffs[c, s].astype(F32)
            diff = diff[:1], diff[1:]
            start = cmul((firsts[unit, 0], firsts[unit, 1]), diff)
            wgt = jnp.concatenate(filled(1, start, unit), axis=0).astype(BF16)
            return total + dot(paths[unit], wgt, NT)

        prod = loop(n_facet, one, jnp.zeros((2 * room, 2 * M), F32))
        re, im = prod[:n_rows], prod[room : room + n_rows]
        at = slice(place * 2 * M, (place + 1) * 2 * M)
        sides[:n_rows, at] = (re + minus_plus * swapped(im)).astype(BF16)
        sides[room : room + n_rows, at] = (im - minus_plus * swapped(re)).astype(BF16)

    @pl.when(at_gate)
    def _():
        all_of(NEAR, diffs.at[: half - 2]).wait_recv()

    @pl.when(my_core == 0)
    def _():
        all_of(NEAR, diffs.at[:half]).wait_recv()

    for place in range(half):
        gather(place)
    partial[...] = dot(sides[:, : half * 2 * M], wall[:half].reshape(half * 2 * M, YN), NN)
    diffs_far.wait_recv()
    for place in range(half, n_col):
        gather(place)

    for sent in (strips_far, strips_near, mark_all, marks_all, peers_all):
        sent.wait_send()

    @pl.when(at_gate)
    def _():
        all_of(MEASURED, measured.at[: n_facet - 1]).wait_send()
        all_of(SEEN, seen_in.at[: n_facet - 1]).wait_send()
        all_of(FAR, diffs).wait_send()
        all_of(NEAR, diffs.at[: n_col - 2]).wait_send()
        all_of(ANSWER, answer.at[0]).wait_send()

    @pl.when(my_core == 0)
    def _():
        all_of(MEASURED, measured.at[:n_facet]).wait_send()
        all_of(SEEN, seen_in.at[:n_facet]).wait_send()
        all_of(ANSWER, answer.at[0]).wait_recv()
        predicted[0, 0] = answer[0]


def finish_kernel(predicted, sides, wall, partial, predicted_hbm, update_hbm, update, sems):
    copies = [pltpu.make_async_copy(predicted, predicted_hbm, sems.at[0])]
    copies[0].start()
    n_rows = update.shape[1]
    room = sides.shape[0] // 2
    depth = sides.shape[1] // 2
    half = wall.shape[0] // 2
    walls = wall[half:].reshape(depth, update.shape[2])
    step = 256
    for i in range(update.shape[2] // step):
        at = slice(i * step, (i + 1) * step)
        prod = dot(sides[:, depth:], walls[:, at], NN) + partial[:, at]
        update[0, :, at] = prod[:n_rows]
        update[1, :, at] = prod[room : room + n_rows]
        copies.append(pltpu.make_async_copy(update.at[:, :, at], update_hbm.at[0, :, :, at], sems.at[1 + i]))
        copies[-1].start()
    for copy in copies:
        copy.wait()


def finish(predicted, sides, wall, partial, facets_shape):
    vmem = pl.BlockSpec(memory_space=pltpu.VMEM)
    hbm = pl.BlockSpec(memory_space=pltpu.HBM)
    return pl.pallas_call(
        finish_kernel,
        out_shape=(
            jax.ShapeDtypeStruct(predicted.shape, F32),
            jax.ShapeDtypeStruct(facets_shape, F32),
        ),
        in_specs=[vmem] * 4,
        out_specs=(hbm, hbm),
        scratch_shapes=[
            pltpu.VMEM(facets_shape[1:], F32),
            pltpu.SemaphoreType.DMA((1 + facets_shape[3] // 256,)),
        ],
        compiler_params=pltpu.CompilerParams(vmem_limit_bytes=2**22),
        name="finish",
    )(predicted, sides, wall, partial)


def body(n_facet, n_col, facets, col_offsets, sub_rows, facet_offsets, vis_pos, observed):
    assert sub_rows.shape[0] == n_facet
    n_rows = facets.shape[2]
    n_vis = vis_pos.shape[3]
    vmem = pl.BlockSpec(memory_space=pltpu.VMEM)
    col_blocks = pltpu.VMEM((n_col, n_rows, 2 * M), BF16)
    table_rows = n_col + n_facet
    room = -(-n_rows // 16) * 16
    wide = -(-n_rows // 128) * 128
    n_units = n_col * n_facet
    sides = (2 * room, n_col * 2 * M)
    wall = (n_col, 2 * M, YN)
    partial = (2 * room, YN)
    held = 4 * (observed.size + math.prod(partial)) + 2 * (math.prod(sides) + math.prod(wall))
    vmem_left = (67043328 - held) // 1024 * 1024 - MARGIN
    results = pl.pallas_call(
            functools.partial(kernel, n_facet, n_col),
            out_shape=(
                pltpu.VMEM(observed.shape, F32),
                pltpu.VMEM(sides, BF16),
                pltpu.VMEM(wall, BF16),
                pltpu.VMEM(partial, F32),
            ),
            in_specs=[pl.BlockSpec(memory_space=pltpu.HBM)] * 6,
            out_specs=(vmem, vmem, vmem, vmem),
            scratch_shapes=[
                pltpu.VMEM((2, n_rows, YN), BF16),
                pltpu.SMEM(col_offsets.shape, jnp.int32),
                pltpu.SMEM(sub_rows.shape[::-1], jnp.int32),
                pltpu.SMEM(facet_offsets.shape[::-1], jnp.int32),
                pltpu.VMEM(vis_pos.shape, jnp.int32),
                pltpu.VMEM(observed.shape, F32),
                pltpu.VMEM((2, M, YN), F32),
                pltpu.VMEM((2, table_rows, YN), F32),
                pltpu.VMEM((n_facet, 2 * M, YN), BF16),
                pltpu.VMEM((n_facet, 2 * M, n_vis), BF16),
                pltpu.VMEM((n_facet, 2 * M, n_vis), F32),
                col_blocks,
                col_blocks,
                pltpu.VMEM((n_facet * 2 * M, 2 * M), F32),
                pltpu.VMEM((n_facet, 2, n_vis), F32),
                pltpu.VMEM((2 * n_facet, n_facet, 2, n_vis), F32),
                pltpu.VMEM((n_facet, 1, n_vis), jnp.int32),
                pltpu.VMEM((2 * n_facet, 2, n_vis), F32),
                pltpu.VMEM((2, 2, n_vis), F32),
                pltpu.VMEM((n_facet, n_col, 1, n_vis + wide), jnp.int32),
                pltpu.VMEM((n_units, n_vis), jnp.int32),
                pltpu.VMEM((n_units, wide), jnp.int32),
                pltpu.VMEM((2, N_POWER, 2, n_units, n_vis), F32),
                pltpu.VMEM((n_units, 2, 8, n_vis), F32),
                pltpu.VMEM((2, M, n_rows), F32),
                pltpu.VMEM((2, n_units, wide), F32),
                pltpu.VMEM((n_units, 2 * room, n_vis), BF16),
                pltpu.VMEM((n_col, n_facet, 2, n_vis), BF16),
                pltpu.SemaphoreType.DMA((6,)),
                pltpu.SemaphoreType.DMA((10,)),
                pltpu.SemaphoreType.DMA((10,)),
            ],
            compiler_params=pltpu.CompilerParams(
                collective_id=0, has_side_effects=True, vmem_limit_bytes=vmem_left
            ),
            name="predict_update",
        )(facets, col_offsets, sub_rows.T, facet_offsets.T, vis_pos, observed)
    return finish(*results, facets.shape)


def solution(mesh):
    in_specs = (
        P("facet", None, "col", None),
        P(),
        P(None, "col"),
        P(),
        P("facet", "col", None, None),
        P("facet", "col", None, None),
    )
    out_specs = (P("facet", "col", None, None), P("facet", None, "col", None))
    step = functools.partial(body, mesh.shape["facet"], mesh.shape["col"])
    return jax.shard_map(step, mesh=mesh, in_specs=in_specs, out_specs=out_specs, check_vma=False)
```

```python
import functools
import math

import jax
import jax.numpy as jnp
from jax import lax
from jax.experimental import pallas as pl
from jax.experimental.pallas import tpu as pltpu
from jax.sharding import PartitionSpec as P

M = 64
SUB = 384
FINE = 1536
YN = 768
MARGIN = 8192
MESH = pl.DeviceIdType.MESH
F32 = jnp.float32
BF16 = jnp.bfloat16


def cis(product, modulus, direction):
    turns = jnp.floor(product * (1.0 / modulus) + 0.5)
    half = (product - turns * modulus) * (direction * math.pi / modulus)
    z = half * half
    s = half * (1.0 + z * (-1 / 6 + z * (1 / 120 + z * (-1 / 5040 + z * (1 / 362880 + z * (-1 / 39916800))))))
    c = 1.0 + z * (-1 / 2 + z * (1 / 24 + z * (-1 / 720 + z * (1 / 40320 + z * (-1 / 3628800 + z * (1 / 479001600))))))
    return 1.0 - 2.0 * s * s, 2.0 * s * c


def iota(shape, axis):
    return lax.broadcasted_iota(jnp.int32, shape, axis).astype(F32)


def dot(left, right, dims):
    return lax.dot_general(left, right, (dims, ((), ())), preferred_element_type=F32)


NN = ((1,), (0,))
NT = ((1,), (1,))
TN = ((0,), (0,))
STRIP, CLOSE, MARK, MARKS, PEER, MEASURED, SEEN, NEAR, FAR, ANSWER = range(10)
N_POWER = 7


def cmul(a, b):
    return a[0] * b[0] - a[1] * b[1], a[0] * b[1] + a[1] * b[0]


def loop(n, step, carry=()):
    return lax.fori_loop(0, n, step, carry, unroll=n <= 4)


def kernel(
    n_facet,
    n_col,
    facets_hbm,
    col_offsets_hbm,
    sub_rows_hbm,
    facet_offsets_hbm,
    vis_pos_hbm,
    observed_hbm,
    predicted,
    sides,
    wall,
    partial,
    facet_buf,
    col_offsets,
    sub_rows,
    facet_offsets,
    vis_pos,
    observed,
    base,
    turn,
    subt,
    u_tab,
    v_tab,
    strip_out,
    strip_in,
    near_prods,
    seen_out,
    seen_in,
    peers,
    measured,
    answer,
    marks,
    points,
    shifts,
    powers,
    firsts,
    own_base,
    own_turn,
    paths,
    diffs,
    load_sem,
    send_sem,
    recv_sem,
):
    my_f = lax.axis_index("facet")
    my_c = lax.axis_index("col")
    n_rows = facet_buf.shape[1]
    n_vis = vis_pos.shape[3]
    room = paths.shape[1] // 2

    loads = [
        pltpu.make_async_copy(source, held, load_sem.at[i])
        for i, (source, held) in enumerate(
            (
                (col_offsets_hbm, col_offsets),
                (sub_rows_hbm, sub_rows),
                (facets_hbm.at[0], facet_buf),
                (facet_offsets_hbm, facet_offsets),
                (vis_pos_hbm, vis_pos),
                (observed_hbm, observed),
            )
        )
    ]
    barrier = pltpu.get_barrier_semaphore()
    n_pair = n_col // 2
    my_pair, my_core = my_c // 2, lax.rem(my_c, 2)
    side = my_pair // (n_pair // 2)
    mirrored = my_pair + side * (n_pair - 1 - 2 * my_pair)
    pair_order = []
    for place in range(n_pair - 1, 0, -1):
        target = place - (mirrored + n_pair - place) // n_pair
        pair_order.append(target + side * (n_pair - 1 - 2 * target))
    pair_order.append(my_pair)
    col_order = []
    for pair in pair_order[:-1]:
        col_order += [2 * pair, 2 * pair + 1]
    col_order += [2 * my_pair + 1 - my_core, my_c]
    bits = n_facet.bit_length() - 1
    assert n_facet == 1 << bits
    facet_order = []
    for i in range(n_facet - 1, -1, -1):
        turns = [(i >> b & 1) * (1 << b) * (1 - 2 * lax.rem(my_f // (1 << b), 2)) for b in range(bits)]
        facet_order.append(my_f + sum(turns))
    for c in col_order[:-1]:
        pl.semaphore_signal(barrier, inc=1, device_id=(my_f, c), device_id_type=MESH)
    for f in facet_order[:-1]:
        pl.semaphore_signal(barrier, inc=1, device_id=(f, my_c), device_id_type=MESH)
    for load in loads:
        load.start()

    def remote(kind, source, into, f, c):
        return pltpu.make_async_remote_copy(
            src_ref=source,
            dst_ref=into,
            send_sem=send_sem.at[kind],
            recv_sem=recv_sem.at[kind],
            device_id=(f, c),
            device_id_type=MESH,
        )

    def all_of(kind, block):
        return remote(kind, block, block, my_f, my_c)

    mark_all = all_of(MARK, marks.at[0, : n_col - 1])
    marks_all = all_of(MARKS, marks.at[: n_facet - 1])
    peers_all = all_of(PEER, peers.at[: n_facet - 1])
    gate = 2 * my_pair + 1
    at_gate = my_core == 1
    seat = my_core * n_facet + my_f
    half = n_col // 2
    strips_far = all_of(STRIP, strip_in.at[:half])
    strips_near = all_of(CLOSE, strip_in.at[: half - 1])
    near_start = side * half
    far_start = half - near_start
    diffs_far = all_of(FAR, diffs.at[:half])

    base_re, base_im = cis(iota((M, YN), 0) * iota((M, YN), 1), YN, -1.0)
    inv_root = 1.0 / math.sqrt(YN)
    base[0] = base_re * inv_root
    base[1] = base_im * inv_root
    along = iota((1, YN), 1)
    loads[0].wait()
    loads[1].wait()
    for c in range(n_col):
        turn[0, pl.ds(c, 1)] = along * col_offsets[c].astype(F32)
    for s in range(n_facet):
        turn[0, pl.ds(n_col + s, 1)] = along * sub_rows[0, s].astype(F32)
    turn_re, turn_im = cis(turn[0], YN, -1.0)
    turn[0] = turn_re
    turn[1] = turn_im

    def table(into, row, slot):
        re, im = turn[0, pl.ds(row, 1)], turn[1, pl.ds(row, 1)]
        into[slot, :M] = (base[0] * re - base[1] * im).astype(BF16)
        into[slot, M:] = (base[0] * im + base[1] * re).astype(BF16)

    lane = lax.broadcasted_iota(jnp.int32, (1, 2 * M), 1)
    minus_plus = jnp.where(lane < M, -1.0, 1.0)

    def swapped(value):
        return pltpu.roll(value, M, 1)

    for load in loads[3:]:
        load.wait()
    wide = marks.shape[3] - n_vis
    own_points = vis_pos[0, 0, :1] + vis_pos[0, 0, 1:] * 65536
    peers[my_f] = own_points
    measured[seat] = observed[0, 0]
    marks[my_f, my_c, :, :n_vis] = own_points
    marks[my_f, my_c, :, n_vis:] = jnp.full((1, wide), sub_rows[0, my_f], jnp.int32)

    loads[2].wait()
    both = facet_buf[...]
    if n_rows % 16:
        both = both.astype(F32).reshape(2 * n_rows, YN).astype(BF16)
    else:
        both = both.reshape(2 * n_rows, YN)
    early = half
    for i, c in enumerate(col_order):
        place = n_col - 1 - i
        table(wall, c, place)
        prod = dot(both, wall[place], NT)
        part = (prod[:n_rows] + minus_plus * swapped(prod[n_rows:])).astype(BF16)
        if i < n_col - 1:
            strip_out[c] = part
        else:
            strip_in[c] = part
        if i == early - 1:
            pl.semaphore_wait(barrier, n_col - 1 + n_facet - 1)
            for ready in col_order[:half]:
                remote(MARK, marks.at[my_f, my_c], marks.at[my_f, my_c], my_f, ready).start()
            for ready in col_order[:early]:
                remote(STRIP, strip_out.at[ready], strip_in.at[my_c], my_f, ready).start()
            for f in facet_order[:-1]:
                remote(PEER, peers.at[my_f], peers.at[my_f], f, my_c).start()
            for ready in col_order[half:-1]:
                remote(MARK, marks.at[my_f, my_c], marks.at[my_f, my_c], my_f, ready).start()
        elif early <= i < n_col - 1:
            kind = STRIP if i < half else CLOSE
            remote(kind, strip_out.at[c], strip_in.at[my_c], my_f, c).start()

    for s in range(n_facet):
        table(subt, n_col + s, s)
    near_re, near_im = cis(
        iota((M, n_rows), 0) * (iota((M, n_rows), 1) + (my_c * n_rows).astype(F32)), YN, -1.0
    )
    own_base[0] = near_re * inv_root
    own_base[1] = near_im * inv_root
    def unpack(packed):
        high = packed // 65536
        return packed - high * 65536, high

    peers_all.wait_recv()

    def to_gates(kind, source, into):
        for f in facet_order[:-1]:
            remote(kind, source, into, f, gate).start()

        @pl.when(my_core == 0)
        def _():
            remote(kind, source, into, my_f, gate).start()

    to_gates(MEASURED, measured.at[seat], measured.at[seat])

    def make_tables(s, carry):
        for tab, which, point in zip((u_tab, v_tab), range(2), unpack(peers[s])):
            at = iota((M, n_vis), 0) + facet_offsets[which, my_f].astype(F32)
            re, im = cis(at * point.astype(F32), FINE, 1.0)
            tab[s, :M] = (re * (1.0 / math.sqrt(SUB))).astype(tab.dtype)
            tab[s, M:] = (im * (1.0 / math.sqrt(SUB))).astype(tab.dtype)
        return carry

    loop(n_facet, make_tables)
    mark_all.wait_recv()
    for f in facet_order[:-1]:
        remote(MARKS, marks.at[my_f], marks.at[my_f], f, my_c).start()

    depth = half * n_rows

    def contribute(start):
        strip = strip_in[pl.ds(start, half)]
        if n_rows % 16:
            strip = strip.astype(F32).reshape(depth, 2 * M).astype(BF16)
        else:
            strip = strip.reshape(depth, 2 * M)
        part = subt[:, :, pl.ds(pl.multiple_of(start * n_rows, depth), depth)]
        return dot(part.reshape(n_facet * 2 * M, depth), strip, NN)

    strips_near.wait_recv()
    near_prods[...] = contribute(near_start)
    strips_far.wait_recv()
    prods = contribute(far_start) + near_prods[...]
    for s in range(n_facet):
        prod = prods[s * 2 * M : (s + 1) * 2 * M]
        part = (prod[:M] + minus_plus * swapped(prod[M:])).astype(BF16)
        with_re = dot(part, u_tab[s, :M], TN)
        with_im = dot(part, u_tab[s, M:], TN)
        rows_re = with_re[:M] - with_im[M:]
        rows_im = with_im[:M] + with_re[M:]
        v_re, v_im = v_tab[s, :M], v_tab[s, M:]
        seen_out[s, :1] = jnp.sum(rows_re * v_re - rows_im * v_im, axis=0, keepdims=True)
        seen_out[s, 1:] = jnp.sum(rows_re * v_im + rows_im * v_re, axis=0, keepdims=True)
    to_gates(SEEN, seen_out, seen_in.at[seat])

    @pl.when(at_gate)
    def _():
        seen_in[seat] = seen_out[...]

    marks_all.wait_recv()
    sub = lax.broadcasted_iota(jnp.int32, (8, n_vis), 0)
    odd = [lax.rem(sub // (1 << p), 2) == 1 for p in range(3)]
    rows_at = (my_c * n_rows).astype(F32)

    def spread(s, carry):
        for c in range(n_col):
            unit = s * n_col + c
            points[pl.ds(unit, 1)] = marks[s, c, :, :n_vis]
            shifts[pl.ds(unit, 1)] = marks[s, c, :, n_vis:]
        rows = pl.ds(pl.multiple_of(s * n_col, n_col), n_col)
        shift = shifts[rows].astype(F32) * (iota((n_col, wide), 1) + rows_at)
        own_turn[0, rows], own_turn[1, rows] = cis(shift, YN, -1.0)
        packed = points[rows]
        for which, point in enumerate(unpack(packed)):
            point = point.astype(F32)
            powers[which, 0, 0, rows], powers[which, 0, 1, rows] = cis(
                point * facet_offsets[which, my_f].astype(F32), FINE, -1.0
            )
            value = cis(point, FINE, -1.0)
            for p in range(1, N_POWER):
                powers[which, p, 0, rows], powers[which, p, 1, rows] = value
                if p < N_POWER - 1:
                    value = cmul(value, value)
        return carry

    loop(n_facet, spread)

    def power(which, p, unit):
        return powers[which, p, 0, pl.ds(unit, 1)], powers[which, p, 1, pl.ds(unit, 1)]

    def first(which, unit):
        value = None
        for p in range(3):
            re, im = power(which, 1 + p, unit)
            step = jnp.where(odd[p], re, 1.0), jnp.where(odd[p], im, 0.0)
            value = step if value is None else cmul(value, step)
        return cmul(value, power(which, 0, unit))

    def filled(which, start, unit):
        parts = [start]
        for p in range(4, N_POWER):
            by = power(which, p, unit)
            parts += [cmul(part, by) for part in parts]
        return [jnp.concatenate([part[i] for part in parts], axis=0) for i in range(2)]

    def make_path(c):
        def one(s, carry):
            unit = s * n_col + c
            u_re, u_im = filled(0, first(0, unit), unit)
            u_re, u_im = u_re.astype(BF16), u_im.astype(BF16)
            v_first = first(1, unit)
            firsts[unit, 0], firsts[unit, 1] = v_first
            re = own_turn[0, pl.ds(unit, 1), :n_rows]
            im = own_turn[1, pl.ds(unit, 1), :n_rows]
            e_re, e_im = cmul((own_base[0], own_base[1]), (re, im))
            e_tab = jnp.concatenate([e_re, e_im], axis=0).astype(BF16)
            paths[unit, :n_rows] = dot(e_tab, jnp.concatenate([u_re, u_im], axis=0), TN).astype(BF16)
            paths[unit, room : room + n_rows] = dot(
                e_tab, jnp.concatenate([u_im, -u_re], axis=0), TN
            ).astype(BF16)
            return carry

        loop(n_facet, one)

    near_order = col_order[::-1]
    for c in near_order[:4]:
        make_path(c)

    weight = SUB / math.sqrt(n_vis) / SUB
    weight *= math.sqrt(YN / (M * n_facet)) * math.sqrt(YN / (M * n_col))

    @pl.when(at_gate)
    def _():
        all_of(MEASURED, measured.at[: 2 * n_facet - 1]).wait_recv()
        all_of(SEEN, seen_in.at[: 2 * n_facet - 1]).wait_recv()
        for core in range(2):
            first = core * n_facet
            pred = seen_in[first]
            for f in range(1, n_facet):
                pred += seen_in[first + f]
            diff = (pred - measured[first : first + n_facet]) * weight
            diffs[2 * my_pair + core] = diff.astype(diffs.dtype)
        block = diffs.at[pl.ds(2 * my_pair, 2)]
        for i, c in enumerate(col_order[:-1]):
            remote(FAR if i < half else NEAR, block, block, my_f, c).start()
        for core in range(2):
            mine = seen_in[core * n_facet, my_f]
            for f in range(1, n_facet):
                mine += seen_in[core * n_facet + f, my_f]
            answer[core] = mine
        remote(ANSWER, answer.at[0], answer.at[0], my_f, 2 * my_pair).start()
        predicted[0, 0] = answer[1]

    for c in near_order[4:]:
        make_path(c)

    def gather(place):
        c = near_order[place]

        def one(s):
            unit = s * n_col + c
            diff = diffs[c, s].astype(F32)
            diff = diff[:1], diff[1:]
            start = cmul((firsts[unit, 0], firsts[unit, 1]), diff)
            wgt = jnp.concatenate(filled(1, start, unit), axis=0).astype(BF16)
            return dot(paths[unit], wgt, NT)

        prod = lax.fori_loop(1, n_facet, lambda s, total: total + one(s), one(0), unroll=n_facet <= 4)
        re, im = prod[:n_rows], prod[room : room + n_rows]
        at = slice(place * 2 * M, (place + 1) * 2 * M)
        sides[:n_rows, at] = (re + minus_plus * swapped(im)).astype(BF16)
        sides[room : room + n_rows, at] = (im - minus_plus * swapped(re)).astype(BF16)

    @pl.when(at_gate)
    def _():
        all_of(NEAR, diffs.at[: half - 2]).wait_recv()

    @pl.when(my_core == 0)
    def _():
        all_of(NEAR, diffs.at[:half]).wait_recv()

    for place in range(half):
        gather(place)
    partial[...] = dot(sides[:, : half * 2 * M], wall[:half].reshape(half * 2 * M, YN), NN)
    diffs_far.wait_recv()
    for place in range(half, n_col):
        gather(place)

    for sent in (strips_far, strips_near, mark_all, marks_all, peers_all):
        sent.wait_send()

    @pl.when(at_gate)
    def _():
        all_of(MEASURED, measured.at[: n_facet - 1]).wait_send()
        all_of(SEEN, seen_in.at[: n_facet - 1]).wait_send()
        all_of(FAR, diffs).wait_send()
        all_of(NEAR, diffs.at[: n_col - 2]).wait_send()
        all_of(ANSWER, answer.at[0]).wait_send()

    @pl.when(my_core == 0)
    def _():
        all_of(MEASURED, measured.at[:n_facet]).wait_send()
        all_of(SEEN, seen_in.at[:n_facet]).wait_send()
        all_of(ANSWER, answer.at[0]).wait_recv()
        predicted[0, 0] = answer[0]


def finish_kernel(predicted, sides, wall, partial, predicted_hbm, update_hbm, update, sems):
    copies = [pltpu.make_async_copy(predicted, predicted_hbm, sems.at[0])]
    copies[0].start()
    n_rows = update.shape[1]
    room = sides.shape[0] // 2
    depth = sides.shape[1] // 2
    half = wall.shape[0] // 2
    walls = wall[half:].reshape(depth, update.shape[2])
    step = 256
    for i in range(update.shape[2] // step):
        at = slice(i * step, (i + 1) * step)
        prod = dot(sides[:, depth:], walls[:, at], NN) + partial[:, at]
        update[0, :, at] = prod[:n_rows]
        update[1, :, at] = prod[room : room + n_rows]
        copies.append(pltpu.make_async_copy(update.at[:, :, at], update_hbm.at[0, :, :, at], sems.at[1 + i]))
        copies[-1].start()
    for copy in copies:
        copy.wait()


def finish(predicted, sides, wall, partial, facets_shape):
    vmem = pl.BlockSpec(memory_space=pltpu.VMEM)
    hbm = pl.BlockSpec(memory_space=pltpu.HBM)
    return pl.pallas_call(
        finish_kernel,
        out_shape=(
            jax.ShapeDtypeStruct(predicted.shape, F32),
            jax.ShapeDtypeStruct(facets_shape, F32),
        ),
        in_specs=[vmem] * 4,
        out_specs=(hbm, hbm),
        scratch_shapes=[
            pltpu.VMEM(facets_shape[1:], F32),
            pltpu.SemaphoreType.DMA((1 + facets_shape[3] // 256,)),
        ],
        compiler_params=pltpu.CompilerParams(vmem_limit_bytes=2**22),
        name="finish",
    )(predicted, sides, wall, partial)


def body(n_facet, n_col, facets, col_offsets, sub_rows, facet_offsets, vis_pos, observed):
    assert sub_rows.shape[0] == n_facet
    n_rows = facets.shape[2]
    n_vis = vis_pos.shape[3]
    vmem = pl.BlockSpec(memory_space=pltpu.VMEM)
    col_blocks = pltpu.VMEM((n_col, n_rows, 2 * M), BF16)
    table_rows = n_col + n_facet
    room = -(-n_rows // 16) * 16
    wide = -(-n_rows // 128) * 128
    n_units = n_col * n_facet
    sides = (2 * room, n_col * 2 * M)
    wall = (n_col, 2 * M, YN)
    partial = (2 * room, YN)
    held = 4 * (observed.size + math.prod(partial)) + 2 * (math.prod(sides) + math.prod(wall))
    vmem_left = (67043328 - held) // 1024 * 1024 - MARGIN
    results = pl.pallas_call(
            functools.partial(kernel, n_facet, n_col),
            out_shape=(
                pltpu.VMEM(observed.shape, F32),
                pltpu.VMEM(sides, BF16),
                pltpu.VMEM(wall, BF16),
                pltpu.VMEM(partial, F32),
            ),
            in_specs=[pl.BlockSpec(memory_space=pltpu.HBM)] * 6,
            out_specs=(vmem, vmem, vmem, vmem),
            scratch_shapes=[
                pltpu.VMEM((2, n_rows, YN), BF16),
                pltpu.SMEM(col_offsets.shape, jnp.int32),
                pltpu.SMEM(sub_rows.shape[::-1], jnp.int32),
                pltpu.SMEM(facet_offsets.shape[::-1], jnp.int32),
                pltpu.VMEM(vis_pos.shape, jnp.int32),
                pltpu.VMEM(observed.shape, F32),
                pltpu.VMEM((2, M, YN), F32),
                pltpu.VMEM((2, table_rows, YN), F32),
                pltpu.VMEM((n_facet, 2 * M, YN), BF16),
                pltpu.VMEM((n_facet, 2 * M, n_vis), BF16),
                pltpu.VMEM((n_facet, 2 * M, n_vis), F32),
                col_blocks,
                col_blocks,
                pltpu.VMEM((n_facet * 2 * M, 2 * M), F32),
                pltpu.VMEM((n_facet, 2, n_vis), F32),
                pltpu.VMEM((2 * n_facet, n_facet, 2, n_vis), F32),
                pltpu.VMEM((n_facet, 1, n_vis), jnp.int32),
                pltpu.VMEM((2 * n_facet, 2, n_vis), F32),
                pltpu.VMEM((2, 2, n_vis), F32),
                pltpu.VMEM((n_facet, n_col, 1, n_vis + wide), jnp.int32),
                pltpu.VMEM((n_units, n_vis), jnp.int32),
                pltpu.VMEM((n_units, wide), jnp.int32),
                pltpu.VMEM((2, N_POWER, 2, n_units, n_vis), F32),
                pltpu.VMEM((n_units, 2, 8, n_vis), F32),
                pltpu.VMEM((2, M, n_rows), F32),
                pltpu.VMEM((2, n_units, wide), F32),
                pltpu.VMEM((n_units, 2 * room, n_vis), BF16),
                pltpu.VMEM((n_col, n_facet, 2, n_vis), BF16),
                pltpu.SemaphoreType.DMA((6,)),
                pltpu.SemaphoreType.DMA((10,)),
                pltpu.SemaphoreType.DMA((10,)),
            ],
            compiler_params=pltpu.CompilerParams(
                collective_id=0, has_side_effects=True, vmem_limit_bytes=vmem_left
            ),
            name="predict_update",
        )(facets, col_offsets, sub_rows.T, facet_offsets.T, vis_pos, observed)
    return finish(*results, facets.shape)


def solution(mesh):
    in_specs = (
        P("facet", None, "col", None),
        P(),
        P(None, "col"),
        P(),
        P("facet", "col", None, None),
        P("facet", "col", None, None),
    )
    out_specs = (P("facet", "col", None, None), P("facet", None, "col", None))
    step = functools.partial(body, mesh.shape["facet"], mesh.shape["col"])
    return jax.shard_map(step, mesh=mesh, in_specs=in_specs, out_specs=out_specs, check_vma=False)
```

```python
import functools
import math

import jax
import jax.numpy as jnp
from jax import lax
from jax.experimental import pallas as pl
from jax.experimental.pallas import tpu as pltpu
from jax.sharding import PartitionSpec as P

M = 64
SUB = 384
FINE = 1536
YN = 768
MARGIN = 8192
MESH = pl.DeviceIdType.MESH
F32 = jnp.float32
BF16 = jnp.bfloat16


def cis(product, modulus, direction):
    turns = jnp.floor(product * (1.0 / modulus) + 0.5)
    half = (product - turns * modulus) * (direction * math.pi / modulus)
    z = half * half
    s = half * (1.0 + z * (-1 / 6 + z * (1 / 120 + z * (-1 / 5040 + z * (1 / 362880 + z * (-1 / 39916800))))))
    c = 1.0 + z * (-1 / 2 + z * (1 / 24 + z * (-1 / 720 + z * (1 / 40320 + z * (-1 / 3628800 + z * (1 / 479001600))))))
    return 1.0 - 2.0 * s * s, 2.0 * s * c


def iota(shape, axis):
    return lax.broadcasted_iota(jnp.int32, shape, axis).astype(F32)


def dot(left, right, dims):
    return lax.dot_general(left, right, (dims, ((), ())), preferred_element_type=F32)


NN = ((1,), (0,))
NT = ((1,), (1,))
TN = ((0,), (0,))
STRIP, CLOSE, MARK, MARKS, PEER, MEASURED, SEEN, MINE, NEAR, FAR, ANSWER = range(11)
N_POWER = 7


def cmul(a, b):
    return a[0] * b[0] - a[1] * b[1], a[0] * b[1] + a[1] * b[0]


def loop(n, step, carry=()):
    return lax.fori_loop(0, n, step, carry, unroll=n <= 4)


def kernel(
    n_facet,
    n_col,
    facets_hbm,
    col_offsets_hbm,
    sub_rows_hbm,
    facet_offsets_hbm,
    vis_pos_hbm,
    observed_hbm,
    predicted,
    sides,
    wall,
    partial,
    facet_buf,
    col_offsets,
    sub_rows,
    facet_offsets,
    vis_pos,
    observed,
    base,
    turn,
    subt,
    u_tab,
    v_tab,
    strip_out,
    strip_in,
    near_prods,
    seen_out,
    seen_in,
    peers,
    measured,
    answer,
    marks,
    points,
    shifts,
    powers,
    firsts,
    own_base,
    own_turn,
    paths,
    diffs,
    load_sem,
    send_sem,
    recv_sem,
):
    my_f = lax.axis_index("facet")
    my_c = lax.axis_index("col")
    n_rows = facet_buf.shape[1]
    n_vis = vis_pos.shape[3]
    room = paths.shape[1] // 2

    loads = [
        pltpu.make_async_copy(source, held, load_sem.at[i])
        for i, (source, held) in enumerate(
            (
                (col_offsets_hbm, col_offsets),
                (sub_rows_hbm, sub_rows),
                (facets_hbm.at[0], facet_buf),
                (facet_offsets_hbm, facet_offsets),
                (vis_pos_hbm, vis_pos),
                (observed_hbm, observed),
            )
        )
    ]
    barrier = pltpu.get_barrier_semaphore()
    n_pair = n_col // 2
    my_pair, my_core = my_c // 2, lax.rem(my_c, 2)
    side = my_pair // (n_pair // 2)
    mirrored = my_pair + side * (n_pair - 1 - 2 * my_pair)
    pair_order = []
    for place in range(n_pair - 1, 0, -1):
        target = place - (mirrored + n_pair - place) // n_pair
        pair_order.append(target + side * (n_pair - 1 - 2 * target))
    pair_order.append(my_pair)
    col_order = []
    for pair in pair_order[:-1]:
        col_order += [2 * pair, 2 * pair + 1]
    col_order += [2 * my_pair + 1 - my_core, my_c]
    bits = n_facet.bit_length() - 1
    assert n_facet == 1 << bits
    facet_order = []
    for i in range(n_facet - 1, -1, -1):
        turns = [(i >> b & 1) * (1 << b) * (1 - 2 * lax.rem(my_f // (1 << b), 2)) for b in range(bits)]
        facet_order.append(my_f + sum(turns))
    for c in col_order[:-1]:
        pl.semaphore_signal(barrier, inc=1, device_id=(my_f, c), device_id_type=MESH)
    for f in facet_order[:-1]:
        pl.semaphore_signal(barrier, inc=1, device_id=(f, my_c), device_id_type=MESH)
    for load in loads:
        load.start()

    def remote(kind, source, into, f, c):
        return pltpu.make_async_remote_copy(
            src_ref=source,
            dst_ref=into,
            send_sem=send_sem.at[kind],
            recv_sem=recv_sem.at[kind],
            device_id=(f, c),
            device_id_type=MESH,
        )

    def all_of(kind, block):
        return remote(kind, block, block, my_f, my_c)

    mark_all = all_of(MARK, marks.at[0, : n_col - 1])
    marks_all = all_of(MARKS, marks.at[: n_facet - 1])
    peers_all = all_of(PEER, peers.at[: n_facet - 1])
    gate = 2 * my_pair + 1
    at_gate = my_core == 1
    seat = my_core * n_facet + my_f
    half = n_col // 2
    strips_far = all_of(STRIP, strip_in.at[:half])
    strips_near = all_of(CLOSE, strip_in.at[: half - 1])
    near_start = side * half
    far_start = half - near_start
    diffs_far = all_of(FAR, diffs.at[:half])

    base_re, base_im = cis(iota((M, YN), 0) * iota((M, YN), 1), YN, -1.0)
    inv_root = 1.0 / math.sqrt(YN)
    base[0] = base_re * inv_root
    base[1] = base_im * inv_root
    along = iota((1, YN), 1)
    loads[0].wait()
    loads[1].wait()
    for c in range(n_col):
        turn[0, pl.ds(c, 1)] = along * col_offsets[c].astype(F32)
    for s in range(n_facet):
        turn[0, pl.ds(n_col + s, 1)] = along * sub_rows[0, s].astype(F32)
    turn_re, turn_im = cis(turn[0], YN, -1.0)
    turn[0] = turn_re
    turn[1] = turn_im

    def table(into, row, slot):
        re, im = turn[0, pl.ds(row, 1)], turn[1, pl.ds(row, 1)]
        into[slot, :M] = (base[0] * re - base[1] * im).astype(BF16)
        into[slot, M:] = (base[0] * im + base[1] * re).astype(BF16)

    lane = lax.broadcasted_iota(jnp.int32, (1, 2 * M), 1)
    minus_plus = jnp.where(lane < M, -1.0, 1.0)

    def swapped(value):
        return pltpu.roll(value, M, 1)

    for load in loads[3:]:
        load.wait()
    wide = marks.shape[3] - n_vis
    own_points = vis_pos[0, 0, :1] + vis_pos[0, 0, 1:] * 65536
    peers[my_f] = own_points
    measured[seat] = observed[0, 0]
    marks[my_f, my_c, :, :n_vis] = own_points
    marks[my_f, my_c, :, n_vis:] = jnp.full((1, wide), sub_rows[0, my_f], jnp.int32)

    loads[2].wait()
    both = facet_buf[...]
    if n_rows % 16:
        both = both.astype(F32).reshape(2 * n_rows, YN).astype(BF16)
    else:
        both = both.reshape(2 * n_rows, YN)
    early = half
    for i, c in enumerate(col_order):
        place = n_col - 1 - i
        table(wall, c, place)
        prod = dot(both, wall[place], NT)
        part = (prod[:n_rows] + minus_plus * swapped(prod[n_rows:])).astype(BF16)
        if i < n_col - 1:
            strip_out[c] = part
        else:
            strip_in[c] = part
        if i == early - 1:
            pl.semaphore_wait(barrier, n_col - 1 + n_facet - 1)
            for ready in col_order[:half]:
                remote(MARK, marks.at[my_f, my_c], marks.at[my_f, my_c], my_f, ready).start()
            for ready in col_order[:early]:
                remote(STRIP, strip_out.at[ready], strip_in.at[my_c], my_f, ready).start()
            for f in facet_order[:-1]:
                remote(PEER, peers.at[my_f], peers.at[my_f], f, my_c).start()
            for ready in col_order[half:-1]:
                remote(MARK, marks.at[my_f, my_c], marks.at[my_f, my_c], my_f, ready).start()
        elif early <= i < n_col - 1:
            kind = STRIP if i < half else CLOSE
            remote(kind, strip_out.at[c], strip_in.at[my_c], my_f, c).start()

    for s in range(n_facet):
        table(subt, n_col + s, s)
    near_re, near_im = cis(
        iota((M, n_rows), 0) * (iota((M, n_rows), 1) + (my_c * n_rows).astype(F32)), YN, -1.0
    )
    own_base[0] = near_re * inv_root
    own_base[1] = near_im * inv_root
    def unpack(packed):
        high = packed // 65536
        return packed - high * 65536, high

    peers_all.wait_recv()

    def to_gates(kind, source, into):
        for f in facet_order[:-1]:
            remote(kind, source, into, f, gate).start()

        @pl.when(my_core == 0)
        def _():
            remote(kind, source, into, my_f, gate).start()

    to_gates(MEASURED, measured.at[seat], measured.at[seat])

    def make_tables(s, carry):
        for tab, which, point in zip((u_tab, v_tab), range(2), unpack(peers[s])):
            at = iota((M, n_vis), 0) + facet_offsets[which, my_f].astype(F32)
            re, im = cis(at * point.astype(F32), FINE, 1.0)
            tab[s, :M] = (re * (1.0 / math.sqrt(SUB))).astype(tab.dtype)
            tab[s, M:] = (im * (1.0 / math.sqrt(SUB))).astype(tab.dtype)
        return carry

    loop(n_facet, make_tables)
    mark_all.wait_recv()
    for f in facet_order[:-1]:
        remote(MARKS, marks.at[my_f], marks.at[my_f], f, my_c).start()

    depth = half * n_rows

    def contribute(start):
        strip = strip_in[pl.ds(start, half)]
        if n_rows % 16:
            strip = strip.astype(F32).reshape(depth, 2 * M).astype(BF16)
        else:
            strip = strip.reshape(depth, 2 * M)
        part = subt[:, :, pl.ds(pl.multiple_of(start * n_rows, depth), depth)]
        return dot(part.reshape(n_facet * 2 * M, depth), strip, NN)

    strips_near.wait_recv()
    near_prods[...] = contribute(near_start)
    strips_far.wait_recv()
    prods = contribute(far_start) + near_prods[...]
    for s in range(n_facet):
        prod = prods[s * 2 * M : (s + 1) * 2 * M]
        part = (prod[:M] + minus_plus * swapped(prod[M:])).astype(BF16)
        with_re = dot(part, u_tab[s, :M], TN)
        with_im = dot(part, u_tab[s, M:], TN)
        rows_re = with_re[:M] - with_im[M:]
        rows_im = with_im[:M] + with_re[M:]
        v_re, v_im = v_tab[s, :M], v_tab[s, M:]
        seen_out[s, :1] = jnp.sum(rows_re * v_re - rows_im * v_im, axis=0, keepdims=True)
        seen_out[s, 1:] = jnp.sum(rows_re * v_im + rows_im * v_re, axis=0, keepdims=True)
    to_gates(SEEN, seen_out, seen_in.at[seat])

    @pl.when(at_gate)
    def _():
        seen_in[seat] = seen_out[...]

    marks_all.wait_recv()
    sub = lax.broadcasted_iota(jnp.int32, (8, n_vis), 0)
    odd = [lax.rem(sub // (1 << p), 2) == 1 for p in range(3)]
    rows_at = (my_c * n_rows).astype(F32)

    def spread(s, carry):
        for c in range(n_col):
            unit = s * n_col + c
            points[pl.ds(unit, 1)] = marks[s, c, :, :n_vis]
            shifts[pl.ds(unit, 1)] = marks[s, c, :, n_vis:]
        rows = pl.ds(pl.multiple_of(s * n_col, n_col), n_col)
        shift = shifts[rows].astype(F32) * (iota((n_col, wide), 1) + rows_at)
        own_turn[0, rows], own_turn[1, rows] = cis(shift, YN, -1.0)
        packed = points[rows]
        for which, point in enumerate(unpack(packed)):
            point = point.astype(F32)
            powers[which, 0, 0, rows], powers[which, 0, 1, rows] = cis(
                point * facet_offsets[which, my_f].astype(F32), FINE, -1.0
            )
            value = cis(point, FINE, -1.0)
            for p in range(1, N_POWER):
                powers[which, p, 0, rows], powers[which, p, 1, rows] = value
                if p < N_POWER - 1:
                    value = cmul(value, value)
        return carry

    loop(n_facet, spread)

    def power(which, p, unit):
        return powers[which, p, 0, pl.ds(unit, 1)], powers[which, p, 1, pl.ds(unit, 1)]

    def first(which, unit):
        value = None
        for p in range(3):
            re, im = power(which, 1 + p, unit)
            step = jnp.where(odd[p], re, 1.0), jnp.where(odd[p], im, 0.0)
            value = step if value is None else cmul(value, step)
        return cmul(value, power(which, 0, unit))

    def filled(which, start, unit):
        parts = [start]
        for p in range(4, N_POWER):
            by = power(which, p, unit)
            parts += [cmul(part, by) for part in parts]
        return [jnp.concatenate([part[i] for part in parts], axis=0) for i in range(2)]

    def make_path(c):
        def one(s, carry):
            unit = s * n_col + c
            u_re, u_im = filled(0, first(0, unit), unit)
            u_re, u_im = u_re.astype(BF16), u_im.astype(BF16)
            v_first = first(1, unit)
            firsts[unit, 0], firsts[unit, 1] = v_first
            re = own_turn[0, pl.ds(unit, 1), :n_rows]
            im = own_turn[1, pl.ds(unit, 1), :n_rows]
            e_re, e_im = cmul((own_base[0], own_base[1]), (re, im))
            e_tab = jnp.concatenate([e_re, e_im], axis=0).astype(BF16)
            paths[unit, :n_rows] = dot(e_tab, jnp.concatenate([u_re, u_im], axis=0), TN).astype(BF16)
            paths[unit, room : room + n_rows] = dot(
                e_tab, jnp.concatenate([u_im, -u_re], axis=0), TN
            ).astype(BF16)
            return carry

        loop(n_facet, one)

    near_order = col_order[::-1]
    for c in near_order[:4]:
        make_path(c)

    weight = SUB / math.sqrt(n_vis) / SUB
    weight *= math.sqrt(YN / (M * n_facet)) * math.sqrt(YN / (M * n_col))

    @pl.when(at_gate)
    def _():
        all_of(MEASURED, measured.at[: 2 * n_facet - 1]).wait_recv()
        all_of(SEEN, seen_in.at[: 2 * n_facet - 1]).wait_recv()
        for core in range(2):
            first = core * n_facet
            pred = seen_in[first]
            for f in range(1, n_facet):
                pred += seen_in[first + f]
            diff = (pred - measured[first : first + n_facet]) * weight
            diffs[2 * my_pair + core] = diff.astype(diffs.dtype)
        block = diffs.at[pl.ds(2 * my_pair, 2)]
        for i, c in enumerate(col_order[:-1]):
            remote(FAR if i < half else NEAR if i < n_col - 2 else MINE, block, block, my_f, c).start()
        for core in range(2):
            mine = seen_in[core * n_facet, my_f]
            for f in range(1, n_facet):
                mine += seen_in[core * n_facet + f, my_f]
            answer[core] = mine
        remote(ANSWER, answer.at[0], answer.at[0], my_f, 2 * my_pair).start()
        predicted[0, 0] = answer[1]

    for c in near_order[4:]:
        make_path(c)

    def gather(place):
        c = near_order[place]

        def one(s):
            unit = s * n_col + c
            diff = diffs[c, s].astype(F32)
            diff = diff[:1], diff[1:]
            start = cmul((firsts[unit, 0], firsts[unit, 1]), diff)
            wgt = jnp.concatenate(filled(1, start, unit), axis=0).astype(BF16)
            return dot(paths[unit], wgt, NT)

        prod = lax.fori_loop(1, n_facet, lambda s, total: total + one(s), one(0), unroll=n_facet <= 4)
        re, im = prod[:n_rows], prod[room : room + n_rows]
        at = slice(place * 2 * M, (place + 1) * 2 * M)
        sides[:n_rows, at] = (re + minus_plus * swapped(im)).astype(BF16)
        sides[room : room + n_rows, at] = (im - minus_plus * swapped(re)).astype(BF16)

    @pl.when(my_core == 0)
    def _():
        all_of(MINE, diffs.at[:2]).wait_recv()

    for step in range(2):
        gather(step)
    diffs_near = all_of(NEAR, diffs.at[: half - 2])
    diffs_near.wait_recv()
    for step in range(2, half):
        gather(step)
    partial[...] = dot(sides[:, : half * 2 * M], wall[:half].reshape(half * 2 * M, YN), NN)
    diffs_far.wait_recv()
    for place in range(half, n_col):
        gather(place)

    for sent in (strips_far, strips_near, mark_all, marks_all, peers_all):
        sent.wait_send()

    @pl.when(at_gate)
    def _():
        all_of(MEASURED, measured.at[: n_facet - 1]).wait_send()
        all_of(SEEN, seen_in.at[: n_facet - 1]).wait_send()
        all_of(FAR, diffs).wait_send()
        all_of(NEAR, diffs.at[: n_col - 4]).wait_send()
        all_of(MINE, diffs.at[:2]).wait_send()
        all_of(ANSWER, answer.at[0]).wait_send()

    @pl.when(my_core == 0)
    def _():
        all_of(MEASURED, measured.at[:n_facet]).wait_send()
        all_of(SEEN, seen_in.at[:n_facet]).wait_send()
        all_of(ANSWER, answer.at[0]).wait_recv()
        predicted[0, 0] = answer[0]


def finish_kernel(predicted, sides, wall, partial, predicted_hbm, update_hbm, update, sems):
    copies = [pltpu.make_async_copy(predicted, predicted_hbm, sems.at[0])]
    copies[0].start()
    n_rows = update.shape[1]
    room = sides.shape[0] // 2
    depth = sides.shape[1] // 2
    half = wall.shape[0] // 2
    walls = wall[half:].reshape(depth, update.shape[2])
    step = 256
    for i in range(update.shape[2] // step):
        at = slice(i * step, (i + 1) * step)
        prod = dot(sides[:, depth:], walls[:, at], NN) + partial[:, at]
        update[0, :, at] = prod[:n_rows]
        update[1, :, at] = prod[room : room + n_rows]
        copies.append(pltpu.make_async_copy(update.at[:, :, at], update_hbm.at[0, :, :, at], sems.at[1 + i]))
        copies[-1].start()
    for copy in copies:
        copy.wait()


def finish(predicted, sides, wall, partial, facets_shape):
    vmem = pl.BlockSpec(memory_space=pltpu.VMEM)
    hbm = pl.BlockSpec(memory_space=pltpu.HBM)
    return pl.pallas_call(
        finish_kernel,
        out_shape=(
            jax.ShapeDtypeStruct(predicted.shape, F32),
            jax.ShapeDtypeStruct(facets_shape, F32),
        ),
        in_specs=[vmem] * 4,
        out_specs=(hbm, hbm),
        scratch_shapes=[
            pltpu.VMEM(facets_shape[1:], F32),
            pltpu.SemaphoreType.DMA((1 + facets_shape[3] // 256,)),
        ],
        compiler_params=pltpu.CompilerParams(vmem_limit_bytes=2**22),
        name="finish",
    )(predicted, sides, wall, partial)


def body(n_facet, n_col, facets, col_offsets, sub_rows, facet_offsets, vis_pos, observed):
    assert sub_rows.shape[0] == n_facet
    n_rows = facets.shape[2]
    n_vis = vis_pos.shape[3]
    vmem = pl.BlockSpec(memory_space=pltpu.VMEM)
    col_blocks = pltpu.VMEM((n_col, n_rows, 2 * M), BF16)
    table_rows = n_col + n_facet
    room = -(-n_rows // 16) * 16
    wide = -(-n_rows // 128) * 128
    n_units = n_col * n_facet
    sides = (2 * room, n_col * 2 * M)
    wall = (n_col, 2 * M, YN)
    partial = (2 * room, YN)
    held = 4 * (observed.size + math.prod(partial)) + 2 * (math.prod(sides) + math.prod(wall))
    vmem_left = (67043328 - held) // 1024 * 1024 - MARGIN
    results = pl.pallas_call(
            functools.partial(kernel, n_facet, n_col),
            out_shape=(
                pltpu.VMEM(observed.shape, F32),
                pltpu.VMEM(sides, BF16),
                pltpu.VMEM(wall, BF16),
                pltpu.VMEM(partial, F32),
            ),
            in_specs=[pl.BlockSpec(memory_space=pltpu.HBM)] * 6,
            out_specs=(vmem, vmem, vmem, vmem),
            scratch_shapes=[
                pltpu.VMEM((2, n_rows, YN), BF16),
                pltpu.SMEM(col_offsets.shape, jnp.int32),
                pltpu.SMEM(sub_rows.shape[::-1], jnp.int32),
                pltpu.SMEM(facet_offsets.shape[::-1], jnp.int32),
                pltpu.VMEM(vis_pos.shape, jnp.int32),
                pltpu.VMEM(observed.shape, F32),
                pltpu.VMEM((2, M, YN), F32),
                pltpu.VMEM((2, table_rows, YN), F32),
                pltpu.VMEM((n_facet, 2 * M, YN), BF16),
                pltpu.VMEM((n_facet, 2 * M, n_vis), BF16),
                pltpu.VMEM((n_facet, 2 * M, n_vis), F32),
                col_blocks,
                col_blocks,
                pltpu.VMEM((n_facet * 2 * M, 2 * M), F32),
                pltpu.VMEM((n_facet, 2, n_vis), F32),
                pltpu.VMEM((2 * n_facet, n_facet, 2, n_vis), F32),
                pltpu.VMEM((n_facet, 1, n_vis), jnp.int32),
                pltpu.VMEM((2 * n_facet, 2, n_vis), F32),
                pltpu.VMEM((2, 2, n_vis), F32),
                pltpu.VMEM((n_facet, n_col, 1, n_vis + wide), jnp.int32),
                pltpu.VMEM((n_units, n_vis), jnp.int32),
                pltpu.VMEM((n_units, wide), jnp.int32),
                pltpu.VMEM((2, N_POWER, 2, n_units, n_vis), F32),
                pltpu.VMEM((n_units, 2, 8, n_vis), F32),
                pltpu.VMEM((2, M, n_rows), F32),
                pltpu.VMEM((2, n_units, wide), F32),
                pltpu.VMEM((n_units, 2 * room, n_vis), BF16),
                pltpu.VMEM((n_col, n_facet, 2, n_vis), BF16),
                pltpu.SemaphoreType.DMA((6,)),
                pltpu.SemaphoreType.DMA((11,)),
                pltpu.SemaphoreType.DMA((11,)),
            ],
            compiler_params=pltpu.CompilerParams(
                collective_id=0, has_side_effects=True, vmem_limit_bytes=vmem_left
            ),
            name="predict_update",
        )(facets, col_offsets, sub_rows.T, facet_offsets.T, vis_pos, observed)
    return finish(*results, facets.shape)


def solution(mesh):
    in_specs = (
        P("facet", None, "col", None),
        P(),
        P(None, "col"),
        P(),
        P("facet", "col", None, None),
        P("facet", "col", None, None),
    )
    out_specs = (P("facet", "col", None, None), P("facet", None, "col", None))
    step = functools.partial(body, mesh.shape["facet"], mesh.shape["col"])
    return jax.shard_map(step, mesh=mesh, in_specs=in_specs, out_specs=out_specs, check_vma=False)
```

```python
import functools
import math

import jax
import jax.numpy as jnp
from jax import lax
from jax.experimental import pallas as pl
from jax.experimental.pallas import tpu as pltpu
from jax.sharding import PartitionSpec as P

M = 64
SUB = 384
FINE = 1536
YN = 768
MARGIN = 8192
MESH = pl.DeviceIdType.MESH
F32 = jnp.float32
BF16 = jnp.bfloat16


def cis(product, modulus, direction):
    turns = jnp.floor(product * (1.0 / modulus) + 0.5)
    half = (product - turns * modulus) * (direction * math.pi / modulus)
    z = half * half
    s = half * (1.0 + z * (-1 / 6 + z * (1 / 120 + z * (-1 / 5040 + z * (1 / 362880 + z * (-1 / 39916800))))))
    c = 1.0 + z * (-1 / 2 + z * (1 / 24 + z * (-1 / 720 + z * (1 / 40320 + z * (-1 / 3628800 + z * (1 / 479001600))))))
    return 1.0 - 2.0 * s * s, 2.0 * s * c


def iota(shape, axis):
    return lax.broadcasted_iota(jnp.int32, shape, axis).astype(F32)


def dot(left, right, dims):
    return lax.dot_general(left, right, (dims, ((), ())), preferred_element_type=F32)


NN = ((1,), (0,))
NT = ((1,), (1,))
TN = ((0,), (0,))
STRIP, CLOSE, MARK, MARKS, PEER, MEASURED, SEEN, NEAR, FAR, ANSWER = range(10)
N_POWER = 7


def cmul(a, b):
    return a[0] * b[0] - a[1] * b[1], a[0] * b[1] + a[1] * b[0]


def loop(n, step, carry=()):
    return lax.fori_loop(0, n, step, carry, unroll=n <= 4)


def kernel(
    n_facet,
    n_col,
    facets_hbm,
    col_offsets_hbm,
    sub_rows_hbm,
    facet_offsets_hbm,
    vis_pos_hbm,
    observed_hbm,
    predicted,
    sides,
    wall,
    partial,
    facet_buf,
    col_offsets,
    sub_rows,
    facet_offsets,
    vis_pos,
    observed,
    base,
    turn,
    subt,
    u_tab,
    v_tab,
    strip_out,
    strip_in,
    near_prods,
    seen_out,
    seen_in,
    peers,
    measured,
    answer,
    marks,
    points,
    shifts,
    powers,
    firsts,
    own_base,
    own_turn,
    paths,
    diffs,
    load_sem,
    send_sem,
    recv_sem,
):
    my_f = lax.axis_index("facet")
    my_c = lax.axis_index("col")
    n_rows = facet_buf.shape[1]
    n_vis = vis_pos.shape[3]
    room = paths.shape[1] // 2

    loads = [
        pltpu.make_async_copy(source, held, load_sem.at[i])
        for i, (source, held) in enumerate(
            (
                (col_offsets_hbm, col_offsets),
                (sub_rows_hbm, sub_rows),
                (facets_hbm.at[0], facet_buf),
                (facet_offsets_hbm, facet_offsets),
                (vis_pos_hbm, vis_pos),
                (observed_hbm, observed),
            )
        )
    ]
    barrier = pltpu.get_barrier_semaphore()
    n_pair = n_col // 2
    my_pair, my_core = my_c // 2, lax.rem(my_c, 2)
    side = my_pair // (n_pair // 2)
    mirrored = my_pair + side * (n_pair - 1 - 2 * my_pair)
    pair_order = []
    for place in range(n_pair - 1, 0, -1):
        target = place - (mirrored + n_pair - place) // n_pair
        pair_order.append(target + side * (n_pair - 1 - 2 * target))
    pair_order.append(my_pair)
    col_order = []
    for pair in pair_order[:-1]:
        col_order += [2 * pair, 2 * pair + 1]
    col_order += [2 * my_pair + 1 - my_core, my_c]
    bits = n_facet.bit_length() - 1
    assert n_facet == 1 << bits
    facet_order = []
    for i in range(n_facet - 1, -1, -1):
        turns = [(i >> b & 1) * (1 << b) * (1 - 2 * lax.rem(my_f // (1 << b), 2)) for b in range(bits)]
        facet_order.append(my_f + sum(turns))
    for c in col_order[:-1]:
        pl.semaphore_signal(barrier, inc=1, device_id=(my_f, c), device_id_type=MESH)
    for f in facet_order[:-1]:
        pl.semaphore_signal(barrier, inc=1, device_id=(f, my_c), device_id_type=MESH)
    for load in loads:
        load.start()

    def remote(kind, source, into, f, c):
        return pltpu.make_async_remote_copy(
            src_ref=source,
            dst_ref=into,
            send_sem=send_sem.at[kind],
            recv_sem=recv_sem.at[kind],
            device_id=(f, c),
            device_id_type=MESH,
        )

    def all_of(kind, block):
        return remote(kind, block, block, my_f, my_c)

    mark_all = all_of(MARK, marks.at[0, : n_col - 1])
    marks_all = all_of(MARKS, marks.at[: n_facet - 1])
    peers_all = all_of(PEER, peers.at[: n_facet - 1])
    gate = 2 * my_pair + 1
    at_gate = my_core == 1
    seat = my_core * n_facet + my_f
    half = n_col // 2
    strips_far = all_of(STRIP, strip_in.at[:half])
    strips_near = all_of(CLOSE, strip_in.at[: half - 1])
    near_start = side * half
    far_start = half - near_start
    diffs_far = all_of(FAR, diffs.at[:half])

    base_re, base_im = cis(iota((M, YN), 0) * iota((M, YN), 1), YN, -1.0)
    inv_root = 1.0 / math.sqrt(YN)
    base[0] = base_re * inv_root
    base[1] = base_im * inv_root
    along = iota((1, YN), 1)
    loads[0].wait()
    loads[1].wait()
    for c in range(n_col):
        turn[0, pl.ds(c, 1)] = along * col_offsets[c].astype(F32)
    for s in range(n_facet):
        turn[0, pl.ds(n_col + s, 1)] = along * sub_rows[0, s].astype(F32)
    turn_re, turn_im = cis(turn[0], YN, -1.0)
    turn[0] = turn_re
    turn[1] = turn_im

    def table(into, row, slot):
        re, im = turn[0, pl.ds(row, 1)], turn[1, pl.ds(row, 1)]
        into[slot, :M] = (base[0] * re - base[1] * im).astype(BF16)
        into[slot, M:] = (base[0] * im + base[1] * re).astype(BF16)

    lane = lax.broadcasted_iota(jnp.int32, (1, 2 * M), 1)
    minus_plus = jnp.where(lane < M, -1.0, 1.0)

    def swapped(value):
        return pltpu.roll(value, M, 1)

    for load in loads[3:]:
        load.wait()
    wide = marks.shape[3] - n_vis
    own_points = vis_pos[0, 0, :1] + vis_pos[0, 0, 1:] * 65536
    peers[my_f] = own_points
    measured[seat] = observed[0, 0]
    marks[my_f, my_c, :, :n_vis] = own_points
    marks[my_f, my_c, :, n_vis:] = jnp.full((1, wide), sub_rows[0, my_f], jnp.int32)

    loads[2].wait()
    both = facet_buf[...]
    if n_rows % 16:
        both = both.astype(F32).reshape(2 * n_rows, YN).astype(BF16)
    else:
        both = both.reshape(2 * n_rows, YN)
    early = half - 1
    for i, c in enumerate(col_order):
        place = n_col - 1 - i
        table(wall, c, place)
        prod = dot(both, wall[place], NT)
        part = (prod[:n_rows] + minus_plus * swapped(prod[n_rows:])).astype(BF16)
        if i < n_col - 1:
            strip_out[c] = part
        else:
            strip_in[c] = part
        if i == early - 1:
            pl.semaphore_wait(barrier, n_col - 1 + n_facet - 1)
            for ready in col_order[:half]:
                remote(MARK, marks.at[my_f, my_c], marks.at[my_f, my_c], my_f, ready).start()
            for ready in col_order[:early]:
                remote(STRIP, strip_out.at[ready], strip_in.at[my_c], my_f, ready).start()
            for f in facet_order[:-1]:
                remote(PEER, peers.at[my_f], peers.at[my_f], f, my_c).start()
            for ready in col_order[half:-1]:
                remote(MARK, marks.at[my_f, my_c], marks.at[my_f, my_c], my_f, ready).start()
        elif early <= i < n_col - 1:
            kind = STRIP if i < half else CLOSE
            remote(kind, strip_out.at[c], strip_in.at[my_c], my_f, c).start()

    for s in range(n_facet):
        table(subt, n_col + s, s)
    near_re, near_im = cis(
        iota((M, n_rows), 0) * (iota((M, n_rows), 1) + (my_c * n_rows).astype(F32)), YN, -1.0
    )
    own_base[0] = near_re * inv_root
    own_base[1] = near_im * inv_root
    def unpack(packed):
        high = packed // 65536
        return packed - high * 65536, high

    peers_all.wait_recv()

    def to_gates(kind, source, into):
        for f in facet_order[:-1]:
            remote(kind, source, into, f, gate).start()

        @pl.when(my_core == 0)
        def _():
            remote(kind, source, into, my_f, gate).start()

    to_gates(MEASURED, measured.at[seat], measured.at[seat])

    def make_tables(s, carry):
        for tab, which, point in zip((u_tab, v_tab), range(2), unpack(peers[s])):
            at = iota((M, n_vis), 0) + facet_offsets[which, my_f].astype(F32)
            re, im = cis(at * point.astype(F32), FINE, 1.0)
            tab[s, :M] = (re * (1.0 / math.sqrt(SUB))).astype(tab.dtype)
            tab[s, M:] = (im * (1.0 / math.sqrt(SUB))).astype(tab.dtype)
        return carry

    loop(n_facet, make_tables)
    mark_all.wait_recv()
    for f in facet_order[:-1]:
        remote(MARKS, marks.at[my_f], marks.at[my_f], f, my_c).start()

    depth = half * n_rows

    def contribute(start):
        strip = strip_in[pl.ds(start, half)]
        if n_rows % 16:
            strip = strip.astype(F32).reshape(depth, 2 * M).astype(BF16)
        else:
            strip = strip.reshape(depth, 2 * M)
        part = subt[:, :, pl.ds(pl.multiple_of(start * n_rows, depth), depth)]
        return dot(part.reshape(n_facet * 2 * M, depth), strip, NN)

    strips_near.wait_recv()
    near_prods[...] = contribute(near_start)
    strips_far.wait_recv()
    prods = contribute(far_start) + near_prods[...]
    for s in range(n_facet):
        prod = prods[s * 2 * M : (s + 1) * 2 * M]
        part = (prod[:M] + minus_plus * swapped(prod[M:])).astype(BF16)
        with_re = dot(part, u_tab[s, :M], TN)
        with_im = dot(part, u_tab[s, M:], TN)
        rows_re = with_re[:M] - with_im[M:]
        rows_im = with_im[:M] + with_re[M:]
        v_re, v_im = v_tab[s, :M], v_tab[s, M:]
        seen_out[s, :1] = jnp.sum(rows_re * v_re - rows_im * v_im, axis=0, keepdims=True)
        seen_out[s, 1:] = jnp.sum(rows_re * v_im + rows_im * v_re, axis=0, keepdims=True)
    to_gates(SEEN, seen_out, seen_in.at[seat])

    @pl.when(at_gate)
    def _():
        seen_in[seat] = seen_out[...]

    marks_all.wait_recv()
    sub = lax.broadcasted_iota(jnp.int32, (8, n_vis), 0)
    odd = [lax.rem(sub // (1 << p), 2) == 1 for p in range(3)]
    rows_at = (my_c * n_rows).astype(F32)

    def spread(s, carry):
        for c in range(n_col):
            unit = s * n_col + c
            points[pl.ds(unit, 1)] = marks[s, c, :, :n_vis]
            shifts[pl.ds(unit, 1)] = marks[s, c, :, n_vis:]
        rows = pl.ds(pl.multiple_of(s * n_col, n_col), n_col)
        shift = shifts[rows].astype(F32) * (iota((n_col, wide), 1) + rows_at)
        own_turn[0, rows], own_turn[1, rows] = cis(shift, YN, -1.0)
        packed = points[rows]
        for which, point in enumerate(unpack(packed)):
            point = point.astype(F32)
            powers[which, 0, 0, rows], powers[which, 0, 1, rows] = cis(
                point * facet_offsets[which, my_f].astype(F32), FINE, -1.0
            )
            value = cis(point, FINE, -1.0)
            for p in range(1, N_POWER):
                powers[which, p, 0, rows], powers[which, p, 1, rows] = value
                if p < N_POWER - 1:
                    value = cmul(value, value)
        return carry

    loop(n_facet, spread)

    def power(which, p, unit):
        return powers[which, p, 0, pl.ds(unit, 1)], powers[which, p, 1, pl.ds(unit, 1)]

    def first(which, unit):
        value = None
        for p in range(3):
            re, im = power(which, 1 + p, unit)
            step = jnp.where(odd[p], re, 1.0), jnp.where(odd[p], im, 0.0)
            value = step if value is None else cmul(value, step)
        return cmul(value, power(which, 0, unit))

    def filled(which, start, unit):
        parts = [start]
        for p in range(4, N_POWER):
            by = power(which, p, unit)
            parts += [cmul(part, by) for part in parts]
        return [jnp.concatenate([part[i] for part in parts], axis=0) for i in range(2)]

    def make_path(c):
        def one(s, carry):
            unit = s * n_col + c
            u_re, u_im = filled(0, first(0, unit), unit)
            u_re, u_im = u_re.astype(BF16), u_im.astype(BF16)
            v_first = first(1, unit)
            firsts[unit, 0], firsts[unit, 1] = v_first
            re = own_turn[0, pl.ds(unit, 1), :n_rows]
            im = own_turn[1, pl.ds(unit, 1), :n_rows]
            e_re, e_im = cmul((own_base[0], own_base[1]), (re, im))
            e_tab = jnp.concatenate([e_re, e_im], axis=0).astype(BF16)
            paths[unit, :n_rows] = dot(e_tab, jnp.concatenate([u_re, u_im], axis=0), TN).astype(BF16)
            paths[unit, room : room + n_rows] = dot(
                e_tab, jnp.concatenate([u_im, -u_re], axis=0), TN
            ).astype(BF16)
            return carry

        loop(n_facet, one)

    near_order = col_order[::-1]
    for c in near_order[:4]:
        make_path(c)

    weight = SUB / math.sqrt(n_vis) / SUB
    weight *= math.sqrt(YN / (M * n_facet)) * math.sqrt(YN / (M * n_col))

    @pl.when(at_gate)
    def _():
        all_of(MEASURED, measured.at[: 2 * n_facet - 1]).wait_recv()
        all_of(SEEN, seen_in.at[: 2 * n_facet - 1]).wait_recv()
        for core in range(2):
            first = core * n_facet
            pred = seen_in[first]
            for f in range(1, n_facet):
                pred += seen_in[first + f]
            diff = (pred - measured[first : first + n_facet]) * weight
            diffs[2 * my_pair + core] = diff.astype(diffs.dtype)
        block = diffs.at[pl.ds(2 * my_pair, 2)]
        for i, c in enumerate(col_order[:-1]):
            remote(FAR if i < half else NEAR, block, block, my_f, c).start()
        for core in range(2):
            mine = seen_in[core * n_facet, my_f]
            for f in range(1, n_facet):
                mine += seen_in[core * n_facet + f, my_f]
            answer[core] = mine
        remote(ANSWER, answer.at[0], answer.at[0], my_f, 2 * my_pair).start()
        predicted[0, 0] = answer[1]

    for c in near_order[4:]:
        make_path(c)

    def gather(place):
        c = near_order[place]

        def one(s):
            unit = s * n_col + c
            diff = diffs[c, s].astype(F32)
            diff = diff[:1], diff[1:]
            start = cmul((firsts[unit, 0], firsts[unit, 1]), diff)
            wgt = jnp.concatenate(filled(1, start, unit), axis=0).astype(BF16)
            return dot(paths[unit], wgt, NT)

        prod = lax.fori_loop(1, n_facet, lambda s, total: total + one(s), one(0), unroll=n_facet <= 4)
        re, im = prod[:n_rows], prod[room : room + n_rows]
        at = slice(place * 2 * M, (place + 1) * 2 * M)
        sides[:n_rows, at] = (re + minus_plus * swapped(im)).astype(BF16)
        sides[room : room + n_rows, at] = (im - minus_plus * swapped(re)).astype(BF16)

    @pl.when(at_gate)
    def _():
        all_of(NEAR, diffs.at[: half - 2]).wait_recv()

    @pl.when(my_core == 0)
    def _():
        all_of(NEAR, diffs.at[:half]).wait_recv()

    for place in range(half):
        gather(place)
    partial[...] = dot(sides[:, : half * 2 * M], wall[:half].reshape(half * 2 * M, YN), NN)
    diffs_far.wait_recv()
    for place in range(half, n_col):
        gather(place)

    for sent in (strips_far, strips_near, mark_all, marks_all, peers_all):
        sent.wait_send()

    @pl.when(at_gate)
    def _():
        all_of(MEASURED, measured.at[: n_facet - 1]).wait_send()
        all_of(SEEN, seen_in.at[: n_facet - 1]).wait_send()
        all_of(FAR, diffs).wait_send()
        all_of(NEAR, diffs.at[: n_col - 2]).wait_send()
        all_of(ANSWER, answer.at[0]).wait_send()

    @pl.when(my_core == 0)
    def _():
        all_of(MEASURED, measured.at[:n_facet]).wait_send()
        all_of(SEEN, seen_in.at[:n_facet]).wait_send()
        all_of(ANSWER, answer.at[0]).wait_recv()
        predicted[0, 0] = answer[0]


def finish_kernel(predicted, sides, wall, partial, predicted_hbm, update_hbm, update, sems):
    copies = [pltpu.make_async_copy(predicted, predicted_hbm, sems.at[0])]
    copies[0].start()
    n_rows = update.shape[1]
    room = sides.shape[0] // 2
    depth = sides.shape[1] // 2
    half = wall.shape[0] // 2
    walls = wall[half:].reshape(depth, update.shape[2])
    step = 256
    for i in range(update.shape[2] // step):
        at = slice(i * step, (i + 1) * step)
        prod = dot(sides[:, depth:], walls[:, at], NN) + partial[:, at]
        update[0, :, at] = prod[:n_rows]
        update[1, :, at] = prod[room : room + n_rows]
        copies.append(pltpu.make_async_copy(update.at[:, :, at], update_hbm.at[0, :, :, at], sems.at[1 + i]))
        copies[-1].start()
    for copy in copies:
        copy.wait()


def finish(predicted, sides, wall, partial, facets_shape):
    vmem = pl.BlockSpec(memory_space=pltpu.VMEM)
    hbm = pl.BlockSpec(memory_space=pltpu.HBM)
    return pl.pallas_call(
        finish_kernel,
        out_shape=(
            jax.ShapeDtypeStruct(predicted.shape, F32),
            jax.ShapeDtypeStruct(facets_shape, F32),
        ),
        in_specs=[vmem] * 4,
        out_specs=(hbm, hbm),
        scratch_shapes=[
            pltpu.VMEM(facets_shape[1:], F32),
            pltpu.SemaphoreType.DMA((1 + facets_shape[3] // 256,)),
        ],
        compiler_params=pltpu.CompilerParams(vmem_limit_bytes=2**22),
        name="finish",
    )(predicted, sides, wall, partial)


def body(n_facet, n_col, facets, col_offsets, sub_rows, facet_offsets, vis_pos, observed):
    assert sub_rows.shape[0] == n_facet
    n_rows = facets.shape[2]
    n_vis = vis_pos.shape[3]
    vmem = pl.BlockSpec(memory_space=pltpu.VMEM)
    col_blocks = pltpu.VMEM((n_col, n_rows, 2 * M), BF16)
    table_rows = n_col + n_facet
    room = -(-n_rows // 16) * 16
    wide = -(-n_rows // 128) * 128
    n_units = n_col * n_facet
    sides = (2 * room, n_col * 2 * M)
    wall = (n_col, 2 * M, YN)
    partial = (2 * room, YN)
    held = 4 * (observed.size + math.prod(partial)) + 2 * (math.prod(sides) + math.prod(wall))
    vmem_left = (67043328 - held) // 1024 * 1024 - MARGIN
    results = pl.pallas_call(
            functools.partial(kernel, n_facet, n_col),
            out_shape=(
                pltpu.VMEM(observed.shape, F32),
                pltpu.VMEM(sides, BF16),
                pltpu.VMEM(wall, BF16),
                pltpu.VMEM(partial, F32),
            ),
            in_specs=[pl.BlockSpec(memory_space=pltpu.HBM)] * 6,
            out_specs=(vmem, vmem, vmem, vmem),
            scratch_shapes=[
                pltpu.VMEM((2, n_rows, YN), BF16),
                pltpu.SMEM(col_offsets.shape, jnp.int32),
                pltpu.SMEM(sub_rows.shape[::-1], jnp.int32),
                pltpu.SMEM(facet_offsets.shape[::-1], jnp.int32),
                pltpu.VMEM(vis_pos.shape, jnp.int32),
                pltpu.VMEM(observed.shape, F32),
                pltpu.VMEM((2, M, YN), F32),
                pltpu.VMEM((2, table_rows, YN), F32),
                pltpu.VMEM((n_facet, 2 * M, YN), BF16),
                pltpu.VMEM((n_facet, 2 * M, n_vis), BF16),
                pltpu.VMEM((n_facet, 2 * M, n_vis), F32),
                col_blocks,
                col_blocks,
                pltpu.VMEM((n_facet * 2 * M, 2 * M), F32),
                pltpu.VMEM((n_facet, 2, n_vis), F32),
                pltpu.VMEM((2 * n_facet, n_facet, 2, n_vis), F32),
                pltpu.VMEM((n_facet, 1, n_vis), jnp.int32),
                pltpu.VMEM((2 * n_facet, 2, n_vis), F32),
                pltpu.VMEM((2, 2, n_vis), F32),
                pltpu.VMEM((n_facet, n_col, 1, n_vis + wide), jnp.int32),
                pltpu.VMEM((n_units, n_vis), jnp.int32),
                pltpu.VMEM((n_units, wide), jnp.int32),
                pltpu.VMEM((2, N_POWER, 2, n_units, n_vis), F32),
                pltpu.VMEM((n_units, 2, 8, n_vis), F32),
                pltpu.VMEM((2, M, n_rows), F32),
                pltpu.VMEM((2, n_units, wide), F32),
                pltpu.VMEM((n_units, 2 * room, n_vis), BF16),
                pltpu.VMEM((n_col, n_facet, 2, n_vis), BF16),
                pltpu.SemaphoreType.DMA((6,)),
                pltpu.SemaphoreType.DMA((10,)),
                pltpu.SemaphoreType.DMA((10,)),
            ],
            compiler_params=pltpu.CompilerParams(
                collective_id=0, has_side_effects=True, vmem_limit_bytes=vmem_left
            ),
            name="predict_update",
        )(facets, col_offsets, sub_rows.T, facet_offsets.T, vis_pos, observed)
    return finish(*results, facets.shape)


def solution(mesh):
    in_specs = (
        P("facet", None, "col", None),
        P(),
        P(None, "col"),
        P(),
        P("facet", "col", None, None),
        P("facet", "col", None, None),
    )
    out_specs = (P("facet", "col", None, None), P("facet", None, "col", None))
    step = functools.partial(body, mesh.shape["facet"], mesh.shape["col"])
    return jax.shard_map(step, mesh=mesh, in_specs=in_specs, out_specs=out_specs, check_vma=False)
```
